256 devices in a mesh: row: 16 (over x, y), col: 16 (over z, core).
Axes of the slice: x: 4, y: 4, z: 8, core: 2. Of those that a mesh axis runs over, the one named last changes fastest.
Arguments:
- points: bfloat16 [40960, 64], P(('row', 'col')), may hold values from -5 to 5
- start_vectors: bfloat16 [40960, 32], P(('row', 'col')), may hold values from -12 to 12
Outputs:
- basis: float32 [40960, 32], P(('row', 'col'))
The draws below stay inside these ranges and needn't reach their ends.
All inputs are finite; a program needn't handle non-finite values.
Results may differ from the reference program's by a relative error of at most 0.007.
Values may be sent and summed in bfloat16 or wider, within the bound.
No kernel may reach another device: no remote copies, remote signals or barrier semaphores. Data moves between devices by JAX's collectives and lax.ppermute only.
A program may use at most 64 MiB of HBM per device.

```python
import jax
import jax.numpy as jnp
from jax import lax

F = 64
K = 32
ITERS = 2
PTS_BLK = 2560
POINTS = 40960


def draw_points(key, part):
    order_key, center_key, noise_key, sigma_key = jax.random.split(jax.random.fold_in(key, 11), 4)
    pairs = POINTS // 2
    order = jax.random.permutation(order_key, POINTS)
    pair_of = jnp.zeros((POINTS,), jnp.int32).at[order].set(jnp.arange(POINTS, dtype=jnp.int32) // 2)
    sigma = jnp.exp(jax.random.uniform(sigma_key, (pairs, 1), jnp.float32, jnp.log(0.15), jnp.log(0.4)))
    centers = jnp.clip(jax.random.normal(center_key, (pairs, F), jnp.float32), -4.0, 4.0)
    noise = jnp.clip(jax.random.normal(noise_key, (POINTS, F), jnp.float32), -3.0, 3.0)
    values = centers[pair_of] + sigma[pair_of] * noise
    return jnp.clip(values, -5.0, 5.0).astype(jnp.bfloat16)


def draw_start_vectors(key, part):
    position = jnp.arange(POINTS, dtype=jnp.float32)[:, None] / POINTS
    base = jnp.clip(jax.random.normal(key, (POINTS, K), jnp.float32), -3.0, 3.0)
    values = base * jnp.exp(jnp.log(4.0) * position)
    return jnp.clip(values, -12.0, 12.0).astype(jnp.bfloat16)


def setup_inputs(seed: int = 0) -> dict:
    key_of = jax.random.split(jax.random.key(seed), 3)
    return {
        "points": draw_points(jax.random.fold_in(key_of[2], 71), 0),
        "start_vectors": draw_start_vectors(jax.random.fold_in(key_of[2], 71), 0),
    }


KERNEL_SCALE = 5.12

def kernel_block(block_pts, block_sq, all_pts, all_sq):
    cross = jnp.dot(block_pts.astype(jnp.float32), all_pts.T.astype(jnp.float32), preferred_element_type=jnp.float32)
    dist = block_sq[:, None] + all_sq[None, :] - 2.0 * cross
    return jnp.exp(dist * (-KERNEL_SCALE / F)).astype(jnp.bfloat16)

def reference(points, start_vectors):
    sq_norms = jnp.sum(jnp.square(points.astype(jnp.float32)), axis=1)
    height = min(512, PTS_BLK)
    count = POINTS // height
    stacked = (points.reshape(count, height, F), sq_norms.reshape(count, height))

    def degree_block(item):
        weights = kernel_block(item[0], item[1], points, sq_norms)
        return jnp.sum(weights, axis=1, dtype=jnp.float32)
    degree = lax.map(degree_block, stacked).reshape(POINTS)
    vectors = start_vectors
    ortho = jnp.zeros((POINTS, K), jnp.float32)
    for step in range(ITERS):

        def product_block(item, panel=vectors):
            weights = kernel_block(item[0], item[1], points, sq_norms)
            return jnp.dot(weights.astype(jnp.float32), panel.astype(jnp.float32), preferred_element_type=jnp.float32)
        product = lax.map(product_block, stacked).reshape(POINTS, K)
        scaled = product / degree[:, None]
        gram = jnp.dot(scaled.T.astype(jnp.float32), scaled.astype(jnp.float32), precision=lax.Precision.HIGHEST, preferred_element_type=jnp.float32) / POINTS
        lower = jnp.linalg.cholesky(gram)
        ortho = lax.linalg.triangular_solve(lower, scaled, left_side=False, lower=True, transpose_a=True)
        vectors = ortho.astype(jnp.bfloat16)
    return ortho
```

```python
import math

import jax
import jax.numpy as jnp
from jax import lax
from jax.experimental import pallas as pl
from jax.experimental.pallas import tpu as pltpu
from jax.sharding import PartitionSpec as P

KERNEL_SCALE = 5.12
F32 = jnp.float32
BF16 = jnp.bfloat16
HIGHEST = lax.Precision.HIGHEST
LANES = 128
SMALL = pltpu.CompilerParams(vmem_limit_bytes=32 * 1024 * 1024)
VEC, ONES, NORM, END = 64, 96, 99, 102


def lane_of(shape):
    return lax.broadcasted_iota(jnp.int32, shape, len(shape) - 1)


def roll(x, shift):
    shift %= LANES
    return pltpu.roll(x, shift, 1) if shift else x


def pieces(x):
    first = x.astype(BF16).astype(F32)
    second = (x - first).astype(BF16).astype(F32)
    return first, second, x - first - second


def widen(x):
    rows, width = x.shape
    return jnp.concatenate([x, jnp.zeros((rows, LANES - width), x.dtype)], axis=1)


def quarters_packed(x):
    n = x.shape[0] // 4
    x = jnp.where(lane_of(x.shape) < 32, x, 0.0)
    parts = [roll(x[q * n : (q + 1) * n], 32 * q) for q in range(4)]
    return (parts[0] + parts[1]) + (parts[2] + parts[3])


def quarters_unpacked(x):
    keep = lane_of(x.shape) < 32
    parts = [jnp.where(keep, roll(x, -32 * q), 0.0) for q in range(4)]
    return jnp.concatenate(parts, axis=0)


def inverse_factor(gram):
    n = gram.shape[0]
    lane = lane_of(gram.shape)
    row = lax.broadcasted_iota(jnp.int32, gram.shape, 0)
    a = jnp.where(lane < n, gram, 0.0) + jnp.where(lane == row + n, 1.0, 0.0)
    for j in range(n):
        pivot = a[j : j + 1, j : j + 1]
        scale = 1.0 / jnp.sqrt(pivot)
        top = a[j : j + 1, :] * scale
        column = jnp.where(row > j, a[:, j : j + 1] * scale, 0.0)
        a = jnp.where(row == j, top, a - column * top)
    return jnp.where(lane < n, roll(a, -n), 0.0)


def pack_body(count, log_scale):
    def body(points_ref, vectors_ref, cols_ref, rows_ref):
        pts = points_ref[...].astype(F32)
        half = pts.shape[0] // 2
        wide = widen(pts)
        norm = jnp.sum(wide * wide, axis=1, keepdims=True) * (-0.5 * log_scale)
        vec = roll(widen(vectors_ref[...].astype(F32)), VEC)
        lane = lane_of(wide.shape)
        out = jnp.where(lane < VEC, wide, vec)
        out = jnp.where((lane >= ONES) & (lane < NORM), 1.0, out)
        for i, piece in enumerate(pieces(norm)):
            out = jnp.where(lane == NORM + i, piece, out)
        out = out.astype(BF16)
        packed = (wide[:half] + roll(wide[half:], VEC)).astype(BF16)
        for i in range(count):
            cols_ref[i] = out
            rows_ref[i] = packed

    return body


def left_operand(packed, log_scale):
    raw = packed.astype(F32)
    lane = lane_of(raw.shape)
    low = lane < VEC
    scaled = raw * log_scale
    first = scaled.astype(BF16).astype(F32)
    second = scaled - first
    squares = raw * raw
    halves = []
    for side in range(2):
        mine = low if side == 0 else jnp.logical_not(low)
        norm = jnp.sum(jnp.where(mine, squares, 0.0), axis=1, keepdims=True) * (-0.5 * log_scale)
        one, two = (first, second) if side == 0 else (roll(first, VEC), roll(second, VEC))
        one = jnp.where(low, one, jnp.where((lane >= NORM) & (lane < END), 1.0, 0.0))
        for i, piece in enumerate(pieces(norm)):
            one = jnp.where(lane == ONES + i, piece, one)
        two = jnp.where(low, two, 0.0)
        halves.append(jnp.concatenate([one.astype(BF16), two.astype(BF16)], axis=1))
    return jnp.concatenate(halves, axis=0)


def first_body(count, group, log_scale):
    total = count * group
    chunk = 512

    def body(rows_ref, cols_ref, aff_ref, send_ref):
        def block(b, carry):
            left = left_operand(rows_ref[b], log_scale)
            acc = jnp.zeros((group, LANES), F32)
            for start in range(0, total, chunk):
                cols = cols_ref[start : start + chunk, :]
                power = lax.dot_general(
                    left,
                    jnp.concatenate([cols, cols], axis=1),
                    (((1,), (1,)), ((), ())),
                    preferred_element_type=F32,
                )
                weights = jnp.exp2(power).astype(BF16)
                aff_ref[b, :, start : start + chunk] = weights
                acc = acc + jnp.dot(weights, cols, preferred_element_type=F32)
            send_ref[b, 0:40, :] = quarters_packed(roll(acc, -VEC))
            lane = lane_of((8, LANES))
            degree = jnp.zeros((8, LANES), F32)
            for k in range(group // 8):
                column = acc[8 * k : 8 * k + 8, ONES : ONES + 1]
                degree = jnp.where(lane == k, column, degree)
            send_ref[b, 40:48, :] = degree
            return carry

        lax.fori_loop(0, count, block, 0)

    return body


def gram_of(x):
    return lax.dot_general(
        x, x, (((0,), (0,)), ((), ())), precision=HIGHEST, preferred_element_type=F32
    )


def scale_body(count):
    def body(recv_ref, spread_ref, degree_ref):
        total = jnp.sum(recv_ref[...], axis=0)
        degree = total[40:48]
        lane = lane_of((8, LANES))
        wide = []
        for j in range(5):
            piece = jnp.broadcast_to(degree[:, j : j + 1], (8, LANES))
            for q in range(1, 4):
                k = 5 * q + j
                piece = jnp.where(lane >= 32 * q, degree[:, k : k + 1], piece)
            wide.append(piece)
        wide = jnp.concatenate(wide, axis=0)
        degree_ref[...] = wide
        scaled = quarters_unpacked(total[0:40] / wide)
        gram = gram_of(scaled)[0:32]
        first = scaled.astype(BF16).astype(F32)
        out = first + roll(scaled - first, 32)
        one, two, three = pieces(jnp.where(lane_of(gram.shape) < 32, gram, 0.0))
        zeros = jnp.zeros((out.shape[0] - 64, LANES), F32)
        extra = jnp.concatenate([roll(one, 64) + roll(two, 96), roll(three, 64), zeros], axis=0)
        out = (out + extra).astype(BF16)
        for i in range(count):
            spread_ref[i] = out

    return body


def second_body(count, group):
    def body(aff_ref, spread_ref, send_ref):
        sums = jnp.zeros((64, LANES), F32)
        for i in range(count):
            sums = sums + spread_ref[i * group : i * group + 64, :].astype(F32)
        gram = roll(sums[0:32], -64) + roll(sums[0:32], -96) + roll(sums[32:64], -64)
        gram = quarters_packed(gram)

        def block(b, carry):
            acc = jnp.dot(aff_ref[b], spread_ref[...], preferred_element_type=F32)
            send_ref[b, 0:40, :] = quarters_packed(acc + roll(acc, -32))
            send_ref[b, 40:48, :] = gram
            return carry

        lax.fori_loop(0, count, block, 0)

    return body


def apply_inverse(x, inverse):
    inverse = jnp.concatenate([inverse, jnp.zeros((LANES - 32, LANES), F32)], axis=0)
    return lax.dot_general(
        x, inverse, (((1,), (1,)), ((), ())), precision=HIGHEST, preferred_element_type=F32
    )


def middle_body(count, points):
    def body(recv_ref, degree_ref, scaled_ref, gram_ref):
        total = jnp.sum(recv_ref[...], axis=0)
        inverse = inverse_factor(quarters_unpacked(total[40:48]) / points)
        product = quarters_unpacked(total[0:40] / degree_ref[...])
        scaled = apply_inverse(product, inverse)
        scaled_ref[...] = scaled
        gram = quarters_packed(gram_of(scaled)[0:32])
        for i in range(count):
            gram_ref[i] = gram

    return body


def again_body(count):
    def body(recv_ref, gram_ref):
        gram = jnp.sum(recv_ref[...], axis=0)
        for i in range(count):
            gram_ref[i] = gram

    return body


def last_body(points):
    def body(recv_ref, scaled_ref, out_ref):
        gram = quarters_unpacked(jnp.sum(recv_ref[...], axis=0)) / points
        out_ref[...] = apply_inverse(scaled_ref[...], inverse_factor(gram))[:, 0:32]

    return body


def shards(points, start_vectors):
    group, features = points.shape
    row, col = lax.axis_size("row"), lax.axis_size("col")
    total = group * row * col
    log_scale = 2.0 * KERNEL_SCALE / features * math.log2(math.e)
    shape = jax.ShapeDtypeStruct

    def exchange(x, axis):
        return lax.all_to_all(x, axis, 0, 0, tiled=True)

    cols, rows = pl.pallas_call(
        pack_body(row, log_scale),
        out_shape=(shape((row, group, LANES), BF16), shape((col, group // 2, LANES), BF16)),
        name="pack",
        compiler_params=SMALL,
    )(points, start_vectors)
    cols = exchange(cols, "row").reshape(row * group, LANES)
    rows = exchange(rows, "col")
    aff, send = pl.pallas_call(
        first_body(col, group, log_scale),
        out_shape=(pltpu.VMEM((col, group, row * group), BF16), shape((col, 48, LANES), F32)),
        name="first",
        compiler_params=SMALL,
    )(rows, cols)
    spread, degree = pl.pallas_call(
        scale_body(row),
        out_shape=(shape((row, group, LANES), BF16), shape((40, LANES), F32)),
        name="scale",
        compiler_params=SMALL,
    )(exchange(send, "col"))
    spread = exchange(spread, "row").reshape(row * group, LANES)
    send = pl.pallas_call(
        second_body(col, group), out_shape=shape((col, 48, LANES), F32), name="second",
        compiler_params=SMALL,
    )(aff, spread)
    scaled, gram = pl.pallas_call(
        middle_body(row, total),
        out_shape=(shape((group, LANES), F32), shape((row, 8, LANES), F32)),
        name="middle",
    )(exchange(send, "col"), degree)
    gram = pl.pallas_call(
        again_body(col), out_shape=shape((col, 8, LANES), F32), name="again"
    )(exchange(gram, "row"))
    return pl.pallas_call(
        last_body(total), out_shape=shape((group, 32), F32), name="last"
    )(exchange(gram, "col"), scaled)


def solution(mesh):
    spec = P(("row", "col"), None)
    return jax.shard_map(
        shards, mesh=mesh, in_specs=(spec, spec), out_specs=spec, check_vma=False
    )
```

```python
import math

import jax
import jax.numpy as jnp
from jax import lax
from jax.experimental import pallas as pl
from jax.experimental.pallas import tpu as pltpu
from jax.sharding import PartitionSpec as P

KERNEL_SCALE = 5.12
F32 = jnp.float32
BF16 = jnp.bfloat16
LANES = 128
PARAMS = pltpu.CompilerParams(vmem_limit_bytes=32 * 1024 * 1024)
REST = 32
WIDTH = 512
NORM, ONES, END = 64, 67, 70


def lane_of(shape):
    return lax.broadcasted_iota(jnp.int32, shape, len(shape) - 1)


def row_of(shape):
    return lax.broadcasted_iota(jnp.int32, shape, len(shape) - 2)


def roll(x, shift):
    shift %= LANES
    return pltpu.roll(x, shift, 1) if shift else x


def fold(x, place=0):
    h = x.shape[0] // 4
    group = lane_of((h, LANES)) // REST
    out = jnp.zeros((h, LANES), F32)
    for g in range(4):
        out = jnp.where(group == g, roll(x[g * h : (g + 1) * h], REST * (g - place)), out)
    return out


def unfold(pieces):
    h = pieces[0].shape[0]
    group = lane_of((h, LANES)) // REST
    rows = []
    for g in range(4):
        out = jnp.zeros((h, LANES), F32)
        for q, piece in enumerate(pieces):
            out = jnp.where(group == q, roll(piece, REST * (q - g)), out)
        rows.append(out)
    return jnp.concatenate(rows, axis=0)


def split(x):
    first = x.astype(BF16).astype(F32)
    second = (x - first).astype(BF16).astype(F32)
    return first, second, x - first - second


def widen(x):
    return jnp.concatenate([x, jnp.zeros((x.shape[0], LANES - x.shape[1]), x.dtype)], axis=1)


def main_and_rest(x):
    return x[:, 0:LANES], fold(widen(x[:, LANES : LANES + REST]))


def copies(ref, value):
    for i in range(ref.shape[0]):
        ref[i] = value


def pack_body(points_ref, vectors_ref, cols_ref, rows_ref):
    pts = points_ref[...].astype(F32)
    main, rest = main_and_rest(pts)
    copies(rows_ref, jnp.concatenate([main, rest], axis=0).astype(BF16))
    features, group = pts.shape
    half = group // 2
    flat = jnp.concatenate([main, widen(pts[:, LANES:])], axis=1)
    flat = jnp.concatenate([flat, jnp.zeros_like(flat)], axis=0).T
    by_point = flat[0:half] + roll(flat[half:group], features)
    main, rest = main_and_rest(vectors_ref[...].astype(F32))
    parts = [by_point, main, rest, jnp.zeros((8, LANES), F32)]
    copies(cols_ref, jnp.concatenate(parts, axis=0).astype(BF16))


def first_body(log_scale):
    def body(rows_ref, cols_ref, aff_ref, send_ref, left_ref, right_ref, vec_ref):
        count = rows_ref.shape[0]
        total = left_ref.shape[0]

        def put_right(tile, raw):
            n, at = divmod(tile * LANES, WIDTH)
            scaled = raw * log_scale
            first = scaled.astype(BF16)
            norm = jnp.sum(raw * raw, axis=0, keepdims=True) * (-0.5 * log_scale)
            row = row_of((16, LANES))
            extra = jnp.where(row < ONES - NORM, 1.0, 0.0)
            for i, piece in enumerate(split(norm)):
                extra = jnp.where(row == ONES - NORM + i, piece, extra)
            right_ref[n, 0:64, at : at + LANES] = first
            right_ref[n, 64:80, at : at + LANES] = extra.astype(BF16)
            right_ref[n, 80:128, at : at + LANES] = jnp.zeros((48, LANES), BF16)
            right_ref[n, 128:192, at : at + LANES] = (scaled - first.astype(F32)).astype(BF16)
            right_ref[n, 192:256, at : at + LANES] = jnp.zeros((64, LANES), BF16)

        for i in range(count):
            put_right(i, rows_ref[i, 0:64].astype(F32))
        for m in range(count // 4):
            rests = [rows_ref[4 * m + q, 64:80].astype(F32) for q in range(4)]
            put_right(count + m, unfold(rests))

        lane = lane_of((80, LANES))
        low = lane < NORM
        for i in range(count):
            raw = cols_ref[i, 0:80].astype(F32)
            squares = raw * raw
            blocks = []
            for side in range(2):
                mine = low if side == 0 else jnp.logical_not(low)
                norm = jnp.sum(jnp.where(mine, squares, 0.0), axis=1, keepdims=True)
                norm = norm * (-0.5 * log_scale)
                block = jnp.where(low, raw if side == 0 else roll(raw, NORM), 0.0)
                for k, piece in enumerate(split(norm)):
                    block = jnp.where(lane == NORM + k, piece, block)
                block = jnp.where((lane >= ONES) & (lane < END), 1.0, block)
                blocks.append(block.astype(BF16))
            at = i * LANES
            left_ref[at : at + 80, :] = blocks[0]
            left_ref[at + 80 : at + LANES, :] = blocks[1][0:48]
            at = count * LANES + i * REST
            left_ref[at : at + REST, :] = blocks[1][48:80]

        vec_ref[32:48, :] = jnp.where(row_of((16, total)) == 0, 1.0, 0.0).astype(BF16)
        for i in range(count):
            vec_ref[0:32, i * LANES : (i + 1) * LANES] = cols_ref[i, 80:112]
        for m in range(count // 4):
            rests = [cols_ref[4 * m + q, 112:128].astype(F32)[0:8] for q in range(4)]
            at = (count + m) * LANES
            vec_ref[0:32, at : at + LANES] = unfold(rests).astype(BF16)

        chunk = 512

        def product(n):
            right = right_ref[n]
            for at in range(0, total, chunk):
                left = left_ref[at : at + chunk, :]
                power = jnp.dot(
                    jnp.concatenate([left, left], axis=1), right, preferred_element_type=F32
                )
                aff_ref[n, at : at + chunk, :] = jnp.exp2(power).astype(BF16)
            return jnp.dot(vec_ref[...], aff_ref[n], preferred_element_type=F32)

        def block(n, carry):
            out = product(n)
            for k in range(WIDTH // LANES):
                tile = out[:, k * LANES : (k + 1) * LANES]
                send_ref[n * (WIDTH // LANES) + k, 0:32, :] = tile[0:32]
                send_ref[n * (WIDTH // LANES) + k, 40:48, :] = tile[32:40]
            return carry

        lax.fori_loop(0, count * LANES // WIDTH, block, 0)
        out = product(count * LANES // WIDTH)
        for m in range(count // 4):
            tile = out[:, m * LANES : (m + 1) * LANES]
            for q in range(4):
                send_ref[4 * m + q, 32:40, :] = fold(tile[0:32], q)
                send_ref[4 * m + q, 41:42, :] = roll(tile[32:40], -REST * q)[0:1]

    return body


def gram_of(x):
    return lax.dot_general(
        x,
        x,
        (((1,), (1,)), ((), ())),
        precision=lax.Precision.HIGHEST,
        preferred_element_type=F32,
    )


def whole(main, rest):
    return jnp.concatenate([main, unfold([rest])], axis=1)


def scale_body(recv_ref, spread_ref, degree_ref):
    total = jnp.sum(recv_ref[...], axis=0)
    rest = jnp.where(lane_of((1, LANES)) < REST, total[41:42], 0.0)
    rest = jnp.broadcast_to(rest, (8, LANES))
    rest = (rest + roll(rest, REST)) + (roll(rest, 2 * REST) + roll(rest, 3 * REST))
    degree_ref[0:8, :] = jnp.broadcast_to(total[40:41], (8, LANES))
    degree_ref[8:16, :] = rest
    main, rest = total[0:32] / total[40:41], total[32:40] / rest
    gram = fold(widen(gram_of(whole(main, rest))))
    copies(spread_ref, jnp.concatenate([main, rest, gram], axis=0))


def second_body(aff_ref, spread_ref, send_ref, vec_ref):
    count = spread_ref.shape[0]
    gram = jnp.sum(spread_ref[:, 40:48, :], axis=0)

    def put(tile, value):
        first = value.astype(BF16)
        at = tile * LANES
        vec_ref[0:32, at : at + LANES] = first
        vec_ref[32:64, at : at + LANES] = (value - first.astype(F32)).astype(BF16)

    for i in range(count):
        put(i, spread_ref[i, 0:32, :])
    for m in range(count // 4):
        put(count + m, unfold([spread_ref[4 * m + q, 32:40, :] for q in range(4)]))

    def product(n):
        out = jnp.dot(vec_ref[...], aff_ref[n], preferred_element_type=F32)
        return out[0:32] + out[32:64]

    def block(n, carry):
        out = product(n)
        for k in range(WIDTH // LANES):
            send_ref[n * (WIDTH // LANES) + k, 0:32, :] = out[:, k * LANES : (k + 1) * LANES]
            send_ref[n * (WIDTH // LANES) + k, 40:48, :] = gram
        return carry

    lax.fori_loop(0, count * LANES // WIDTH, block, 0)
    out = product(count * LANES // WIDTH)
    for m in range(count // 4):
        for q in range(4):
            send_ref[4 * m + q, 32:40, :] = fold(out[:, m * LANES : (m + 1) * LANES], q)


def solved(gram, right):
    size = gram.shape[0]
    wide = right.shape[1] // LANES
    columns = [
        jnp.broadcast_to(gram[8 * (k // 8) :, k : k + 1], (size - 8 * (k // 8), LANES))
        for k in range(size)
    ]
    rows = [right[8 * g : 8 * g + 8] for g in range(size // 8)]
    for j in range(size):
        base, at = j // 8, j % 8
        pivot = columns[j][at : at + 1]
        scale = lax.rsqrt(pivot)
        scale = scale * (1.5 - 0.5 * pivot * scale * scale)
        factor = columns[j] * scale
        for k in range(j + 1, size):
            skip = 8 * (k // 8 - base)
            mine = factor[k - 8 * base : k - 8 * base + 1]
            columns[k] = columns[k] - factor[skip:] * mine
        top = rows[base][at : at + 1] * jnp.concatenate([scale] * wide, axis=1)
        for g in range(base, size // 8):
            part = factor[8 * (g - base) : 8 * (g - base) + 8]
            if g == base:
                row = row_of((8, LANES))
                part = jnp.where(row > at, part, 0.0)
            new = rows[g] - jnp.concatenate([part] * wide, axis=1) * top
            if g == base:
                new = jnp.where(row_of(new.shape) == at, top, new)
            rows[g] = new
    return jnp.concatenate(rows, axis=0)


def middle_body(points):
    def body(recv_ref, degree_ref, scaled_ref, gram_ref):
        total = jnp.sum(recv_ref[...], axis=0)
        main = total[0:32] / degree_ref[0:1, :]
        rest = total[32:40] / degree_ref[8:16, :]
        scaled = solved(unfold([total[40:48]]) / points, whole(main, rest))
        scaled_ref[...] = scaled
        copies(gram_ref, fold(widen(gram_of(scaled))))

    return body


def again_body(recv_ref, gram_ref):
    copies(gram_ref, jnp.sum(recv_ref[...], axis=0))


def last_body(points):
    def body(recv_ref, scaled_ref, out_ref):
        gram = unfold([jnp.sum(recv_ref[...], axis=0)]) / points
        out_ref[...] = solved(gram, scaled_ref[...])[:, 0 : out_ref.shape[1]]

    return body


def shards(points, start_vectors):
    group, features = points.shape
    row, col = lax.axis_size("row"), lax.axis_size("col")
    total = group * row * col
    log_scale = 2.0 * KERNEL_SCALE / features * math.log2(math.e)
    blocks = col * group // WIDTH
    shape = jax.ShapeDtypeStruct

    def exchange(x, axis):
        return lax.all_to_all(x, axis, 0, 0, tiled=True)

    def call(body, name, out_shape, *args, scratch=()):
        return pl.pallas_call(
            body, out_shape=out_shape, scratch_shapes=scratch, name=name, compiler_params=PARAMS
        )(*args)

    cols, rows = call(
        pack_body,
        "pack",
        (shape((row, 128, LANES), BF16), shape((col, 80, LANES), BF16)),
        points.T,
        start_vectors.T,
    )
    rows = exchange(rows, "col")
    cols = exchange(cols, "row")
    aff, send = call(
        first_body(log_scale),
        "first",
        (pltpu.VMEM((blocks, row * group, WIDTH), BF16), shape((col, 48, LANES), F32)),
        rows,
        cols,
        scratch=(
            pltpu.VMEM((row * group, LANES), BF16),
            pltpu.VMEM((blocks, 256, WIDTH), BF16),
            pltpu.VMEM((48, row * group), BF16),
        ),
    )
    spread, degree = call(
        scale_body,
        "scale",
        (shape((row, 48, LANES), F32), shape((16, LANES), F32)),
        exchange(send, "col"),
    )
    send = call(
        second_body,
        "second",
        shape((col, 48, LANES), F32),
        aff,
        exchange(spread, "row"),
        scratch=(pltpu.VMEM((64, row * group), BF16),),
    )
    scaled, gram = call(
        middle_body(total),
        "middle",
        (shape((32, 2 * LANES), F32), shape((row, 8, LANES), F32)),
        exchange(send, "col"),
        degree,
    )
    gram = call(again_body, "again", shape((col, 8, LANES), F32), exchange(gram, "row"))
    out = call(
        last_body(total), "last", shape((32, group), F32), exchange(gram, "col"), scaled
    )
    return out.T


def solution(mesh):
    spec = P(("row", "col"), None)
    return jax.shard_map(
        shards, mesh=mesh, in_specs=(spec, spec), out_specs=spec, check_vma=False
    )
```

```python
import math

import jax
import jax.numpy as jnp
from jax import lax
from jax.experimental import pallas as pl
from jax.experimental.pallas import tpu as pltpu
from jax.sharding import Mesh
from jax.sharding import PartitionSpec as P

KERNEL_SCALE = 5.12
F32 = jnp.float32
BF16 = jnp.bfloat16
LANES = 128
PARAMS = pltpu.CompilerParams(vmem_limit_bytes=32 * 1024 * 1024)
REST = 32
WIDTH = 512
NORM, ONES, END = 64, 67, 70


def lane_of(shape):
    return lax.broadcasted_iota(jnp.int32, shape, len(shape) - 1)


def row_of(shape):
    return lax.broadcasted_iota(jnp.int32, shape, len(shape) - 2)


def roll(x, shift):
    shift %= LANES
    return pltpu.roll(x, shift, 1) if shift else x


def fold(x, place=0):
    h = x.shape[0] // 4
    group = lane_of((h, LANES)) // REST
    out = jnp.zeros((h, LANES), F32)
    for g in range(4):
        out = jnp.where(group == g, roll(x[g * h : (g + 1) * h], REST * (g - place)), out)
    return out


def unfold(pieces):
    h = pieces[0].shape[0]
    group = lane_of((h, LANES)) // REST
    rows = []
    for g in range(4):
        out = jnp.zeros((h, LANES), F32)
        for q, piece in enumerate(pieces):
            out = jnp.where(group == q, roll(piece, REST * (q - g)), out)
        rows.append(out)
    return jnp.concatenate(rows, axis=0)


def split(x):
    first = x.astype(BF16).astype(F32)
    second = (x - first).astype(BF16).astype(F32)
    return first, second, x - first - second


def widen(x):
    return jnp.concatenate([x, jnp.zeros((x.shape[0], LANES - x.shape[1]), x.dtype)], axis=1)


def main_and_rest(x):
    return x[:, 0:LANES], fold(widen(x[:, LANES : LANES + REST]))


def copies(ref, value):
    for i in range(ref.shape[0]):
        ref[i] = value


def pack_body(points_hbm, vectors_hbm, cols_ref, rows_ref, points_ref, vectors_ref, sems):
    loads = (
        pltpu.make_async_copy(points_hbm, points_ref, sems.at[0]),
        pltpu.make_async_copy(vectors_hbm, vectors_ref, sems.at[1]),
    )
    for load in loads:
        load.start()
    for load in loads:
        load.wait()
    pts = points_ref[...].astype(F32)
    main, rest = main_and_rest(pts)
    copies(rows_ref, jnp.concatenate([main, rest], axis=0).astype(BF16))
    features, group = pts.shape
    half = group // 2
    flat = jnp.concatenate([main, widen(pts[:, LANES:])], axis=1)
    flat = jnp.concatenate([flat, jnp.zeros_like(flat)], axis=0).T
    by_point = flat[0:half] + roll(flat[half:group], features)
    main, rest = main_and_rest(vectors_ref[...].astype(F32))
    parts = [by_point, main, rest, jnp.zeros((8, LANES), F32)]
    copies(cols_ref, jnp.concatenate(parts, axis=0).astype(BF16))


def blocks_of(count):
    lanes = count * LANES
    main = [(at, WIDTH) for at in range(0, lanes, WIDTH)]
    return main, (lanes, lanes // 4)


def put_columns(log_scale, cols_ref, left_ref, vec_ref):
    count = cols_ref.shape[0]
    total = left_ref.shape[0]
    lane = lane_of((80, LANES))
    low = lane < NORM
    for i in range(count):
        raw = cols_ref[i, 0:80].astype(F32)
        squares = raw * raw
        blocks = []
        for side in range(2):
            mine = low if side == 0 else jnp.logical_not(low)
            norm = jnp.sum(jnp.where(mine, squares, 0.0), axis=1, keepdims=True)
            norm = norm * (-0.5 * log_scale)
            block = jnp.where(low, raw if side == 0 else roll(raw, NORM), 0.0)
            for k, piece in enumerate(split(norm)):
                block = jnp.where(lane == NORM + k, piece, block)
            block = jnp.where((lane >= ONES) & (lane < END), 1.0, block)
            blocks.append(block.astype(BF16))
        at = i * LANES
        left_ref[at : at + 80, :] = blocks[0]
        left_ref[at + 80 : at + LANES, :] = blocks[1][0:48]
        at = count * LANES + i * REST
        left_ref[at : at + REST, :] = blocks[1][48:80]
    vec_ref[32:48, :] = jnp.where(row_of((16, total)) == 0, 1.0, 0.0).astype(BF16)
    for i in range(count):
        vec_ref[0:32, i * LANES : (i + 1) * LANES] = cols_ref[i, 80:112]
    for m in range(count // 4):
        rests = [cols_ref[4 * m + q, 112:128].astype(F32)[0:8] for q in range(4)]
        at = (count + m) * LANES
        vec_ref[0:32, at : at + LANES] = unfold(rests).astype(BF16)


def put_rows(log_scale, rows_ref, right_ref):
    count = rows_ref.shape[0]

    def put(tile, raw):
        at = tile * LANES
        scaled = raw * log_scale
        first = scaled.astype(BF16)
        norm = jnp.sum(raw * raw, axis=0, keepdims=True) * (-0.5 * log_scale)
        row = row_of((16, LANES))
        extra = jnp.where(row < ONES - NORM, 1.0, 0.0)
        for i, piece in enumerate(split(norm)):
            extra = jnp.where(row == ONES - NORM + i, piece, extra)
        right_ref[0:64, at : at + LANES] = first
        right_ref[64:80, at : at + LANES] = extra.astype(BF16)
        right_ref[80:128, at : at + LANES] = jnp.zeros((48, LANES), BF16)
        right_ref[128:192, at : at + LANES] = (scaled - first.astype(F32)).astype(BF16)
        right_ref[192:256, at : at + LANES] = jnp.zeros((64, LANES), BF16)

    for i in range(count):
        put(i, rows_ref[i, 0:64].astype(F32))
    for m in range(count // 4):
        put(count + m, unfold([rows_ref[4 * m + q, 64:80].astype(F32) for q in range(4)]))


def affinity_product(left_ref, right_ref, vec_ref, aff_ref, send_ref):
    total = left_ref.shape[0]
    main, rest = blocks_of(send_ref.shape[0])
    chunk = 512

    def product(at, width):
        right = right_ref[:, at : at + width]
        for start in range(0, total, chunk):
            left = left_ref[start : start + chunk, :]
            power = jnp.dot(
                jnp.concatenate([left, left], axis=1), right, preferred_element_type=F32
            )
            aff_ref[start : start + chunk, at : at + width] = jnp.exp2(power).astype(BF16)
        return jnp.dot(
            vec_ref[...], aff_ref[:, at : at + width], preferred_element_type=F32
        )

    for at, width in main:
        out = product(at, width)
        for k in range(width // LANES):
            tile = out[:, k * LANES : (k + 1) * LANES]
            send_ref[at // LANES + k, 0:32, :] = tile[0:32]
            send_ref[at // LANES + k, 40:48, :] = tile[32:40]
    out = product(*rest)
    for m in range(rest[1] // LANES):
        tile = out[:, m * LANES : (m + 1) * LANES]
        for q in range(4):
            send_ref[4 * m + q, 32:40, :] = fold(tile[0:32], q)
            send_ref[4 * m + q, 41:42, :] = roll(tile[32:40], -REST * q)[0:1]


def away_body(log_scale):
    def body(rows_ref, cols_ref, aff_ref, send_ref, left_ref, vec_ref, right_ref):
        put_columns(log_scale, cols_ref, left_ref, vec_ref)
        put_rows(log_scale, rows_ref, right_ref)
        affinity_product(left_ref, right_ref, vec_ref, aff_ref, send_ref)

    return body


def home_body(log_scale):
    def body(rows_ref, left_ref, vec_ref, aff_ref, send_ref, right_ref):
        put_rows(log_scale, rows_ref, right_ref)
        affinity_product(left_ref, right_ref, vec_ref, aff_ref, send_ref)

    return body


def join_body(mine_ref, other_ref, out_ref):
    out_ref[...] = mine_ref[...] + other_ref[...]


def gram_of(x):
    return lax.dot_general(
        x,
        x,
        (((1,), (1,)), ((), ())),
        precision=lax.Precision.HIGHEST,
        preferred_element_type=F32,
    )


def whole(main, rest):
    return jnp.concatenate([main, unfold([rest])], axis=1)


def scale_body(recv_ref, spread_ref, degree_ref):
    total = jnp.sum(recv_ref[...], axis=0)
    rest = jnp.where(lane_of((1, LANES)) < REST, total[41:42], 0.0)
    rest = jnp.broadcast_to(rest, (8, LANES))
    rest = (rest + roll(rest, REST)) + (roll(rest, 2 * REST) + roll(rest, 3 * REST))
    degree_ref[0:8, :] = jnp.broadcast_to(total[40:41], (8, LANES))
    degree_ref[8:16, :] = rest
    main, rest = total[0:32] / total[40:41], total[32:40] / rest
    gram = fold(widen(gram_of(whole(main, rest))))
    copies(spread_ref, jnp.concatenate([main, rest, gram], axis=0))


def put_vectors(spread_ref, vec_ref):
    count = spread_ref.shape[0]

    def put(tile, value):
        first = value.astype(BF16)
        at = tile * LANES
        vec_ref[0:32, at : at + LANES] = first
        vec_ref[32:64, at : at + LANES] = (value - first.astype(F32)).astype(BF16)

    for i in range(count):
        put(i, spread_ref[i, 0:32, :])
    for m in range(count // 4):
        put(count + m, unfold([spread_ref[4 * m + q, 32:40, :] for q in range(4)]))


def second_product(aff_ref, vec_ref, gram, send_ref):
    main, rest = blocks_of(send_ref.shape[0])

    def product(at, width):
        out = jnp.dot(vec_ref[...], aff_ref[:, at : at + width], preferred_element_type=F32)
        return out[0:32] + out[32:64]

    for at, width in main:
        out = product(at, width)
        for k in range(width // LANES):
            send_ref[at // LANES + k, 0:32, :] = out[:, k * LANES : (k + 1) * LANES]
            send_ref[at // LANES + k, 40:48, :] = gram
    out = product(*rest)
    for m in range(rest[1] // LANES):
        for q in range(4):
            send_ref[4 * m + q, 32:40, :] = fold(out[:, m * LANES : (m + 1) * LANES], q)


def away_again_body(aff_ref, spread_ref, send_ref, vec_ref, gram_ref):
    gram = jnp.sum(spread_ref[:, 40:48, :], axis=0)
    gram_ref[...] = gram
    put_vectors(spread_ref, vec_ref)
    second_product(aff_ref, vec_ref, gram, send_ref)


def home_again_body(aff_ref, vec_ref, gram_ref, send_ref):
    second_product(aff_ref, vec_ref, gram_ref[...], send_ref)


def solved(gram, right):
    size = gram.shape[0]
    wide = right.shape[1] // LANES
    columns = [
        jnp.broadcast_to(gram[8 * (k // 8) :, k : k + 1], (size - 8 * (k // 8), LANES))
        for k in range(size)
    ]
    rows = [right[8 * g : 8 * g + 8] for g in range(size // 8)]
    for j in range(size):
        base, at = j // 8, j % 8
        pivot = columns[j][at : at + 1]
        scale = lax.rsqrt(pivot)
        scale = scale * (1.5 - 0.5 * pivot * scale * scale)
        factor = columns[j] * scale
        for k in range(j + 1, size):
            skip = 8 * (k // 8 - base)
            mine = factor[k - 8 * base : k - 8 * base + 1]
            columns[k] = columns[k] - factor[skip:] * mine
        top = rows[base][at : at + 1] * jnp.concatenate([scale] * wide, axis=1)
        for g in range(base, size // 8):
            part = factor[8 * (g - base) : 8 * (g - base) + 8]
            if g == base:
                row = row_of((8, LANES))
                part = jnp.where(row > at, part, 0.0)
            new = rows[g] - jnp.concatenate([part] * wide, axis=1) * top
            if g == base:
                new = jnp.where(row_of(new.shape) == at, top, new)
            rows[g] = new
    return jnp.concatenate(rows, axis=0)


def middle_body(points):
    def body(recv_ref, degree_ref, scaled_ref, gram_ref):
        total = jnp.sum(recv_ref[...], axis=0)
        main = total[0:32] / degree_ref[0:1, :]
        rest = total[32:40] / degree_ref[8:16, :]
        scaled = solved(unfold([total[40:48]]) / points, whole(main, rest))
        scaled_ref[...] = scaled
        copies(gram_ref, fold(widen(gram_of(scaled))))

    return body


def again_body(recv_ref, gram_ref):
    copies(gram_ref, jnp.sum(recv_ref[...], axis=0))


def last_body(points):
    def body(recv_ref, scaled_ref, out_ref):
        gram = unfold([jnp.sum(recv_ref[...], axis=0)]) / points
        out_ref[...] = solved(gram, scaled_ref[...])[:, 0 : out_ref.shape[1]]

    return body


def shards(points, start_vectors):
    group, features = points.shape
    row, half, cores = lax.axis_size("row"), lax.axis_size("z"), lax.axis_size("core")
    col = half * cores
    total = group * row * col
    log_scale = 2.0 * KERNEL_SCALE / features * math.log2(math.e)
    lanes = half * group
    shape = jax.ShapeDtypeStruct

    def exchange(x, axis):
        return lax.all_to_all(x, axis, 0, 0, tiled=True)

    def swap(x):
        return lax.ppermute(x, "core", [(0, 1), (1, 0)])

    def call(body, name, out_shape, *args, scratch=(), **kwargs):
        return pl.pallas_call(
            body,
            out_shape=out_shape,
            scratch_shapes=scratch,
            name=name,
            compiler_params=PARAMS,
            **kwargs,
        )(*args)

    hbm_space = pl.BlockSpec(memory_space=pltpu.HBM)
    cols, rows = call(
        pack_body,
        "pack",
        (shape((row, 128, LANES), BF16), shape((half, 80, LANES), BF16)),
        points.T,
        start_vectors.T,
        scratch=(
            pltpu.VMEM((features, group), BF16),
            pltpu.VMEM((start_vectors.shape[1], group), BF16),
            pltpu.SemaphoreType.DMA((2,)),
        ),
        in_specs=[hbm_space, hbm_space],
    )
    home_rows = exchange(rows, "z")
    away_rows = swap(home_rows)
    cols = exchange(cols, "row")
    aff_shape = pltpu.VMEM((row * group, lanes), BF16)
    send_shape = shape((half, 48, LANES), F32)
    right_shape = pltpu.VMEM((256, lanes), BF16)
    away_aff, away_send, left, vec = call(
        away_body(log_scale),
        "away",
        (
            aff_shape,
            send_shape,
            pltpu.VMEM((row * group, LANES), BF16),
            pltpu.VMEM((48, row * group), BF16),
        ),
        away_rows,
        cols,
        scratch=(right_shape,),
    )
    other = swap(away_send)
    home_aff, home_send = call(
        home_body(log_scale),
        "home",
        (aff_shape, send_shape),
        home_rows,
        left,
        vec,
        scratch=(right_shape,),
    )
    send = call(join_body, "join", send_shape, home_send, other)
    spread, degree = call(
        scale_body,
        "scale",
        (shape((row, 48, LANES), F32), shape((16, LANES), F32)),
        exchange(send, "z"),
    )
    away_send, vec, gram = call(
        away_again_body,
        "away_again",
        (send_shape, pltpu.VMEM((64, row * group), BF16), pltpu.VMEM((8, LANES), F32)),
        away_aff,
        exchange(spread, "row"),
    )
    other = swap(away_send)
    home_send = call(home_again_body, "home_again", send_shape, home_aff, vec, gram)
    send = call(join_body, "join_again", send_shape, home_send, other)
    scaled, gram = call(
        middle_body(total),
        "middle",
        (shape((32, 2 * LANES), F32), shape((row, 8, LANES), F32)),
        exchange(send, "z"),
        degree,
    )
    gram = call(again_body, "again", shape((col, 8, LANES), F32), exchange(gram, "row"))
    out = call(
        last_body(total),
        "last",
        shape((32, group), F32),
        exchange(gram, ("z", "core")),
        scaled,
    )
    return out.T


def solution(mesh):
    rows, cols = mesh.devices.shape
    finer = Mesh(mesh.devices.reshape(rows, cols // 2, 2), ("row", "z", "core"))
    spec = P(("row", "z", "core"), None)
    return jax.shard_map(
        shards, mesh=finer, in_specs=(spec, spec), out_specs=spec, check_vma=False
    )
```

```python
import math

import jax
import jax.numpy as jnp
from jax import lax
from jax.experimental import pallas as pl
from jax.experimental.pallas import tpu as pltpu
from jax.sharding import Mesh
from jax.sharding import PartitionSpec as P

KERNEL_SCALE = 5.12
F32 = jnp.float32
BF16 = jnp.bfloat16
LANES = 128
PARAMS = pltpu.CompilerParams(vmem_limit_bytes=32 * 1024 * 1024)
REST = 32
WIDTH = 512
NORM, ONES, END = 64, 67, 70


def lane_of(shape):
    return lax.broadcasted_iota(jnp.int32, shape, len(shape) - 1)


def row_of(shape):
    return lax.broadcasted_iota(jnp.int32, shape, len(shape) - 2)


def roll(x, shift):
    shift %= LANES
    return pltpu.roll(x, shift, 1) if shift else x


def fold(x, place=0):
    h = x.shape[0] // 4
    group = lane_of((h, LANES)) // REST
    out = jnp.zeros((h, LANES), F32)
    for g in range(4):
        out = jnp.where(group == g, roll(x[g * h : (g + 1) * h], REST * (g - place)), out)
    return out


def unfold(pieces):
    h = pieces[0].shape[0]
    group = lane_of((h, LANES)) // REST
    rows = []
    for g in range(4):
        out = jnp.zeros((h, LANES), F32)
        for q, piece in enumerate(pieces):
            out = jnp.where(group == q, roll(piece, REST * (q - g)), out)
        rows.append(out)
    return jnp.concatenate(rows, axis=0)


def split(x):
    first = x.astype(BF16).astype(F32)
    second = (x - first).astype(BF16).astype(F32)
    return first, second, x - first - second


def widen(x):
    return jnp.concatenate([x, jnp.zeros((x.shape[0], LANES - x.shape[1]), x.dtype)], axis=1)


def main_and_rest(x):
    return x[:, 0:LANES], fold(widen(x[:, LANES : LANES + REST]))


def copies(ref, value):
    for i in range(ref.shape[0]):
        ref[i] = value


def pack_body(points_hbm, vectors_hbm, cols_ref, rows_ref, points_ref, vectors_ref, sems):
    loads = (
        pltpu.make_async_copy(points_hbm, points_ref, sems.at[0]),
        pltpu.make_async_copy(vectors_hbm, vectors_ref, sems.at[1]),
    )
    for load in loads:
        load.start()
    for load in loads:
        load.wait()
    pts = points_ref[...].astype(F32)
    main, rest = main_and_rest(pts)
    copies(rows_ref, jnp.concatenate([main, rest], axis=0).astype(BF16))
    features, group = pts.shape
    half = group // 2
    flat = jnp.concatenate([main, widen(pts[:, LANES:])], axis=1)
    flat = jnp.concatenate([flat, jnp.zeros_like(flat)], axis=0).T
    by_point = flat[0:half] + roll(flat[half:group], features)
    main, rest = main_and_rest(vectors_ref[...].astype(F32))
    copies(cols_ref, jnp.concatenate([by_point, main, rest], axis=0).astype(BF16))


def blocks_of(count):
    lanes = count * LANES
    main = [(at, WIDTH) for at in range(0, lanes, WIDTH)]
    return main, (lanes, lanes // 4)


def put_columns(log_scale, cols_ref, left_ref, vec_ref):
    count = cols_ref.shape[0]
    total = left_ref.shape[0]
    lane = lane_of((80, LANES))
    low = lane < NORM
    for i in range(count):
        raw = cols_ref[i, 0:80].astype(F32)
        squares = raw * raw
        blocks = []
        for side in range(2):
            mine = low if side == 0 else jnp.logical_not(low)
            norm = jnp.sum(jnp.where(mine, squares, 0.0), axis=1, keepdims=True)
            norm = norm * (-0.5 * log_scale)
            block = jnp.where(low, raw if side == 0 else roll(raw, NORM), 0.0)
            for k, piece in enumerate(split(norm)):
                block = jnp.where(lane == NORM + k, piece, block)
            block = jnp.where((lane >= ONES) & (lane < END), 1.0, block)
            blocks.append(block.astype(BF16))
        at = i * LANES
        left_ref[at : at + 80, :] = blocks[0]
        left_ref[at + 80 : at + LANES, :] = blocks[1][0:48]
        at = count * LANES + i * REST
        left_ref[at : at + REST, :] = blocks[1][48:80]
    vec_ref[32:48, :] = jnp.where(row_of((16, total)) == 0, 1.0, 0.0).astype(BF16)
    for i in range(count):
        vec_ref[0:32, i * LANES : (i + 1) * LANES] = cols_ref[i, 80:112]
    for m in range(count // 4):
        rests = [cols_ref[4 * m + q, 112:120].astype(F32) for q in range(4)]
        at = (count + m) * LANES
        vec_ref[0:32, at : at + LANES] = unfold(rests).astype(BF16)


def put_rows(log_scale, rows_ref, right_ref):
    count = rows_ref.shape[0]

    def put(tile, raw):
        at = tile * LANES
        scaled = raw * log_scale
        first = scaled.astype(BF16)
        norm = jnp.sum(raw * raw, axis=0, keepdims=True) * (-0.5 * log_scale)
        row = row_of((16, LANES))
        extra = jnp.where(row < ONES - NORM, 1.0, 0.0)
        for i, piece in enumerate(split(norm)):
            extra = jnp.where(row == ONES - NORM + i, piece, extra)
        right_ref[0:64, at : at + LANES] = first
        right_ref[64:80, at : at + LANES] = extra.astype(BF16)
        right_ref[80:128, at : at + LANES] = jnp.zeros((48, LANES), BF16)
        right_ref[128:192, at : at + LANES] = (scaled - first.astype(F32)).astype(BF16)
        right_ref[192:256, at : at + LANES] = jnp.zeros((64, LANES), BF16)

    for i in range(count):
        put(i, rows_ref[i, 0:64].astype(F32))
    for m in range(count // 4):
        put(count + m, unfold([rows_ref[4 * m + q, 64:80].astype(F32) for q in range(4)]))


def affinity_product(left_ref, right_ref, vec_ref, aff_ref, send_ref):
    total = left_ref.shape[0]
    main, rest = blocks_of(send_ref.shape[0])
    chunk = 512

    def product(at, width):
        right = right_ref[:, at : at + width]
        for start in range(0, total, chunk):
            left = left_ref[start : start + chunk, :]
            power = jnp.dot(
                jnp.concatenate([left, left], axis=1), right, preferred_element_type=F32
            )
            aff_ref[start : start + chunk, at : at + width] = jnp.exp2(power).astype(BF16)
        return jnp.dot(
            vec_ref[...], aff_ref[:, at : at + width], preferred_element_type=F32
        )

    for at, width in main:
        out = product(at, width)
        for k in range(width // LANES):
            tile = out[:, k * LANES : (k + 1) * LANES]
            send_ref[at // LANES + k, 0:32, :] = tile[0:32]
            send_ref[at // LANES + k, 40:48, :] = tile[32:40]
    out = product(*rest)
    for m in range(rest[1] // LANES):
        tile = out[:, m * LANES : (m + 1) * LANES]
        for q in range(4):
            send_ref[4 * m + q, 32:40, :] = fold(tile[0:32], q)
            send_ref[4 * m + q, 41:42, :] = roll(tile[32:40], -REST * q)[0:1]


def away_body(log_scale):
    def body(right_ref, cols_ref, aff_ref, send_ref, left_ref, vec_ref):
        put_columns(log_scale, cols_ref, left_ref, vec_ref)
        affinity_product(left_ref, right_ref, vec_ref, aff_ref, send_ref)

    return body


def rows_body(log_scale):
    def body(away_ref, home_ref, away_right_ref, home_right_ref):
        put_rows(log_scale, away_ref, away_right_ref)
        put_rows(log_scale, home_ref, home_right_ref)

    return body


def join_body(mine_ref, other_ref, out_ref):
    out_ref[...] = mine_ref[...] + other_ref[...]


def gram_of(x):
    return lax.dot_general(
        x,
        x,
        (((1,), (1,)), ((), ())),
        precision=lax.Precision.HIGHEST,
        preferred_element_type=F32,
    )


def whole(main, rest):
    return jnp.concatenate([main, unfold([rest])], axis=1)


def scale_body(recv_ref, spread_ref, degree_ref):
    total = jnp.sum(recv_ref[...], axis=0)
    rest = jnp.where(lane_of((1, LANES)) < REST, total[41:42], 0.0)
    rest = jnp.broadcast_to(rest, (8, LANES))
    rest = (rest + roll(rest, REST)) + (roll(rest, 2 * REST) + roll(rest, 3 * REST))
    degree_ref[0:8, :] = jnp.broadcast_to(total[40:41], (8, LANES))
    degree_ref[8:16, :] = rest
    main, rest = total[0:32] / total[40:41], total[32:40] / rest
    gram = fold(widen(gram_of(whole(main, rest))))
    copies(spread_ref, jnp.concatenate([main, rest, gram], axis=0))


def put_vectors(spread_ref, vec_ref):
    count = spread_ref.shape[0]

    def put(tile, value):
        first = value.astype(BF16)
        at = tile * LANES
        vec_ref[0:32, at : at + LANES] = first
        vec_ref[32:64, at : at + LANES] = (value - first.astype(F32)).astype(BF16)

    for i in range(count):
        put(i, spread_ref[i, 0:32, :])
    for m in range(count // 4):
        put(count + m, unfold([spread_ref[4 * m + q, 32:40, :] for q in range(4)]))


def second_product(aff_ref, vec_ref, gram, send_ref):
    main, rest = blocks_of(send_ref.shape[0])

    def product(at, width):
        out = jnp.dot(vec_ref[...], aff_ref[:, at : at + width], preferred_element_type=F32)
        return out[0:32] + out[32:64]

    for at, width in main:
        out = product(at, width)
        for k in range(width // LANES):
            send_ref[at // LANES + k, 0:32, :] = out[:, k * LANES : (k + 1) * LANES]
            send_ref[at // LANES + k, 40:48, :] = gram
    out = product(*rest)
    for m in range(rest[1] // LANES):
        for q in range(4):
            send_ref[4 * m + q, 32:40, :] = fold(out[:, m * LANES : (m + 1) * LANES], q)


def away_again_body(aff_ref, spread_ref, send_ref, vec_ref, gram_ref):
    gram = jnp.sum(spread_ref[:, 40:48, :], axis=0)
    gram_ref[...] = gram
    put_vectors(spread_ref, vec_ref)
    second_product(aff_ref, vec_ref, gram, send_ref)


def home_again_body(aff_ref, vec_ref, gram_ref, send_ref):
    second_product(aff_ref, vec_ref, gram_ref[...], send_ref)


def solved(gram, right):
    size = gram.shape[0]
    wide = right.shape[1] // LANES
    columns = [
        jnp.broadcast_to(gram[8 * (k // 8) :, k : k + 1], (size - 8 * (k // 8), LANES))
        for k in range(size)
    ]
    rows = [right[8 * g : 8 * g + 8] for g in range(size // 8)]
    for j in range(size):
        base, at = j // 8, j % 8
        pivot = columns[j][at : at + 1]
        scale = lax.rsqrt(pivot)
        scale = scale * (1.5 - 0.5 * pivot * scale * scale)
        factor = columns[j] * scale
        for k in range(j + 1, size):
            skip = 8 * (k // 8 - base)
            mine = factor[k - 8 * base : k - 8 * base + 1]
            columns[k] = columns[k] - factor[skip:] * mine
        top = rows[base][at : at + 1] * jnp.concatenate([scale] * wide, axis=1)
        for g in range(base, size // 8):
            part = factor[8 * (g - base) : 8 * (g - base) + 8]
            if g == base:
                row = row_of((8, LANES))
                part = jnp.where(row > at, part, 0.0)
            new = rows[g] - jnp.concatenate([part] * wide, axis=1) * top
            if g == base:
                new = jnp.where(row_of(new.shape) == at, top, new)
            rows[g] = new
    return jnp.concatenate(rows, axis=0)


def middle_body(points):
    def body(recv_ref, degree_ref, scaled_ref, gram_ref):
        total = jnp.sum(recv_ref[...], axis=0)
        main = total[0:32] / degree_ref[0:1, :]
        rest = total[32:40] / degree_ref[8:16, :]
        scaled = solved(unfold([total[40:48]]) / points, whole(main, rest))
        scaled_ref[...] = scaled
        copies(gram_ref, fold(widen(gram_of(scaled))))

    return body


def again_body(recv_ref, gram_ref):
    copies(gram_ref, jnp.sum(recv_ref[...], axis=0))


def last_body(points):
    def body(recv_ref, scaled_ref, out_ref):
        gram = unfold([jnp.sum(recv_ref[...], axis=0)]) / points
        out_ref[...] = solved(gram, scaled_ref[...])[:, 0 : out_ref.shape[1]]

    return body


def shards(points, start_vectors):
    group, features = points.shape
    row, half, cores = lax.axis_size("row"), lax.axis_size("z"), lax.axis_size("core")
    col = half * cores
    total = group * row * col
    log_scale = 2.0 * KERNEL_SCALE / features * math.log2(math.e)
    lanes = half * group
    right_shape = pltpu.VMEM((256, lanes), BF16)
    shape = jax.ShapeDtypeStruct

    def exchange(x, axis):
        return lax.all_to_all(x, axis, 0, 0, tiled=True)

    def swap(x):
        return lax.ppermute(x, "core", [(0, 1), (1, 0)])

    def call(body, name, out_shape, *args, scratch=(), **kwargs):
        return pl.pallas_call(
            body,
            out_shape=out_shape,
            scratch_shapes=scratch,
            name=name,
            compiler_params=PARAMS,
            **kwargs,
        )(*args)

    hbm_space = pl.BlockSpec(memory_space=pltpu.HBM)
    cols, rows = call(
        pack_body,
        "pack",
        (pltpu.VMEM((row, 120, LANES), BF16), pltpu.VMEM((half, 80, LANES), BF16)),
        pltpu.with_memory_space_constraint(points.T, pltpu.HBM),
        pltpu.with_memory_space_constraint(start_vectors.T, pltpu.HBM),
        scratch=(
            pltpu.VMEM((features, group), BF16),
            pltpu.VMEM((start_vectors.shape[1], group), BF16),
            pltpu.SemaphoreType.DMA((2,)),
        ),
        in_specs=[hbm_space, hbm_space],
    )
    home_rows = exchange(rows, "z")
    away_rows = swap(home_rows)
    cols = exchange(cols, "row")
    away_right, home_right = call(
        rows_body(log_scale), "rows", (right_shape, right_shape), away_rows, home_rows
    )
    aff_shape = pltpu.VMEM((row * group, lanes), BF16)
    send_shape = shape((half, 48, LANES), F32)
    away_aff, away_send, left, vec = call(
        away_body(log_scale),
        "away",
        (
            aff_shape,
            send_shape,
            pltpu.VMEM((row * group, LANES), BF16),
            pltpu.VMEM((48, row * group), BF16),
        ),
        away_right,
        cols,
    )
    other = swap(away_send)
    home_aff, home_send = call(
        affinity_product,
        "home",
        (aff_shape, send_shape),
        left,
        home_right,
        vec,
    )
    send = call(join_body, "join", send_shape, home_send, other)
    spread, degree = call(
        scale_body,
        "scale",
        (shape((row, 48, LANES), F32), shape((16, LANES), F32)),
        exchange(send, "z"),
    )
    away_send, vec, gram = call(
        away_again_body,
        "away_again",
        (send_shape, pltpu.VMEM((64, row * group), BF16), pltpu.VMEM((8, LANES), F32)),
        away_aff,
        exchange(spread, "row"),
    )
    other = swap(away_send)
    home_send = call(home_again_body, "home_again", send_shape, home_aff, vec, gram)
    send = call(join_body, "join_again", send_shape, home_send, other)
    scaled, gram = call(
        middle_body(total),
        "middle",
        (shape((32, 2 * LANES), F32), shape((row, 8, LANES), F32)),
        exchange(send, "z"),
        degree,
    )
    gram = call(again_body, "again", shape((col, 8, LANES), F32), exchange(gram, "row"))
    out = call(
        last_body(total),
        "last",
        shape((32, group), F32),
        exchange(gram, ("z", "core")),
        scaled,
    )
    return out.T


def solution(mesh):
    rows, cols = mesh.devices.shape
    finer = Mesh(mesh.devices.reshape(rows, cols // 2, 2), ("row", "z", "core"))
    spec = P(("row", "z", "core"), None)
    return jax.shard_map(
        shards, mesh=finer, in_specs=(spec, spec), out_specs=spec, check_vma=False
    )
```

```python
import math

import jax
import jax.numpy as jnp
from jax import lax
from jax.experimental import pallas as pl
from jax.experimental.pallas import tpu as pltpu
from jax.sharding import Mesh
from jax.sharding import PartitionSpec as P

KERNEL_SCALE = 5.12
F32 = jnp.float32
BF16 = jnp.bfloat16
LANES = 128
PARAMS = pltpu.CompilerParams(vmem_limit_bytes=32 * 1024 * 1024)
REST = 32
WIDTH = 512
NORM, ONES, END = 64, 67, 70


def lane_of(shape):
    return lax.broadcasted_iota(jnp.int32, shape, len(shape) - 1)


def row_of(shape):
    return lax.broadcasted_iota(jnp.int32, shape, len(shape) - 2)


def roll(x, shift):
    shift %= LANES
    return pltpu.roll(x, shift, 1) if shift else x


def fold(x, place=0):
    h = x.shape[0] // 4
    group = lane_of((h, LANES)) // REST
    out = jnp.zeros((h, LANES), F32)
    for g in range(4):
        out = jnp.where(group == g, roll(x[g * h : (g + 1) * h], REST * (g - place)), out)
    return out


def unfold(pieces):
    h = pieces[0].shape[0]
    group = lane_of((h, LANES)) // REST
    rows = []
    for g in range(4):
        out = jnp.zeros((h, LANES), F32)
        for q, piece in enumerate(pieces):
            out = jnp.where(group == q, roll(piece, REST * (q - g)), out)
        rows.append(out)
    return jnp.concatenate(rows, axis=0)


def split(x):
    first = x.astype(BF16).astype(F32)
    second = (x - first).astype(BF16).astype(F32)
    return first, second, x - first - second


def widen(x):
    return jnp.concatenate([x, jnp.zeros((x.shape[0], LANES - x.shape[1]), x.dtype)], axis=1)


def main_and_rest(x):
    return x[:, 0:LANES], fold(widen(x[:, LANES : LANES + REST]))


def copies(ref, value):
    for i in range(ref.shape[0]):
        ref[i] = value


def pack_body(points_hbm, vectors_hbm, cols_ref, rows_ref, points_ref, vectors_ref, sems):
    loads = (
        pltpu.make_async_copy(points_hbm, points_ref, sems.at[0]),
        pltpu.make_async_copy(vectors_hbm, vectors_ref, sems.at[1]),
    )
    for load in loads:
        load.start()
    for load in loads:
        load.wait()
    pts = points_ref[...].astype(F32)
    main, rest = main_and_rest(pts)
    rows_ref[...] = jnp.concatenate([main, rest], axis=0).astype(BF16)
    features, group = pts.shape
    half = group // 2
    flat = jnp.concatenate([main, widen(pts[:, LANES:])], axis=1)
    flat = jnp.concatenate([flat, jnp.zeros_like(flat)], axis=0).T
    by_point = flat[0:half] + roll(flat[half:group], features)
    main, rest = main_and_rest(vectors_ref[...].astype(F32))
    copies(cols_ref, jnp.concatenate([by_point, main, rest], axis=0).astype(BF16))


def blocks_of(count):
    lanes = count * LANES
    main = [(at, WIDTH) for at in range(0, lanes, WIDTH)]
    return main, (lanes, lanes // 4)


def put_columns(log_scale, cols_ref, left_ref, vec_ref):
    count = cols_ref.shape[0]
    total = left_ref.shape[0]
    lane = lane_of((80, LANES))
    low = lane < NORM
    for i in range(count):
        raw = cols_ref[i, 0:80].astype(F32)
        squares = raw * raw
        blocks = []
        for side in range(2):
            mine = low if side == 0 else jnp.logical_not(low)
            norm = jnp.sum(jnp.where(mine, squares, 0.0), axis=1, keepdims=True)
            norm = norm * (-0.5 * log_scale)
            block = jnp.where(low, raw if side == 0 else roll(raw, NORM), 0.0)
            for k, piece in enumerate(split(norm)):
                block = jnp.where(lane == NORM + k, piece, block)
            block = jnp.where((lane >= ONES) & (lane < END), 1.0, block)
            blocks.append(block.astype(BF16))
        at = i * LANES
        left_ref[at : at + 80, :] = blocks[0]
        left_ref[at + 80 : at + LANES, :] = blocks[1][0:48]
        at = count * LANES + i * REST
        left_ref[at : at + REST, :] = blocks[1][48:80]
    vec_ref[32:48, :] = jnp.where(row_of((16, total)) == 0, 1.0, 0.0).astype(BF16)
    for i in range(count):
        vec_ref[0:32, i * LANES : (i + 1) * LANES] = cols_ref[i, 80:112]
    for m in range(count // 4):
        rests = [cols_ref[4 * m + q, 112:120].astype(F32) for q in range(4)]
        at = (count + m) * LANES
        vec_ref[0:32, at : at + LANES] = unfold(rests).astype(BF16)


def put_rows(log_scale, rows_ref, right_ref):
    count = rows_ref.shape[0]

    def put(tile, raw):
        at = tile * LANES
        scaled = raw * log_scale
        first = scaled.astype(BF16)
        norm = jnp.sum(raw * raw, axis=0, keepdims=True) * (-0.5 * log_scale)
        row = row_of((16, LANES))
        extra = jnp.where(row < ONES - NORM, 1.0, 0.0)
        for i, piece in enumerate(split(norm)):
            extra = jnp.where(row == ONES - NORM + i, piece, extra)
        right_ref[0:64, at : at + LANES] = first
        right_ref[64:80, at : at + LANES] = extra.astype(BF16)
        right_ref[80:128, at : at + LANES] = jnp.zeros((48, LANES), BF16)
        right_ref[128:192, at : at + LANES] = (scaled - first.astype(F32)).astype(BF16)
        right_ref[192:256, at : at + LANES] = jnp.zeros((64, LANES), BF16)

    for i in range(count):
        put(i, rows_ref[i, 0:64].astype(F32))
    for m in range(count // 4):
        put(count + m, unfold([rows_ref[4 * m + q, 64:80].astype(F32) for q in range(4)]))


def affinity_product(left_ref, right_ref, vec_ref, aff_ref, send_ref):
    total = left_ref.shape[0]
    main, rest = blocks_of(send_ref.shape[0])
    chunk = 512

    def product(at, width):
        right = right_ref[:, at : at + width]
        for start in range(0, total, chunk):
            left = left_ref[start : start + chunk, :]
            power = jnp.dot(
                jnp.concatenate([left, left], axis=1), right, preferred_element_type=F32
            )
            aff_ref[start : start + chunk, at : at + width] = jnp.exp2(power).astype(BF16)
        return jnp.dot(
            vec_ref[...], aff_ref[:, at : at + width], preferred_element_type=F32
        )

    for at, width in main:
        out = product(at, width)
        for k in range(width // LANES):
            tile = out[:, k * LANES : (k + 1) * LANES]
            send_ref[at // LANES + k, 0:32, :] = tile[0:32]
            send_ref[at // LANES + k, 40:48, :] = tile[32:40]
    out = product(*rest)
    for m in range(rest[1] // LANES):
        tile = out[:, m * LANES : (m + 1) * LANES]
        for q in range(4):
            send_ref[4 * m + q, 32:40, :] = fold(tile[0:32], q)
            send_ref[4 * m + q, 41:42, :] = roll(tile[32:40], -REST * q)[0:1]


def away_body(log_scale):
    def body(right_ref, cols_ref, aff_ref, send_ref, left_ref, vec_ref):
        put_columns(log_scale, cols_ref, left_ref, vec_ref)
        affinity_product(left_ref, right_ref, vec_ref, aff_ref, send_ref)

    return body


def rows_body(log_scale):
    def body(away_ref, home_ref, away_right_ref, home_right_ref):
        put_rows(log_scale, away_ref, away_right_ref)
        put_rows(log_scale, home_ref, home_right_ref)

    return body


def order_body(*refs):
    out_ref = refs[-1]
    count = len(refs) - 1
    here = lax.axis_index("z")
    for t in range(count):
        out_ref[lax.rem(here + count - t, count)] = refs[t][...]


def join_body(mine_ref, other_ref, out_ref):
    out_ref[...] = mine_ref[...] + other_ref[...]


def gram_of(x):
    return lax.dot_general(
        x,
        x,
        (((1,), (1,)), ((), ())),
        precision=lax.Precision.HIGHEST,
        preferred_element_type=F32,
    )


def whole(main, rest):
    return jnp.concatenate([main, unfold([rest])], axis=1)


def scale_body(recv_ref, spread_ref, degree_ref):
    total = jnp.sum(recv_ref[...], axis=0)
    rest = jnp.where(lane_of((1, LANES)) < REST, total[41:42], 0.0)
    rest = jnp.broadcast_to(rest, (8, LANES))
    rest = (rest + roll(rest, REST)) + (roll(rest, 2 * REST) + roll(rest, 3 * REST))
    degree_ref[0:8, :] = jnp.broadcast_to(total[40:41], (8, LANES))
    degree_ref[8:16, :] = rest
    main, rest = total[0:32] / total[40:41], total[32:40] / rest
    gram = fold(widen(gram_of(whole(main, rest))))
    copies(spread_ref, jnp.concatenate([main, rest, gram], axis=0))


def put_vectors(spread_ref, vec_ref):
    count = spread_ref.shape[0]

    def put(tile, value):
        first = value.astype(BF16)
        at = tile * LANES
        vec_ref[0:32, at : at + LANES] = first
        vec_ref[32:64, at : at + LANES] = (value - first.astype(F32)).astype(BF16)

    for i in range(count):
        put(i, spread_ref[i, 0:32, :])
    for m in range(count // 4):
        put(count + m, unfold([spread_ref[4 * m + q, 32:40, :] for q in range(4)]))


def second_product(aff_ref, vec_ref, gram, send_ref):
    main, rest = blocks_of(send_ref.shape[0])

    def product(at, width):
        out = jnp.dot(vec_ref[...], aff_ref[:, at : at + width], preferred_element_type=F32)
        return out[0:32] + out[32:64]

    for at, width in main:
        out = product(at, width)
        for k in range(width // LANES):
            send_ref[at // LANES + k, 0:32, :] = out[:, k * LANES : (k + 1) * LANES]
            send_ref[at // LANES + k, 40:48, :] = gram
    out = product(*rest)
    for m in range(rest[1] // LANES):
        for q in range(4):
            send_ref[4 * m + q, 32:40, :] = fold(out[:, m * LANES : (m + 1) * LANES], q)


def away_again_body(aff_ref, spread_ref, send_ref, vec_ref, gram_ref):
    gram = jnp.sum(spread_ref[:, 40:48, :], axis=0)
    gram_ref[...] = gram
    put_vectors(spread_ref, vec_ref)
    second_product(aff_ref, vec_ref, gram, send_ref)


def home_again_body(aff_ref, vec_ref, gram_ref, send_ref):
    second_product(aff_ref, vec_ref, gram_ref[...], send_ref)


def solved(gram, right):
    size = gram.shape[0]
    wide = right.shape[1] // LANES
    columns = [
        jnp.broadcast_to(gram[8 * (k // 8) :, k : k + 1], (size - 8 * (k // 8), LANES))
        for k in range(size)
    ]
    rows = [right[8 * g : 8 * g + 8] for g in range(size // 8)]
    for j in range(size):
        base, at = j // 8, j % 8
        pivot = columns[j][at : at + 1]
        scale = lax.rsqrt(pivot)
        scale = scale * (1.5 - 0.5 * pivot * scale * scale)
        factor = columns[j] * scale
        for k in range(j + 1, size):
            skip = 8 * (k // 8 - base)
            mine = factor[k - 8 * base : k - 8 * base + 1]
            columns[k] = columns[k] - factor[skip:] * mine
        top = rows[base][at : at + 1] * jnp.concatenate([scale] * wide, axis=1)
        for g in range(base, size // 8):
            part = factor[8 * (g - base) : 8 * (g - base) + 8]
            if g == base:
                row = row_of((8, LANES))
                part = jnp.where(row > at, part, 0.0)
            new = rows[g] - jnp.concatenate([part] * wide, axis=1) * top
            if g == base:
                new = jnp.where(row_of(new.shape) == at, top, new)
            rows[g] = new
    return jnp.concatenate(rows, axis=0)


def middle_body(points):
    def body(recv_ref, degree_ref, scaled_ref, gram_ref):
        total = jnp.sum(recv_ref[...], axis=0)
        main = total[0:32] / degree_ref[0:1, :]
        rest = total[32:40] / degree_ref[8:16, :]
        scaled = solved(unfold([total[40:48]]) / points, whole(main, rest))
        scaled_ref[...] = scaled
        copies(gram_ref, fold(widen(gram_of(scaled))))

    return body


def again_body(recv_ref, gram_ref):
    copies(gram_ref, jnp.sum(recv_ref[...], axis=0))


def last_body(points):
    def body(recv_ref, scaled_ref, out_ref):
        gram = unfold([jnp.sum(recv_ref[...], axis=0)]) / points
        out_ref[...] = solved(gram, scaled_ref[...])[:, 0 : out_ref.shape[1]]

    return body


def shards(points, start_vectors):
    group, features = points.shape
    row, half, cores = lax.axis_size("row"), lax.axis_size("z"), lax.axis_size("core")
    col = half * cores
    total = group * row * col
    log_scale = 2.0 * KERNEL_SCALE / features * math.log2(math.e)
    lanes = half * group
    right_shape = pltpu.VMEM((256, lanes), BF16)
    shape = jax.ShapeDtypeStruct

    def exchange(x, axis):
        return lax.all_to_all(x, axis, 0, 0, tiled=True)

    def swap(x):
        return lax.ppermute(x, "core", [(0, 1), (1, 0)])

    def call(body, out_shape, *args, scratch=(), **kwargs):
        return pl.pallas_call(
            body, out_shape=out_shape, scratch_shapes=scratch, compiler_params=PARAMS, **kwargs
        )(*args)

    hbm_space = pl.BlockSpec(memory_space=pltpu.HBM)
    cols, rows = call(
        pack_body,
        (pltpu.VMEM((row, 120, LANES), BF16), pltpu.VMEM((80, LANES), BF16)),
        pltpu.with_memory_space_constraint(points.T, pltpu.HBM),
        pltpu.with_memory_space_constraint(start_vectors.T, pltpu.HBM),
        scratch=(
            pltpu.VMEM((features, group), BF16),
            pltpu.VMEM((start_vectors.shape[1], group), BF16),
            pltpu.SemaphoreType.DMA((2,)),
        ),
        in_specs=[hbm_space, hbm_space],
    )
    forth = [(i, (i + 1) % half) for i in range(half)]
    back = [(i, (i - 1) % half) for i in range(half)]
    cols = exchange(cols, "row")
    ahead, behind = [rows], [rows]
    for _ in range(half // 2):
        behind.append(lax.ppermute(behind[-1], "z", forth))
        if len(behind) + len(ahead) - 1 < half:
            ahead.append(lax.ppermute(ahead[-1], "z", back))
    home_rows = call(order_body, pltpu.VMEM((half, 80, LANES), BF16), *behind, *ahead[:0:-1])
    away_rows = swap(home_rows)
    away_right, home_right = call(
        rows_body(log_scale), (right_shape, right_shape), away_rows, home_rows
    )
    aff_shape = pltpu.VMEM((row * group, lanes), BF16)
    send_shape = shape((half, 48, LANES), F32)
    away_aff, away_send, left, vec = call(
        away_body(log_scale),
        (
            aff_shape,
            send_shape,
            pltpu.VMEM((row * group, LANES), BF16),
            pltpu.VMEM((48, row * group), BF16),
        ),
        away_right,
        cols,
    )
    other = swap(away_send)
    home_aff, home_send = call(affinity_product, (aff_shape, send_shape), left, home_right, vec)
    send = call(join_body, send_shape, home_send, other)
    spread, degree = call(
        scale_body, (shape((row, 48, LANES), F32), shape((16, LANES), F32)), exchange(send, "z")
    )
    away_send, vec, gram = call(
        away_again_body,
        (send_shape, pltpu.VMEM((64, row * group), BF16), pltpu.VMEM((8, LANES), F32)),
        away_aff,
        exchange(spread, "row"),
    )
    other = swap(away_send)
    home_send = call(home_again_body, send_shape, home_aff, vec, gram)
    send = call(join_body, send_shape, home_send, other)
    scaled, gram = call(
        middle_body(total),
        (shape((32, 2 * LANES), F32), shape((row, 8, LANES), F32)),
        exchange(send, "z"),
        degree,
    )
    gram = call(again_body, shape((col, 8, LANES), F32), exchange(gram, "row"))
    out = call(last_body(total), shape((32, group), F32), exchange(gram, ("z", "core")), scaled)
    return out.T


def solution(mesh):
    rows, cols = mesh.devices.shape
    finer = Mesh(mesh.devices.reshape(rows, cols // 2, 2), ("row", "z", "core"))
    spec = P(("row", "z", "core"), None)
    return jax.shard_map(
        shards, mesh=finer, in_specs=(spec, spec), out_specs=spec, check_vma=False
    )
```

```python
import math

import jax
import jax.numpy as jnp
from jax import lax
from jax.experimental import pallas as pl
from jax.experimental.pallas import tpu as pltpu
from jax.sharding import Mesh
from jax.sharding import PartitionSpec as P

KERNEL_SCALE = 5.12
F32 = jnp.float32
BF16 = jnp.bfloat16
LANES = 128
PARAMS = pltpu.CompilerParams(vmem_limit_bytes=32 * 1024 * 1024)
REST = 32
WIDTH = 512
NORM, ONES, END = 64, 67, 70


def lane_of(shape):
    return lax.broadcasted_iota(jnp.int32, shape, len(shape) - 1)


def row_of(shape):
    return lax.broadcasted_iota(jnp.int32, shape, len(shape) - 2)


def roll(x, shift):
    shift %= LANES
    return pltpu.roll(x, shift, 1) if shift else x


def fold(x, place=0):
    h = x.shape[0] // 4
    group = lane_of((h, LANES)) // REST
    out = jnp.zeros((h, LANES), F32)
    for g in range(4):
        out = jnp.where(group == g, roll(x[g * h : (g + 1) * h], REST * (g - place)), out)
    return out


def unfold(pieces):
    h = pieces[0].shape[0]
    group = lane_of((h, LANES)) // REST
    rows = []
    for g in range(4):
        out = jnp.zeros((h, LANES), F32)
        for q, piece in enumerate(pieces):
            out = jnp.where(group == q, roll(piece, REST * (q - g)), out)
        rows.append(out)
    return jnp.concatenate(rows, axis=0)


def split(x):
    first = x.astype(BF16).astype(F32)
    second = (x - first).astype(BF16).astype(F32)
    return first, second, x - first - second


def widen(x):
    return jnp.concatenate([x, jnp.zeros((x.shape[0], LANES - x.shape[1]), x.dtype)], axis=1)


def main_and_rest(x):
    return x[:, 0:LANES], fold(widen(x[:, LANES : LANES + REST]))


def copies(ref, value):
    for i in range(ref.shape[0]):
        ref[i] = value


def pack_body(points_hbm, vectors_hbm, cols_ref, rows_ref, points_ref, vectors_ref, sems):
    loads = (
        pltpu.make_async_copy(points_hbm, points_ref, sems.at[0]),
        pltpu.make_async_copy(vectors_hbm, vectors_ref, sems.at[1]),
    )
    for load in loads:
        load.start()
    for load in loads:
        load.wait()
    pts = points_ref[...].astype(F32)
    main, rest = main_and_rest(pts)
    rows_ref[...] = jnp.concatenate([main, rest], axis=0).astype(BF16)
    features, group = pts.shape
    half = group // 2
    flat = jnp.concatenate([main, widen(pts[:, LANES:])], axis=1)
    flat = jnp.concatenate([flat, jnp.zeros_like(flat)], axis=0).T
    by_point = flat[0:half] + roll(flat[half:group], features)
    main, rest = main_and_rest(vectors_ref[...].astype(F32))
    copies(cols_ref, jnp.concatenate([by_point, main, rest], axis=0).astype(BF16))


def blocks_of(count):
    lanes = count * LANES
    main = [(at, WIDTH) for at in range(0, lanes, WIDTH)]
    return main, (lanes, lanes // 4)


def put_columns(log_scale, cols_ref, left_ref, vec_ref):
    count = cols_ref.shape[0]
    total = left_ref.shape[0]
    lane = lane_of((80, LANES))
    low = lane < NORM
    for i in range(count):
        raw = cols_ref[i, 0:80].astype(F32)
        squares = raw * raw
        blocks = []
        for side in range(2):
            mine = low if side == 0 else jnp.logical_not(low)
            norm = jnp.sum(jnp.where(mine, squares, 0.0), axis=1, keepdims=True)
            norm = norm * (-0.5 * log_scale)
            block = jnp.where(low, raw if side == 0 else roll(raw, NORM), 0.0)
            for k, piece in enumerate(split(norm)):
                block = jnp.where(lane == NORM + k, piece, block)
            block = jnp.where((lane >= ONES) & (lane < END), 1.0, block)
            blocks.append(block.astype(BF16))
        at = i * LANES
        left_ref[at : at + 80, :] = blocks[0]
        left_ref[at + 80 : at + LANES, :] = blocks[1][0:48]
        at = count * LANES + i * REST
        left_ref[at : at + REST, :] = blocks[1][48:80]
    vec_ref[32:48, :] = jnp.where(row_of((16, total)) == 0, 1.0, 0.0).astype(BF16)
    for i in range(count):
        vec_ref[0:32, i * LANES : (i + 1) * LANES] = cols_ref[i, 80:112]
    for m in range(count // 4):
        rests = [cols_ref[4 * m + q, 112:120].astype(F32) for q in range(4)]
        at = (count + m) * LANES
        vec_ref[0:32, at : at + LANES] = unfold(rests).astype(BF16)


def put_rows(log_scale, rows_ref, core, right_ref):
    count = rows_ref.shape[0] // 2

    def put(tile, raw):
        at = tile * LANES
        scaled = raw * log_scale
        first = scaled.astype(BF16)
        norm = jnp.sum(raw * raw, axis=0, keepdims=True) * (-0.5 * log_scale)
        row = row_of((16, LANES))
        extra = jnp.where(row < ONES - NORM, 1.0, 0.0)
        for i, piece in enumerate(split(norm)):
            extra = jnp.where(row == ONES - NORM + i, piece, extra)
        right_ref[0:64, at : at + LANES] = first
        right_ref[64:80, at : at + LANES] = extra.astype(BF16)
        right_ref[80:128, at : at + LANES] = jnp.zeros((48, LANES), BF16)
        right_ref[128:192, at : at + LANES] = (scaled - first.astype(F32)).astype(BF16)
        right_ref[192:256, at : at + LANES] = jnp.zeros((64, LANES), BF16)

    for i in range(count):
        put(i, rows_ref[2 * i + core, 0:64].astype(F32))
    for m in range(count // 4):
        rests = [rows_ref[2 * (4 * m + q) + core, 64:80].astype(F32) for q in range(4)]
        put(count + m, unfold(rests))


def affinity_product(left_ref, right_ref, vec_ref, aff_ref, send_ref):
    total = left_ref.shape[0]
    main, rest = blocks_of(send_ref.shape[0])
    chunk = 512

    def product(at, width):
        right = right_ref[:, at : at + width]
        for start in range(0, total, chunk):
            left = left_ref[start : start + chunk, :]
            power = jnp.dot(
                jnp.concatenate([left, left], axis=1), right, preferred_element_type=F32
            )
            aff_ref[start : start + chunk, at : at + width] = jnp.exp2(power).astype(BF16)
        return jnp.dot(
            vec_ref[...], aff_ref[:, at : at + width], preferred_element_type=F32
        )

    for at, width in main:
        out = product(at, width)
        for k in range(width // LANES):
            tile = out[:, k * LANES : (k + 1) * LANES]
            send_ref[at // LANES + k, 0:32, :] = tile[0:32]
            send_ref[at // LANES + k, 40:48, :] = tile[32:40]
    out = product(*rest)
    for m in range(rest[1] // LANES):
        tile = out[:, m * LANES : (m + 1) * LANES]
        for q in range(4):
            send_ref[4 * m + q, 32:40, :] = fold(tile[0:32], q)
            send_ref[4 * m + q, 41:42, :] = roll(tile[32:40], -REST * q)[0:1]


def away_body(log_scale):
    def body(right_ref, cols_ref, aff_ref, send_ref, left_ref, vec_ref):
        put_columns(log_scale, cols_ref, left_ref, vec_ref)
        affinity_product(left_ref, right_ref, vec_ref, aff_ref, send_ref)

    return body


def rows_body(log_scale):
    def body(rows_ref, away_right_ref, home_right_ref):
        core = lax.axis_index("core")
        put_rows(log_scale, rows_ref, 1 - core, away_right_ref)
        put_rows(log_scale, rows_ref, core, home_right_ref)

    return body


def join_body(mine_ref, other_ref, out_ref):
    out_ref[...] = mine_ref[...] + other_ref[...]


def gram_of(x):
    return lax.dot_general(
        x,
        x,
        (((1,), (1,)), ((), ())),
        precision=lax.Precision.HIGHEST,
        preferred_element_type=F32,
    )


def whole(main, rest):
    return jnp.concatenate([main, unfold([rest])], axis=1)


def scale_body(recv_ref, spread_ref, degree_ref):
    total = jnp.sum(recv_ref[...], axis=0)
    rest = jnp.where(lane_of((1, LANES)) < REST, total[41:42], 0.0)
    rest = jnp.broadcast_to(rest, (8, LANES))
    rest = (rest + roll(rest, REST)) + (roll(rest, 2 * REST) + roll(rest, 3 * REST))
    degree_ref[0:8, :] = jnp.broadcast_to(total[40:41], (8, LANES))
    degree_ref[8:16, :] = rest
    main, rest = total[0:32] / total[40:41], total[32:40] / rest
    gram = fold(widen(gram_of(whole(main, rest))))
    copies(spread_ref, jnp.concatenate([main, rest, gram], axis=0))


def put_vectors(spread_ref, vec_ref):
    count = spread_ref.shape[0]

    def put(tile, value):
        first = value.astype(BF16)
        at = tile * LANES
        vec_ref[0:32, at : at + LANES] = first
        vec_ref[32:64, at : at + LANES] = (value - first.astype(F32)).astype(BF16)

    for i in range(count):
        put(i, spread_ref[i, 0:32, :])
    for m in range(count // 4):
        put(count + m, unfold([spread_ref[4 * m + q, 32:40, :] for q in range(4)]))


def second_product(aff_ref, vec_ref, gram, send_ref):
    main, rest = blocks_of(send_ref.shape[0])

    def product(at, width):
        out = jnp.dot(vec_ref[...], aff_ref[:, at : at + width], preferred_element_type=F32)
        return out[0:32] + out[32:64]

    for at, width in main:
        out = product(at, width)
        for k in range(width // LANES):
            send_ref[at // LANES + k, 0:32, :] = out[:, k * LANES : (k + 1) * LANES]
            send_ref[at // LANES + k, 40:48, :] = gram
    out = product(*rest)
    for m in range(rest[1] // LANES):
        for q in range(4):
            send_ref[4 * m + q, 32:40, :] = fold(out[:, m * LANES : (m + 1) * LANES], q)


def away_again_body(aff_ref, spread_ref, send_ref, vec_ref, gram_ref):
    gram = jnp.sum(spread_ref[:, 40:48, :], axis=0)
    gram_ref[...] = gram
    put_vectors(spread_ref, vec_ref)
    second_product(aff_ref, vec_ref, gram, send_ref)


def home_again_body(aff_ref, vec_ref, gram_ref, send_ref):
    second_product(aff_ref, vec_ref, gram_ref[...], send_ref)


def solved(gram, right):
    size = gram.shape[0]
    wide = right.shape[1] // LANES
    columns = [
        jnp.broadcast_to(gram[8 * (k // 8) :, k : k + 1], (size - 8 * (k // 8), LANES))
        for k in range(size)
    ]
    rows = [right[8 * g : 8 * g + 8] for g in range(size // 8)]
    for j in range(size):
        base, at = j // 8, j % 8
        pivot = columns[j][at : at + 1]
        scale = lax.rsqrt(pivot)
        scale = scale * (1.5 - 0.5 * pivot * scale * scale)
        factor = columns[j] * scale
        for k in range(j + 1, size):
            skip = 8 * (k // 8 - base)
            mine = factor[k - 8 * base : k - 8 * base + 1]
            columns[k] = columns[k] - factor[skip:] * mine
        top = rows[base][at : at + 1] * jnp.concatenate([scale] * wide, axis=1)
        for g in range(base, size // 8):
            part = factor[8 * (g - base) : 8 * (g - base) + 8]
            if g == base:
                row = row_of((8, LANES))
                part = jnp.where(row > at, part, 0.0)
            new = rows[g] - jnp.concatenate([part] * wide, axis=1) * top
            if g == base:
                new = jnp.where(row_of(new.shape) == at, top, new)
            rows[g] = new
    return jnp.concatenate(rows, axis=0)


def middle_body(points):
    def body(recv_ref, degree_ref, scaled_ref, gram_ref):
        total = jnp.sum(recv_ref[...], axis=0)
        main = total[0:32] / degree_ref[0:1, :]
        rest = total[32:40] / degree_ref[8:16, :]
        scaled = solved(unfold([total[40:48]]) / points, whole(main, rest))
        scaled_ref[...] = scaled
        copies(gram_ref, fold(widen(gram_of(scaled))))

    return body


def again_body(recv_ref, gram_ref):
    copies(gram_ref, jnp.sum(recv_ref[...], axis=0))


def last_body(points):
    def body(recv_ref, scaled_ref, out_ref):
        gram = unfold([jnp.sum(recv_ref[...], axis=0)]) / points
        out_ref[...] = solved(gram, scaled_ref[...])[:, 0 : out_ref.shape[1]]

    return body


def shards(points, start_vectors):
    group, features = points.shape
    row, half, cores = lax.axis_size("row"), lax.axis_size("z"), lax.axis_size("core")
    col = half * cores
    total = group * row * col
    log_scale = 2.0 * KERNEL_SCALE / features * math.log2(math.e)
    lanes = half * group
    right_shape = pltpu.VMEM((256, lanes), BF16)
    shape = jax.ShapeDtypeStruct

    def exchange(x, axis):
        return lax.all_to_all(x, axis, 0, 0, tiled=True)

    def swap(x):
        return lax.ppermute(x, "core", [(0, 1), (1, 0)])

    def call(body, out_shape, *args, scratch=(), **kwargs):
        return pl.pallas_call(
            body, out_shape=out_shape, scratch_shapes=scratch, compiler_params=PARAMS, **kwargs
        )(*args)

    hbm_space = pl.BlockSpec(memory_space=pltpu.HBM)
    cols, rows = call(
        pack_body,
        (pltpu.VMEM((row, 120, LANES), BF16), pltpu.VMEM((80, LANES), BF16)),
        pltpu.with_memory_space_constraint(points.T, pltpu.HBM),
        pltpu.with_memory_space_constraint(start_vectors.T, pltpu.HBM),
        scratch=(
            pltpu.VMEM((features, group), BF16),
            pltpu.VMEM((start_vectors.shape[1], group), BF16),
            pltpu.SemaphoreType.DMA((2,)),
        ),
        in_specs=[hbm_space, hbm_space],
    )
    cols = exchange(cols, "row")
    rows = lax.all_gather(rows, ("z", "core"))
    away_right, home_right = call(rows_body(log_scale), (right_shape, right_shape), rows)
    aff_shape = pltpu.VMEM((row * group, lanes), BF16)
    send_shape = shape((half, 48, LANES), F32)
    away_aff, away_send, left, vec = call(
        away_body(log_scale),
        (
            aff_shape,
            send_shape,
            pltpu.VMEM((row * group, LANES), BF16),
            pltpu.VMEM((48, row * group), BF16),
        ),
        away_right,
        cols,
    )
    other = swap(away_send)
    home_aff, home_send = call(affinity_product, (aff_shape, send_shape), left, home_right, vec)
    send = call(join_body, send_shape, home_send, other)
    spread, degree = call(
        scale_body, (shape((row, 48, LANES), F32), shape((16, LANES), F32)), exchange(send, "z")
    )
    away_send, vec, gram = call(
        away_again_body,
        (send_shape, pltpu.VMEM((64, row * group), BF16), pltpu.VMEM((8, LANES), F32)),
        away_aff,
        exchange(spread, "row"),
    )
    other = swap(away_send)
    home_send = call(home_again_body, send_shape, home_aff, vec, gram)
    send = call(join_body, send_shape, home_send, other)
    scaled, gram = call(
        middle_body(total),
        (shape((32, 2 * LANES), F32), shape((row, 8, LANES), F32)),
        exchange(send, "z"),
        degree,
    )
    gram = call(again_body, shape((col, 8, LANES), F32), exchange(gram, "row"))
    out = call(last_body(total), shape((32, group), F32), exchange(gram, ("z", "core")), scaled)
    return out.T


def solution(mesh):
    rows, cols = mesh.devices.shape
    finer = Mesh(mesh.devices.reshape(rows, cols // 2, 2), ("row", "z", "core"))
    spec = P(("row", "z", "core"), None)
    return jax.shard_map(
        shards, mesh=finer, in_specs=(spec, spec), out_specs=spec, check_vma=False
    )
```

```python
import math

import jax
import jax.numpy as jnp
from jax import lax
from jax.experimental import pallas as pl
from jax.experimental.pallas import tpu as pltpu
from jax.sharding import Mesh
from jax.sharding import PartitionSpec as P

KERNEL_SCALE = 5.12
F32 = jnp.float32
BF16 = jnp.bfloat16
LANES = 128
PARAMS = pltpu.CompilerParams(vmem_limit_bytes=32 * 1024 * 1024)
REST = 32
WIDTH = 512
NORM, ONES, END = 64, 67, 70


def lane_of(shape):
    return lax.broadcasted_iota(jnp.int32, shape, len(shape) - 1)


def row_of(shape):
    return lax.broadcasted_iota(jnp.int32, shape, len(shape) - 2)


def roll(x, shift):
    shift %= LANES
    return pltpu.roll(x, shift, 1) if shift else x


def fold(x, place=0):
    h = x.shape[0] // 4
    group = lane_of((h, LANES)) // REST
    out = jnp.zeros((h, LANES), F32)
    for g in range(4):
        out = jnp.where(group == g, roll(x[g * h : (g + 1) * h], REST * (g - place)), out)
    return out


def unfold(pieces):
    h = pieces[0].shape[0]
    group = lane_of((h, LANES)) // REST
    rows = []
    for g in range(4):
        out = jnp.zeros((h, LANES), F32)
        for q, piece in enumerate(pieces):
            out = jnp.where(group == q, roll(piece, REST * (q - g)), out)
        rows.append(out)
    return jnp.concatenate(rows, axis=0)


def split(x):
    first = x.astype(BF16).astype(F32)
    second = (x - first).astype(BF16).astype(F32)
    return first, second, x - first - second


def widen(x):
    return jnp.concatenate([x, jnp.zeros((x.shape[0], LANES - x.shape[1]), x.dtype)], axis=1)


def main_and_rest(x):
    return x[:, 0:LANES], fold(widen(x[:, LANES : LANES + REST]))


def copies(ref, value):
    for i in range(ref.shape[0]):
        ref[i] = value


def pack_body(log_scale):
    def body(points_hbm, vectors_hbm, cols_hbm, rows_ref, points_ref, vectors_ref, block_ref, sems):
        loads = (
            pltpu.make_async_copy(points_hbm, points_ref, sems.at[0]),
            pltpu.make_async_copy(vectors_hbm, vectors_ref, sems.at[1]),
        )
        for load in loads:
            load.start()
        loads[0].wait()
        pts = points_ref[...].astype(F32)
        group = pts.shape[1]
        main, rest = main_and_rest(pts)
        rows_ref[...] = jnp.concatenate([main, rest], axis=0).astype(BF16)
        flat = jnp.concatenate([main, widen(pts[:, LANES:])], axis=1)
        flat = jnp.concatenate([flat, jnp.zeros_like(flat)], axis=0).T[0:group]
        norm = jnp.sum(flat * flat, axis=1, keepdims=True) * (-0.5 * log_scale)
        lane = lane_of(flat.shape)
        for k, piece in enumerate(split(norm)):
            flat = jnp.where(lane == NORM + k, piece, flat)
        flat = jnp.where((lane >= ONES) & (lane < END), 1.0, flat)
        loads[1].wait()
        main, rest = main_and_rest(vectors_ref[...].astype(F32))
        block_ref[...] = jnp.concatenate([flat, main, rest], axis=0).astype(BF16)
        count = cols_hbm.shape[0]
        sends = [
            pltpu.make_async_copy(block_ref, cols_hbm.at[i], sems.at[2 + i]) for i in range(count)
        ]
        for send in sends:
            send.start()
        for send in sends:
            send.wait()

    return body


def blocks_of(count):
    lanes = count * LANES
    main = [(at, WIDTH) for at in range(0, lanes, WIDTH)]
    return main, (lanes, lanes // 4)


def put_columns(cols_ref, left_ref, vec_ref):
    count = cols_ref.shape[0]
    total = left_ref.shape[0]
    for i in range(count):
        left_ref[i * LANES : (i + 1) * LANES, :] = cols_ref[i, 0:128]
        at = count * LANES + i * REST
        left_ref[at : at + REST, :] = cols_ref[i, 128:160]
    vec_ref[32:48, :] = jnp.where(row_of((16, total)) == 0, 1.0, 0.0).astype(BF16)
    for i in range(count):
        vec_ref[0:32, i * LANES : (i + 1) * LANES] = cols_ref[i, 160:192]
    for m in range(count // 4):
        rests = [cols_ref[4 * m + q, 192:200].astype(F32) for q in range(4)]
        at = (count + m) * LANES
        vec_ref[0:32, at : at + LANES] = unfold(rests).astype(BF16)


def put_rows(log_scale, rows_ref, core, right_ref):
    count = rows_ref.shape[0] // 2

    def put(tile, raw):
        at = tile * LANES
        scaled = raw * log_scale
        first = scaled.astype(BF16)
        norm = jnp.sum(raw * raw, axis=0, keepdims=True) * (-0.5 * log_scale)
        row = row_of((16, LANES))
        extra = jnp.where(row < ONES - NORM, 1.0, 0.0)
        for i, piece in enumerate(split(norm)):
            extra = jnp.where(row == ONES - NORM + i, piece, extra)
        right_ref[0:64, at : at + LANES] = first
        right_ref[64:80, at : at + LANES] = extra.astype(BF16)
        right_ref[80:128, at : at + LANES] = jnp.zeros((48, LANES), BF16)
        right_ref[128:192, at : at + LANES] = (scaled - first.astype(F32)).astype(BF16)
        right_ref[192:256, at : at + LANES] = jnp.zeros((64, LANES), BF16)

    for i in range(count):
        put(i, rows_ref[2 * i + core, 0:64].astype(F32))
    for m in range(count // 4):
        rests = [rows_ref[2 * (4 * m + q) + core, 64:80].astype(F32) for q in range(4)]
        put(count + m, unfold(rests))


def affinity_product(left_ref, right_ref, vec_ref, aff_ref, send_ref):
    total = left_ref.shape[0]
    main, rest = blocks_of(send_ref.shape[0])
    chunk = 512

    def product(at, width):
        right = right_ref[:, at : at + width]
        for start in range(0, total, chunk):
            left = left_ref[start : start + chunk, :]
            power = jnp.dot(
                jnp.concatenate([left, left], axis=1), right, preferred_element_type=F32
            )
            aff_ref[start : start + chunk, at : at + width] = jnp.exp2(power).astype(BF16)
        return jnp.dot(
            vec_ref[...], aff_ref[:, at : at + width], preferred_element_type=F32
        )

    for at, width in main:
        out = product(at, width)
        for k in range(width // LANES):
            tile = out[:, k * LANES : (k + 1) * LANES]
            send_ref[at // LANES + k, 0:32, :] = tile[0:32]
            send_ref[at // LANES + k, 40:48, :] = tile[32:40]
    out = product(*rest)
    for m in range(rest[1] // LANES):
        tile = out[:, m * LANES : (m + 1) * LANES]
        for q in range(4):
            send_ref[4 * m + q, 32:40, :] = fold(tile[0:32], q)
            send_ref[4 * m + q, 41:42, :] = roll(tile[32:40], -REST * q)[0:1]


def away_body(right_ref, cols_ref, aff_ref, send_ref, left_ref, vec_ref):
    put_columns(cols_ref, left_ref, vec_ref)
    affinity_product(left_ref, right_ref, vec_ref, aff_ref, send_ref)


def rows_body(log_scale):
    def body(rows_ref, away_right_ref, home_right_ref):
        core = lax.axis_index("core")
        put_rows(log_scale, rows_ref, 1 - core, away_right_ref)
        put_rows(log_scale, rows_ref, core, home_right_ref)

    return body


def join_body(mine_ref, other_ref, out_ref):
    out_ref[...] = mine_ref[...] + other_ref[...]


def gram_of(x):
    return lax.dot_general(
        x,
        x,
        (((1,), (1,)), ((), ())),
        precision=lax.Precision.HIGHEST,
        preferred_element_type=F32,
    )


def whole(main, rest):
    return jnp.concatenate([main, unfold([rest])], axis=1)


def scale_body(recv_ref, spread_ref, degree_ref):
    total = jnp.sum(recv_ref[...], axis=0)
    rest = jnp.where(lane_of((1, LANES)) < REST, total[41:42], 0.0)
    rest = jnp.broadcast_to(rest, (8, LANES))
    rest = (rest + roll(rest, REST)) + (roll(rest, 2 * REST) + roll(rest, 3 * REST))
    degree_ref[0:8, :] = jnp.broadcast_to(total[40:41], (8, LANES))
    degree_ref[8:16, :] = rest
    main, rest = total[0:32] / total[40:41], total[32:40] / rest
    gram = fold(widen(gram_of(whole(main, rest))))
    copies(spread_ref, jnp.concatenate([main, rest, gram], axis=0))


def put_vectors(spread_ref, vec_ref):
    count = spread_ref.shape[0]

    def put(tile, value):
        first = value.astype(BF16)
        at = tile * LANES
        vec_ref[0:32, at : at + LANES] = first
        vec_ref[32:64, at : at + LANES] = (value - first.astype(F32)).astype(BF16)

    for i in range(count):
        put(i, spread_ref[i, 0:32, :])
    for m in range(count // 4):
        put(count + m, unfold([spread_ref[4 * m + q, 32:40, :] for q in range(4)]))


def second_product(aff_ref, vec_ref, gram, send_ref):
    main, rest = blocks_of(send_ref.shape[0])

    def product(at, width):
        out = jnp.dot(vec_ref[...], aff_ref[:, at : at + width], preferred_element_type=F32)
        return out[0:32] + out[32:64]

    for at, width in main:
        out = product(at, width)
        for k in range(width // LANES):
            send_ref[at // LANES + k, 0:32, :] = out[:, k * LANES : (k + 1) * LANES]
            send_ref[at // LANES + k, 40:48, :] = gram
    out = product(*rest)
    for m in range(rest[1] // LANES):
        for q in range(4):
            send_ref[4 * m + q, 32:40, :] = fold(out[:, m * LANES : (m + 1) * LANES], q)


def away_again_body(aff_ref, spread_ref, send_ref, vec_ref, gram_ref):
    gram = jnp.sum(spread_ref[:, 40:48, :], axis=0)
    gram_ref[...] = gram
    put_vectors(spread_ref, vec_ref)
    second_product(aff_ref, vec_ref, gram, send_ref)


def home_again_body(aff_ref, vec_ref, gram_ref, send_ref):
    second_product(aff_ref, vec_ref, gram_ref[...], send_ref)


def solved(gram, right):
    size = gram.shape[0]
    wide = right.shape[1] // LANES
    columns = [
        jnp.broadcast_to(gram[8 * (k // 8) :, k : k + 1], (size - 8 * (k // 8), LANES))
        for k in range(size)
    ]
    rows = [right[8 * g : 8 * g + 8] for g in range(size // 8)]
    for j in range(size):
        base, at = j // 8, j % 8
        pivot = columns[j][at : at + 1]
        scale = lax.rsqrt(pivot)
        scale = scale * (1.5 - 0.5 * pivot * scale * scale)
        factor = columns[j] * scale
        for k in range(j + 1, size):
            skip = 8 * (k // 8 - base)
            mine = factor[k - 8 * base : k - 8 * base + 1]
            columns[k] = columns[k] - factor[skip:] * mine
        top = rows[base][at : at + 1] * jnp.concatenate([scale] * wide, axis=1)
        for g in range(base, size // 8):
            part = factor[8 * (g - base) : 8 * (g - base) + 8]
            if g == base:
                row = row_of((8, LANES))
                part = jnp.where(row > at, part, 0.0)
            new = rows[g] - jnp.concatenate([part] * wide, axis=1) * top
            if g == base:
                new = jnp.where(row_of(new.shape) == at, top, new)
            rows[g] = new
    return jnp.concatenate(rows, axis=0)


def middle_body(points):
    def body(recv_ref, degree_ref, scaled_ref, gram_ref):
        total = jnp.sum(recv_ref[...], axis=0)
        main = total[0:32] / degree_ref[0:1, :]
        rest = total[32:40] / degree_ref[8:16, :]
        scaled = solved(unfold([total[40:48]]) / points, whole(main, rest))
        scaled_ref[...] = scaled
        copies(gram_ref, fold(widen(gram_of(scaled))))

    return body


def again_body(recv_ref, gram_ref):
    copies(gram_ref, jnp.sum(recv_ref[...], axis=0))


def last_body(points):
    def body(recv_ref, scaled_ref, out_ref):
        gram = unfold([jnp.sum(recv_ref[...], axis=0)]) / points
        out_ref[...] = solved(gram, scaled_ref[...])[:, 0 : out_ref.shape[1]]

    return body


def shards(points, start_vectors):
    group, features = points.shape
    row, half, cores = lax.axis_size("row"), lax.axis_size("z"), lax.axis_size("core")
    col = half * cores
    total = group * row * col
    log_scale = 2.0 * KERNEL_SCALE / features * math.log2(math.e)
    lanes = half * group
    right_shape = pltpu.VMEM((256, lanes), BF16)
    shape = jax.ShapeDtypeStruct

    def exchange(x, axis):
        return lax.all_to_all(x, axis, 0, 0, tiled=True)

    def swap(x):
        return lax.ppermute(x, "core", [(0, 1), (1, 0)])

    def call(body, out_shape, *args, scratch=(), **kwargs):
        return pl.pallas_call(
            body, out_shape=out_shape, scratch_shapes=scratch, compiler_params=PARAMS, **kwargs
        )(*args)

    hbm_space = pl.BlockSpec(memory_space=pltpu.HBM)
    cols, rows = call(
        pack_body(log_scale),
        (shape((row, group + 40, LANES), BF16), pltpu.VMEM((80, LANES), BF16)),
        pltpu.with_memory_space_constraint(points.T, pltpu.HBM),
        pltpu.with_memory_space_constraint(start_vectors.T, pltpu.HBM),
        scratch=(
            pltpu.VMEM((features, group), BF16),
            pltpu.VMEM((start_vectors.shape[1], group), BF16),
            pltpu.VMEM((group + 40, LANES), BF16),
            pltpu.SemaphoreType.DMA((2 + row,)),
        ),
        in_specs=[hbm_space, hbm_space],
        out_specs=(hbm_space, pl.BlockSpec(memory_space=pltpu.VMEM)),
    )
    cols = exchange(cols, "row")
    rows = lax.all_gather(rows, ("z", "core"))
    away_right, home_right = call(rows_body(log_scale), (right_shape, right_shape), rows)
    aff_shape = pltpu.VMEM((row * group, lanes), BF16)
    send_shape = shape((half, 48, LANES), F32)
    away_aff, away_send, left, vec = call(
        away_body,
        (
            aff_shape,
            send_shape,
            pltpu.VMEM((row * group, LANES), BF16),
            pltpu.VMEM((48, row * group), BF16),
        ),
        away_right,
        cols,
    )
    other = swap(away_send)
    home_aff, home_send = call(affinity_product, (aff_shape, send_shape), left, home_right, vec)
    send = call(join_body, send_shape, home_send, other)
    spread, degree = call(
        scale_body, (shape((row, 48, LANES), F32), shape((16, LANES), F32)), exchange(send, "z")
    )
    away_send, vec, gram = call(
        away_again_body,
        (send_shape, pltpu.VMEM((64, row * group), BF16), pltpu.VMEM((8, LANES), F32)),
        away_aff,
        exchange(spread, "row"),
    )
    other = swap(away_send)
    home_send = call(home_again_body, send_shape, home_aff, vec, gram)
    send = call(join_body, send_shape, home_send, other)
    scaled, gram = call(
        middle_body(total),
        (shape((32, 2 * LANES), F32), shape((row, 8, LANES), F32)),
        exchange(send, "z"),
        degree,
    )
    gram = call(again_body, shape((col, 8, LANES), F32), exchange(gram, "row"))
    out = call(last_body(total), shape((32, group), F32), exchange(gram, ("z", "core")), scaled)
    return out.T


def solution(mesh):
    rows, cols = mesh.devices.shape
    finer = Mesh(mesh.devices.reshape(rows, cols // 2, 2), ("row", "z", "core"))
    spec = P(("row", "z", "core"), None)
    return jax.shard_map(
        shards, mesh=finer, in_specs=(spec, spec), out_specs=spec, check_vma=False
    )
```

```python
import math

import jax
import jax.numpy as jnp
from jax import lax
from jax.experimental import pallas as pl
from jax.experimental.pallas import tpu as pltpu
from jax.sharding import Mesh
from jax.sharding import PartitionSpec as P

KERNEL_SCALE = 5.12
F32 = jnp.float32
BF16 = jnp.bfloat16
LANES = 128
PARAMS = pltpu.CompilerParams(vmem_limit_bytes=32 * 1024 * 1024)
REST = 32
WIDTH = 512
NORM, ONES, END = 64, 67, 70


def lane_of(shape):
    return lax.broadcasted_iota(jnp.int32, shape, len(shape) - 1)


def row_of(shape):
    return lax.broadcasted_iota(jnp.int32, shape, len(shape) - 2)


def roll(x, shift):
    shift %= LANES
    return pltpu.roll(x, shift, 1) if shift else x


def fold(x, place=0):
    h = x.shape[0] // 4
    group = lane_of((h, LANES)) // REST
    out = jnp.zeros((h, LANES), F32)
    for g in range(4):
        out = jnp.where(group == g, roll(x[g * h : (g + 1) * h], REST * (g - place)), out)
    return out


def unfold(pieces):
    h = pieces[0].shape[0]
    group = lane_of((h, LANES)) // REST
    rows = []
    for g in range(4):
        out = jnp.zeros((h, LANES), F32)
        for q, piece in enumerate(pieces):
            out = jnp.where(group == q, roll(piece, REST * (q - g)), out)
        rows.append(out)
    return jnp.concatenate(rows, axis=0)


def split(x):
    first = x.astype(BF16).astype(F32)
    second = (x - first).astype(BF16).astype(F32)
    return first, second, x - first - second


def widen(x):
    return jnp.concatenate([x, jnp.zeros((x.shape[0], LANES - x.shape[1]), x.dtype)], axis=1)


def main_and_rest(x):
    return x[:, 0:LANES], fold(widen(x[:, LANES : LANES + REST]))


def copies(ref, value):
    for i in range(ref.shape[0]):
        ref[i] = value


def pack_body(log_scale):
    def body(points_hbm, vectors_hbm, cols_hbm, rows_ref, points_ref, vectors_ref, block_ref, sems):
        loads = (
            pltpu.make_async_copy(points_hbm, points_ref, sems.at[0]),
            pltpu.make_async_copy(vectors_hbm, vectors_ref, sems.at[1]),
        )
        for load in loads:
            load.start()
        loads[0].wait()
        pts = points_ref[...].astype(F32)
        group = pts.shape[1]
        main, rest = main_and_rest(pts)
        rows_ref[...] = jnp.concatenate([main, rest], axis=0).astype(BF16)
        flat = jnp.concatenate([pts[:, 0:LANES], widen(pts[:, LANES:])], axis=1)
        norm = jnp.sum(flat * flat, axis=0, keepdims=True) * (-0.5 * log_scale)
        row = row_of((8, flat.shape[1]))
        extra = jnp.where((row >= ONES - NORM) & (row < END - NORM), 1.0, 0.0)
        for k, piece in enumerate(split(norm)):
            extra = jnp.where(row == k, piece, extra)
        rest = jnp.zeros((LANES - NORM - 8, flat.shape[1]), F32)
        flat = jnp.concatenate([flat, extra, rest], axis=0).T[0:group]
        loads[1].wait()
        main, rest = main_and_rest(vectors_ref[...].astype(F32))
        block_ref[...] = jnp.concatenate([flat, main, rest], axis=0).astype(BF16)
        count = cols_hbm.shape[0]
        sends = [
            pltpu.make_async_copy(block_ref, cols_hbm.at[i], sems.at[2 + i]) for i in range(count)
        ]
        for send in sends:
            send.start()
        for send in sends:
            send.wait()

    return body


def blocks_of(count):
    lanes = count * LANES
    main = [(at, WIDTH) for at in range(0, lanes, WIDTH)]
    return main, (lanes, lanes // 4)


def put_columns(cols_ref, left_ref, vec_ref):
    count = cols_ref.shape[0]
    total = left_ref.shape[0]
    for i in range(count):
        left_ref[i * LANES : (i + 1) * LANES, :] = cols_ref[i, 0:128]
        at = count * LANES + i * REST
        left_ref[at : at + REST, :] = cols_ref[i, 128:160]
    vec_ref[32:48, :] = jnp.where(row_of((16, total)) == 0, 1.0, 0.0).astype(BF16)
    for i in range(count):
        vec_ref[0:32, i * LANES : (i + 1) * LANES] = cols_ref[i, 160:192]
    for m in range(count // 4):
        rests = [cols_ref[4 * m + q, 192:200].astype(F32) for q in range(4)]
        at = (count + m) * LANES
        vec_ref[0:32, at : at + LANES] = unfold(rests).astype(BF16)


def put_rows(log_scale, rows_ref, core, right_ref):
    count = rows_ref.shape[0] // 2

    def put(tile, raw):
        at = tile * LANES
        scaled = raw * log_scale
        first = scaled.astype(BF16)
        norm = jnp.sum(raw * raw, axis=0, keepdims=True) * (-0.5 * log_scale)
        row = row_of((16, LANES))
        extra = jnp.where(row < ONES - NORM, 1.0, 0.0)
        for i, piece in enumerate(split(norm)):
            extra = jnp.where(row == ONES - NORM + i, piece, extra)
        right_ref[0:64, at : at + LANES] = first
        right_ref[64:80, at : at + LANES] = extra.astype(BF16)
        right_ref[80:128, at : at + LANES] = jnp.zeros((48, LANES), BF16)
        right_ref[128:192, at : at + LANES] = (scaled - first.astype(F32)).astype(BF16)
        right_ref[192:256, at : at + LANES] = jnp.zeros((64, LANES), BF16)

    for i in range(count):
        put(i, rows_ref[2 * i + core, 0:64].astype(F32))
    for m in range(count // 4):
        rests = [rows_ref[2 * (4 * m + q) + core, 64:80].astype(F32) for q in range(4)]
        put(count + m, unfold(rests))


def affinity_product(left_ref, right_ref, vec_ref, aff_ref, send_ref):
    total = left_ref.shape[0]
    main, rest = blocks_of(send_ref.shape[0])
    chunk = 512

    def product(at, width):
        right = right_ref[:, at : at + width]
        for start in range(0, total, chunk):
            left = left_ref[start : start + chunk, :]
            power = jnp.dot(
                jnp.concatenate([left, left], axis=1), right, preferred_element_type=F32
            )
            aff_ref[start : start + chunk, at : at + width] = jnp.exp2(power).astype(BF16)
        return jnp.dot(
            vec_ref[...], aff_ref[:, at : at + width], preferred_element_type=F32
        )

    for at, width in main:
        out = product(at, width)
        for k in range(width // LANES):
            tile = out[:, k * LANES : (k + 1) * LANES]
            send_ref[at // LANES + k, 0:32, :] = tile[0:32]
            send_ref[at // LANES + k, 40:48, :] = tile[32:40]
    out = product(*rest)
    for m in range(rest[1] // LANES):
        tile = out[:, m * LANES : (m + 1) * LANES]
        for q in range(4):
            send_ref[4 * m + q, 32:40, :] = fold(tile[0:32], q)
            send_ref[4 * m + q, 41:42, :] = roll(tile[32:40], -REST * q)[0:1]


def away_body(right_ref, cols_ref, aff_ref, send_ref, left_ref, vec_ref):
    put_columns(cols_ref, left_ref, vec_ref)
    affinity_product(left_ref, right_ref, vec_ref, aff_ref, send_ref)


def rows_body(log_scale):
    def body(pair_ref, *refs):
        *moved, away_right_ref, home_right_ref, rows_ref = refs
        core = lax.axis_index("core")
        here = lax.axis_index("z")
        count = rows_ref.shape[0] // 2
        steps = len(moved) // 2
        rows_ref[pl.ds(2 * here, 2)] = pair_ref[...]
        for t in range(1, steps + 1):
            mine, other = moved[t - 1], moved[steps + t - 1]
            up = lax.rem(here + count - t, count)
            down = lax.rem(here + t, count)
            rows_ref[pl.ds(2 * lax.select(core == 0, up, down), 2)] = mine[...]
            rows_ref[pl.ds(2 * lax.select(core == 0, down, up), 2)] = other[...]
        put_rows(log_scale, rows_ref, 1 - core, away_right_ref)
        put_rows(log_scale, rows_ref, core, home_right_ref)

    return body


def pair_body(mine_ref, other_ref, out_ref):
    core = lax.axis_index("core")
    out_ref[core] = mine_ref[...]
    out_ref[1 - core] = other_ref[...]


def join_body(mine_ref, other_ref, out_ref):
    out_ref[...] = mine_ref[...] + other_ref[...]


def gram_of(x):
    return lax.dot_general(
        x,
        x,
        (((1,), (1,)), ((), ())),
        precision=lax.Precision.HIGHEST,
        preferred_element_type=F32,
    )


def whole(main, rest):
    return jnp.concatenate([main, unfold([rest])], axis=1)


def scale_body(recv_ref, spread_ref, degree_ref):
    total = jnp.sum(recv_ref[...], axis=0)
    rest = jnp.where(lane_of((1, LANES)) < REST, total[41:42], 0.0)
    rest = jnp.broadcast_to(rest, (8, LANES))
    rest = (rest + roll(rest, REST)) + (roll(rest, 2 * REST) + roll(rest, 3 * REST))
    degree_ref[0:8, :] = jnp.broadcast_to(total[40:41], (8, LANES))
    degree_ref[8:16, :] = rest
    main, rest = total[0:32] / total[40:41], total[32:40] / rest
    gram = fold(widen(gram_of(whole(main, rest))))
    copies(spread_ref, jnp.concatenate([main, rest, gram], axis=0))


def put_vectors(spread_ref, vec_ref):
    count = spread_ref.shape[0]

    def put(tile, value):
        first = value.astype(BF16)
        at = tile * LANES
        vec_ref[0:32, at : at + LANES] = first
        vec_ref[32:64, at : at + LANES] = (value - first.astype(F32)).astype(BF16)

    for i in range(count):
        put(i, spread_ref[i, 0:32, :])
    for m in range(count // 4):
        put(count + m, unfold([spread_ref[4 * m + q, 32:40, :] for q in range(4)]))


def second_product(aff_ref, vec_ref, gram, send_ref):
    main, rest = blocks_of(send_ref.shape[0])

    def product(at, width):
        out = jnp.dot(vec_ref[...], aff_ref[:, at : at + width], preferred_element_type=F32)
        return out[0:32] + out[32:64]

    for at, width in main:
        out = product(at, width)
        for k in range(width // LANES):
            send_ref[at // LANES + k, 0:32, :] = out[:, k * LANES : (k + 1) * LANES]
            send_ref[at // LANES + k, 40:48, :] = gram
    out = product(*rest)
    for m in range(rest[1] // LANES):
        for q in range(4):
            send_ref[4 * m + q, 32:40, :] = fold(out[:, m * LANES : (m + 1) * LANES], q)


def away_again_body(aff_ref, spread_ref, send_ref, vec_ref, gram_ref):
    gram = jnp.sum(spread_ref[:, 40:48, :], axis=0)
    gram_ref[...] = gram
    put_vectors(spread_ref, vec_ref)
    second_product(aff_ref, vec_ref, gram, send_ref)


def home_again_body(aff_ref, vec_ref, gram_ref, send_ref):
    second_product(aff_ref, vec_ref, gram_ref[...], send_ref)


def solved(gram, right):
    size = gram.shape[0]
    wide = right.shape[1] // LANES
    columns = [
        jnp.broadcast_to(gram[8 * (k // 8) :, k : k + 1], (size - 8 * (k // 8), LANES))
        for k in range(size)
    ]
    rows = [right[8 * g : 8 * g + 8] for g in range(size // 8)]
    for j in range(size):
        base, at = j // 8, j % 8
        pivot = columns[j][at : at + 1]
        scale = lax.rsqrt(pivot)
        scale = scale * (1.5 - 0.5 * pivot * scale * scale)
        factor = columns[j] * scale
        for k in range(j + 1, size):
            skip = 8 * (k // 8 - base)
            mine = factor[k - 8 * base : k - 8 * base + 1]
            columns[k] = columns[k] - factor[skip:] * mine
        top = rows[base][at : at + 1] * jnp.concatenate([scale] * wide, axis=1)
        for g in range(base, size // 8):
            part = factor[8 * (g - base) : 8 * (g - base) + 8]
            if g == base:
                row = row_of((8, LANES))
                part = jnp.where(row > at, part, 0.0)
            new = rows[g] - jnp.concatenate([part] * wide, axis=1) * top
            if g == base:
                new = jnp.where(row_of(new.shape) == at, top, new)
            rows[g] = new
    return jnp.concatenate(rows, axis=0)


def middle_body(points):
    def body(recv_ref, degree_ref, scaled_ref, gram_ref):
        total = jnp.sum(recv_ref[...], axis=0)
        main = total[0:32] / degree_ref[0:1, :]
        rest = total[32:40] / degree_ref[8:16, :]
        scaled = solved(unfold([total[40:48]]) / points, whole(main, rest))
        scaled_ref[...] = scaled
        copies(gram_ref, fold(widen(gram_of(scaled))))

    return body


def again_body(recv_ref, gram_ref):
    copies(gram_ref, jnp.sum(recv_ref[...], axis=0))


def last_body(points):
    def body(recv_ref, scaled_ref, out_ref):
        gram = unfold([jnp.sum(recv_ref[...], axis=0)]) / points
        out_ref[...] = solved(gram, scaled_ref[...])[:, 0 : out_ref.shape[1]]

    return body


def shards(points, start_vectors):
    group, features = points.shape
    row, half, cores = lax.axis_size("row"), lax.axis_size("z"), lax.axis_size("core")
    col = half * cores
    total = group * row * col
    log_scale = 2.0 * KERNEL_SCALE / features * math.log2(math.e)
    lanes = half * group
    right_shape = pltpu.VMEM((256, lanes), BF16)
    shape = jax.ShapeDtypeStruct

    def exchange(x, axis):
        return lax.all_to_all(x, axis, 0, 0, tiled=True)

    def swap(x):
        return lax.ppermute(x, "core", [(0, 1), (1, 0)])

    def call(body, out_shape, *args, scratch=(), **kwargs):
        return pl.pallas_call(
            body, out_shape=out_shape, scratch_shapes=scratch, compiler_params=PARAMS, **kwargs
        )(*args)

    hbm_space = pl.BlockSpec(memory_space=pltpu.HBM)
    cols, rows = call(
        pack_body(log_scale),
        (shape((row, group + 40, LANES), BF16), pltpu.VMEM((80, LANES), BF16)),
        pltpu.with_memory_space_constraint(points.T, pltpu.HBM),
        pltpu.with_memory_space_constraint(start_vectors.T, pltpu.HBM),
        scratch=(
            pltpu.VMEM((features, group), BF16),
            pltpu.VMEM((start_vectors.shape[1], group), BF16),
            pltpu.VMEM((group + 40, LANES), BF16),
            pltpu.SemaphoreType.DMA((2 + row,)),
        ),
        in_specs=[hbm_space, hbm_space],
        out_specs=(hbm_space, pl.BlockSpec(memory_space=pltpu.VMEM)),
    )
    cols = exchange(cols, "row")
    other = swap(rows)
    pair = call(pair_body, pltpu.VMEM((2, 80, LANES), BF16), rows, other)
    ways = [(2 * z, 2 * ((z + 1) % half)) for z in range(half)]
    ways += [(2 * z + 1, 2 * ((z - 1) % half) + 1) for z in range(half)]
    mine, others = [pair], []
    for _ in range(half // 2):
        mine.append(lax.ppermute(mine[-1], ("z", "core"), ways))
        others.append(swap(mine[-1]))
    away_right, home_right = call(
        rows_body(log_scale),
        (right_shape, right_shape),
        *mine,
        *others,
        scratch=(pltpu.VMEM((col, 80, LANES), BF16),),
    )
    aff_shape = pltpu.VMEM((row * group, lanes), BF16)
    send_shape = shape((half, 48, LANES), F32)
    away_aff, away_send, left, vec = call(
        away_body,
        (
            aff_shape,
            send_shape,
            pltpu.VMEM((row * group, LANES), BF16),
            pltpu.VMEM((48, row * group), BF16),
        ),
        away_right,
        cols,
    )
    other = swap(away_send)
    home_aff, home_send = call(affinity_product, (aff_shape, send_shape), left, home_right, vec)
    send = call(join_body, send_shape, home_send, other)
    spread, degree = call(
        scale_body, (shape((row, 48, LANES), F32), shape((16, LANES), F32)), exchange(send, "z")
    )
    away_send, vec, gram = call(
        away_again_body,
        (send_shape, pltpu.VMEM((64, row * group), BF16), pltpu.VMEM((8, LANES), F32)),
        away_aff,
        exchange(spread, "row"),
    )
    other = swap(away_send)
    home_send = call(home_again_body, send_shape, home_aff, vec, gram)
    send = call(join_body, send_shape, home_send, other)
    scaled, gram = call(
        middle_body(total),
        (shape((32, 2 * LANES), F32), shape((row, 8, LANES), F32)),
        exchange(send, "z"),
        degree,
    )
    gram = call(again_body, shape((col, 8, LANES), F32), exchange(gram, "row"))
    out = call(last_body(total), shape((32, group), F32), exchange(gram, ("z", "core")), scaled)
    return out.T


def solution(mesh):
    rows, cols = mesh.devices.shape
    finer = Mesh(mesh.devices.reshape(rows, cols // 2, 2), ("row", "z", "core"))
    spec = P(("row", "z", "core"), None)
    return jax.shard_map(
        shards, mesh=finer, in_specs=(spec, spec), out_specs=spec, check_vma=False
    )
```

```python
import math

import jax
import jax.numpy as jnp
from jax import lax
from jax.experimental import pallas as pl
from jax.experimental.pallas import tpu as pltpu
from jax.sharding import Mesh
from jax.sharding import PartitionSpec as P

KERNEL_SCALE = 5.12
F32 = jnp.float32
BF16 = jnp.bfloat16
LANES = 128
PARAMS = pltpu.CompilerParams(vmem_limit_bytes=32 * 1024 * 1024)
REST = 32
WIDTH = 512
NORM, ONES, END = 64, 67, 70


def lane_of(shape):
    return lax.broadcasted_iota(jnp.int32, shape, len(shape) - 1)


def row_of(shape):
    return lax.broadcasted_iota(jnp.int32, shape, len(shape) - 2)


def roll(x, shift):
    shift %= LANES
    return pltpu.roll(x, shift, 1) if shift else x


def fold(x, place=0):
    h = x.shape[0] // 4
    group = lane_of((h, LANES)) // REST
    out = jnp.zeros((h, LANES), F32)
    for g in range(4):
        out = jnp.where(group == g, roll(x[g * h : (g + 1) * h], REST * (g - place)), out)
    return out


def unfold(pieces):
    h = pieces[0].shape[0]
    group = lane_of((h, LANES)) // REST
    rows = []
    for g in range(4):
        out = jnp.zeros((h, LANES), F32)
        for q, piece in enumerate(pieces):
            out = jnp.where(group == q, roll(piece, REST * (q - g)), out)
        rows.append(out)
    return jnp.concatenate(rows, axis=0)


def split(x):
    first = x.astype(BF16).astype(F32)
    second = (x - first).astype(BF16).astype(F32)
    return first, second, x - first - second


def widen(x):
    return jnp.concatenate([x, jnp.zeros((x.shape[0], LANES - x.shape[1]), x.dtype)], axis=1)


def main_and_rest(x):
    return x[:, 0:LANES], fold(widen(x[:, LANES : LANES + REST]))


def copies(ref, value):
    for i in range(ref.shape[0]):
        ref[i] = value


def pack_body(log_scale):
    def body(points_hbm, vectors_hbm, cols_hbm, rows_ref, points_ref, vectors_ref, block_ref, sems):
        loads = (
            pltpu.make_async_copy(points_hbm, points_ref, sems.at[0]),
            pltpu.make_async_copy(vectors_hbm, vectors_ref, sems.at[1]),
        )
        for load in loads:
            load.start()
        loads[0].wait()
        pts = points_ref[...].astype(F32)
        group = pts.shape[1]
        main, rest = main_and_rest(pts)
        rows_ref[...] = jnp.concatenate([main, rest], axis=0).astype(BF16)
        flat = jnp.concatenate([main, widen(pts[:, LANES:])], axis=1)
        norm = jnp.sum(flat * flat, axis=0, keepdims=True) * (-0.5 * log_scale)
        row = row_of((8, flat.shape[1]))
        extra = jnp.where((row >= ONES - NORM) & (row < END - NORM), 1.0, 0.0)
        for k, piece in enumerate(split(norm)):
            extra = jnp.where(row == k, piece, extra)
        blank = jnp.zeros((LANES - NORM - 8, flat.shape[1]), F32)
        flat = jnp.concatenate([flat, extra, blank], axis=0).T[0:group]
        loads[1].wait()
        main, rest = main_and_rest(vectors_ref[...].astype(F32))
        block_ref[...] = jnp.concatenate([flat, main, rest], axis=0).astype(BF16)
        count = cols_hbm.shape[0]
        sends = [
            pltpu.make_async_copy(block_ref, cols_hbm.at[i], sems.at[2 + i]) for i in range(count)
        ]
        for send in sends:
            send.start()
        for send in sends:
            send.wait()

    return body


def blocks_of(count):
    lanes = count * LANES
    main = [(at, WIDTH) for at in range(0, lanes, WIDTH)]
    return main, (lanes, lanes // 4)


def put_columns(cols_ref, left_ref, vec_ref):
    count = cols_ref.shape[0]
    total = left_ref.shape[0]
    for i in range(count):
        left_ref[i * LANES : (i + 1) * LANES, :] = cols_ref[i, 0:128]
        at = count * LANES + i * REST
        left_ref[at : at + REST, :] = cols_ref[i, 128:160]
    vec_ref[32:48, :] = jnp.where(row_of((16, total)) == 0, 1.0, 0.0).astype(BF16)
    for i in range(count):
        vec_ref[0:32, i * LANES : (i + 1) * LANES] = cols_ref[i, 160:192]
    for m in range(count // 4):
        rests = [cols_ref[4 * m + q, 192:200].astype(F32) for q in range(4)]
        at = (count + m) * LANES
        vec_ref[0:32, at : at + LANES] = unfold(rests).astype(BF16)


def put_rows(log_scale, rows_ref, core, right_ref):
    count = rows_ref.shape[0] // 2

    def put(tile, raw):
        at = tile * LANES
        scaled = raw * log_scale
        first = scaled.astype(BF16)
        norm = jnp.sum(raw * raw, axis=0, keepdims=True) * (-0.5 * log_scale)
        row = row_of((16, LANES))
        extra = jnp.where(row < ONES - NORM, 1.0, 0.0)
        for i, piece in enumerate(split(norm)):
            extra = jnp.where(row == ONES - NORM + i, piece, extra)
        right_ref[0:64, at : at + LANES] = first
        right_ref[64:80, at : at + LANES] = extra.astype(BF16)
        right_ref[80:128, at : at + LANES] = jnp.zeros((48, LANES), BF16)
        right_ref[128:192, at : at + LANES] = (scaled - first.astype(F32)).astype(BF16)
        right_ref[192:256, at : at + LANES] = jnp.zeros((64, LANES), BF16)

    for i in range(count):
        put(i, rows_ref[2 * i + core, 0:64].astype(F32))
    for m in range(count // 4):
        rests = [rows_ref[2 * (4 * m + q) + core, 64:80].astype(F32) for q in range(4)]
        put(count + m, unfold(rests))


def affinity_product(left_ref, right_ref, vec_ref, aff_ref, send_ref):
    total = left_ref.shape[0]
    main, rest = blocks_of(send_ref.shape[0])
    chunk = 512

    def weights(at, width):
        right = right_ref[:, at : at + width]
        for start in range(0, total, chunk):
            left = left_ref[start : start + chunk, :]
            power = jnp.dot(
                jnp.concatenate([left, left], axis=1), right, preferred_element_type=F32
            )
            aff_ref[start : start + chunk, at : at + width] = jnp.exp2(power).astype(BF16)

    def product(at, width):
        return jnp.dot(
            vec_ref[...], aff_ref[:, at : at + width], preferred_element_type=F32
        )

    def send_main(at, width):
        out = product(at, width)
        for k in range(width // LANES):
            tile = out[:, k * LANES : (k + 1) * LANES]
            send_ref[at // LANES + k, 0:32, :] = tile[0:32]
            send_ref[at // LANES + k, 40:41, :] = tile[32:33]

    def send_rest(at, width):
        out = product(at, width)
        row = row_of((8, LANES))
        for m in range(width // LANES):
            tile = out[:, m * LANES : (m + 1) * LANES]
            for q in range(4):
                send_ref[4 * m + q, 32:40, :] = fold(tile[0:32], q)
                degree = jnp.broadcast_to(roll(tile[32:40], -REST * q)[0:1], (8, LANES))
                send_ref[4 * m + q, 40:48, :] = jnp.where(row == 1, degree, 0.0)

    weights(*main[0])
    weights(*rest)
    send_rest(*rest)
    send_main(*main[0])
    for block in main[1:]:
        weights(*block)
        send_main(*block)


def away_body(right_ref, cols_ref, aff_ref, send_ref, left_ref, vec_ref):
    put_columns(cols_ref, left_ref, vec_ref)
    affinity_product(left_ref, right_ref, vec_ref, aff_ref, send_ref)


def rows_body(log_scale):
    def body(rows_ref, away_right_ref, home_right_ref):
        core = lax.axis_index("core")
        put_rows(log_scale, rows_ref, 1 - core, away_right_ref)
        put_rows(log_scale, rows_ref, core, home_right_ref)

    return body


def join_body(mine_ref, other_ref, out_ref):
    out_ref[...] = mine_ref[...] + other_ref[...]


def gram_of(x):
    return lax.dot_general(
        x,
        x,
        (((1,), (1,)), ((), ())),
        precision=lax.Precision.HIGHEST,
        preferred_element_type=F32,
    )


def whole(main, rest):
    return jnp.concatenate([main, unfold([rest])], axis=1)


def scale_body(recv_ref, spread_ref, degree_ref):
    total = jnp.sum(recv_ref[...], axis=0)
    rest = jnp.where(lane_of((1, LANES)) < REST, total[41:42], 0.0)
    rest = jnp.broadcast_to(rest, (8, LANES))
    rest = (rest + roll(rest, REST)) + (roll(rest, 2 * REST) + roll(rest, 3 * REST))
    degree_ref[0:8, :] = jnp.broadcast_to(total[40:41], (8, LANES))
    degree_ref[8:16, :] = rest
    main, rest = total[0:32] / total[40:41], total[32:40] / rest
    copies(spread_ref, jnp.concatenate([main, rest], axis=0))


def put_vectors(spread_ref, vec_ref):
    count = spread_ref.shape[0]

    def put(tile, value):
        first = value.astype(BF16)
        at = tile * LANES
        vec_ref[0:32, at : at + LANES] = first
        vec_ref[32:64, at : at + LANES] = (value - first.astype(F32)).astype(BF16)

    for i in range(count):
        put(i, spread_ref[i, 0:32, :])
    for m in range(count // 4):
        put(count + m, unfold([spread_ref[4 * m + q, 32:40, :] for q in range(4)]))


def second_product(aff_ref, vec_ref, send_ref):
    main, rest = blocks_of(send_ref.shape[0])

    def product(at, width):
        out = jnp.dot(vec_ref[...], aff_ref[:, at : at + width], preferred_element_type=F32)
        return out[0:32] + out[32:64]

    out = product(*rest)
    for m in range(rest[1] // LANES):
        for q in range(4):
            send_ref[4 * m + q, 32:40, :] = fold(out[:, m * LANES : (m + 1) * LANES], q)
    for at, width in main:
        out = product(at, width)
        for k in range(width // LANES):
            send_ref[at // LANES + k, 0:32, :] = out[:, k * LANES : (k + 1) * LANES]


def put_gram(gram, send_ref):
    for i in range(send_ref.shape[0]):
        send_ref[i, 40:48, :] = gram


def away_again_body(aff_ref, spread_ref, send_ref, vec_ref, gram_ref):
    put_vectors(spread_ref, vec_ref)
    vec = vec_ref[...]
    gram = lax.dot_general(vec, vec, (((1,), (1,)), ((), ())), preferred_element_type=F32)
    gram = gram[0:32] + gram[32:64]
    gram = fold(widen(gram[:, 0:32] + gram[:, 32:64]))
    gram_ref[...] = gram
    second_product(aff_ref, vec_ref, send_ref)
    put_gram(gram, send_ref)


def home_again_body(aff_ref, vec_ref, gram_ref, send_ref):
    second_product(aff_ref, vec_ref, send_ref)
    put_gram(gram_ref[...], send_ref)


def solved(gram, right):
    size = gram.shape[0]
    wide = right.shape[1] // LANES
    columns = [
        jnp.broadcast_to(gram[8 * (k // 8) :, k : k + 1], (size - 8 * (k // 8), LANES))
        for k in range(size)
    ]
    rows = [right[8 * g : 8 * g + 8] for g in range(size // 8)]
    for j in range(size):
        base, at = j // 8, j % 8
        pivot = columns[j][at : at + 1]
        scale = lax.rsqrt(pivot)
        scale = scale * (1.5 - 0.5 * pivot * scale * scale)
        factor = columns[j] * scale
        for k in range(j + 1, size):
            skip = 8 * (k // 8 - base)
            mine = factor[k - 8 * base : k - 8 * base + 1]
            columns[k] = columns[k] - factor[skip:] * mine
        top = rows[base][at : at + 1] * jnp.concatenate([scale] * wide, axis=1)
        for g in range(base, size // 8):
            part = factor[8 * (g - base) : 8 * (g - base) + 8]
            if g == base:
                row = row_of((8, LANES))
                part = jnp.where(row > at, part, 0.0)
            new = rows[g] - jnp.concatenate([part] * wide, axis=1) * top
            if g == base:
                new = jnp.where(row_of(new.shape) == at, top, new)
            rows[g] = new
    return jnp.concatenate(rows, axis=0)


def middle_body(points):
    def body(recv_ref, degree_ref, scaled_ref, gram_ref):
        total = jnp.sum(recv_ref[...], axis=0)
        main = total[0:32] / degree_ref[0:1, :]
        rest = total[32:40] / degree_ref[8:16, :]
        scaled = solved(unfold([total[40:48]]) / points, whole(main, rest))
        scaled_ref[...] = scaled
        copies(gram_ref, fold(widen(gram_of(scaled))))

    return body


def again_body(recv_ref, gram_ref):
    copies(gram_ref, jnp.sum(recv_ref[...], axis=0))


def last_body(points):
    def body(recv_ref, scaled_ref, out_ref):
        gram = unfold([jnp.sum(recv_ref[...], axis=0)]) / points
        out_ref[...] = solved(gram, scaled_ref[...])[:, 0 : out_ref.shape[1]]

    return body


def shards(points, start_vectors):
    group, features = points.shape
    row, half, cores = lax.axis_size("row"), lax.axis_size("z"), lax.axis_size("core")
    col = half * cores
    total = group * row * col
    log_scale = 2.0 * KERNEL_SCALE / features * math.log2(math.e)
    lanes = half * group
    right_shape = pltpu.VMEM((256, lanes), BF16)
    shape = jax.ShapeDtypeStruct

    def exchange(x, axis):
        return lax.all_to_all(x, axis, 0, 0, tiled=True)

    def swap(x):
        return lax.ppermute(x, "core", [(0, 1), (1, 0)])

    def call(body, out_shape, *args, scratch=(), **kwargs):
        return pl.pallas_call(
            body, out_shape=out_shape, scratch_shapes=scratch, compiler_params=PARAMS, **kwargs
        )(*args)

    hbm_space = pl.BlockSpec(memory_space=pltpu.HBM)
    cols, rows = call(
        pack_body(log_scale),
        (shape((row, group + 40, LANES), BF16), pltpu.VMEM((80, LANES), BF16)),
        pltpu.with_memory_space_constraint(points.T, pltpu.HBM),
        pltpu.with_memory_space_constraint(start_vectors.T, pltpu.HBM),
        scratch=(
            pltpu.VMEM((features, group), BF16),
            pltpu.VMEM((start_vectors.shape[1], group), BF16),
            pltpu.VMEM((group + 40, LANES), BF16),
            pltpu.SemaphoreType.DMA((2 + row,)),
        ),
        in_specs=[hbm_space, hbm_space],
        out_specs=(hbm_space, pl.BlockSpec(memory_space=pltpu.VMEM)),
    )
    cols = exchange(cols, "row")
    rows = lax.all_gather(rows, ("z", "core"))
    away_right, home_right = call(rows_body(log_scale), (right_shape, right_shape), rows)
    aff_shape = pltpu.VMEM((row * group, lanes), BF16)
    send_shape = shape((half, 48, LANES), F32)
    away_aff, away_send, left, vec = call(
        away_body,
        (
            aff_shape,
            send_shape,
            pltpu.VMEM((row * group, LANES), BF16),
            pltpu.VMEM((48, row * group), BF16),
        ),
        away_right,
        cols,
    )
    other = swap(away_send)
    home_aff, home_send = call(affinity_product, (aff_shape, send_shape), left, home_right, vec)
    send = call(join_body, send_shape, home_send, other)
    spread, degree = call(
        scale_body, (shape((row, 40, LANES), F32), shape((16, LANES), F32)), exchange(send, "z")
    )
    away_send, vec, gram = call(
        away_again_body,
        (send_shape, pltpu.VMEM((64, row * group), BF16), pltpu.VMEM((8, LANES), F32)),
        away_aff,
        exchange(spread, "row"),
    )
    other = swap(away_send)
    home_send = call(home_again_body, send_shape, home_aff, vec, gram)
    send = call(join_body, send_shape, home_send, other)
    scaled, gram = call(
        middle_body(total),
        (shape((32, 2 * LANES), F32), shape((row, 8, LANES), F32)),
        exchange(send, "z"),
        degree,
    )
    gram = call(again_body, shape((col, 8, LANES), F32), exchange(gram, "row"))
    out = call(last_body(total), shape((32, group), F32), exchange(gram, ("z", "core")), scaled)
    return out.T


def solution(mesh):
    rows, cols = mesh.devices.shape
    finer = Mesh(mesh.devices.reshape(rows, cols // 2, 2), ("row", "z", "core"))
    spec = P(("row", "z", "core"), None)
    return jax.shard_map(
        shards, mesh=finer, in_specs=(spec, spec), out_specs=spec, check_vma=False
    )
```

```python
import math

import jax
import jax.numpy as jnp
from jax import lax
from jax.experimental import pallas as pl
from jax.experimental.pallas import tpu as pltpu
from jax.sharding import Mesh
from jax.sharding import PartitionSpec as P

KERNEL_SCALE = 5.12
F32 = jnp.float32
BF16 = jnp.bfloat16
LANES = 128
PARAMS = pltpu.CompilerParams(vmem_limit_bytes=32 * 1024 * 1024)
REST = 32
WIDTH = 512
NORM, ONES, END = 64, 67, 70


def lane_of(shape):
    return lax.broadcasted_iota(jnp.int32, shape, len(shape) - 1)


def row_of(shape):
    return lax.broadcasted_iota(jnp.int32, shape, len(shape) - 2)


def roll(x, shift):
    shift %= LANES
    return pltpu.roll(x, shift, 1) if shift else x


def fold(x, place=0):
    h = x.shape[0] // 4
    group = lane_of((h, LANES)) // REST
    out = jnp.zeros((h, LANES), F32)
    for g in range(4):
        out = jnp.where(group == g, roll(x[g * h : (g + 1) * h], REST * (g - place)), out)
    return out


def unfold(pieces):
    h = pieces[0].shape[0]
    group = lane_of((h, LANES)) // REST
    rows = []
    for g in range(4):
        out = jnp.zeros((h, LANES), F32)
        for q, piece in enumerate(pieces):
            out = jnp.where(group == q, roll(piece, REST * (q - g)), out)
        rows.append(out)
    return jnp.concatenate(rows, axis=0)


def split(x):
    first = x.astype(BF16).astype(F32)
    second = (x - first).astype(BF16).astype(F32)
    return first, second, x - first - second


def widen(x):
    return jnp.concatenate([x, jnp.zeros((x.shape[0], LANES - x.shape[1]), x.dtype)], axis=1)


def main_and_rest(x):
    return x[:, 0:LANES], fold(widen(x[:, LANES : LANES + REST]))


def copies(ref, value):
    for i in range(ref.shape[0]):
        ref[i] = value


def pack_body(log_scale):
    def body(points_hbm, vectors_hbm, cols_hbm, rows_ref, points_ref, vectors_ref, block_ref, sems):
        loads = (
            pltpu.make_async_copy(points_hbm, points_ref, sems.at[0]),
            pltpu.make_async_copy(vectors_hbm, vectors_ref, sems.at[1]),
        )
        for load in loads:
            load.start()
        loads[0].wait()
        pts = points_ref[...].astype(F32)
        group = pts.shape[1]
        main, rest = main_and_rest(pts)
        rows_ref[...] = jnp.concatenate([main, rest], axis=0).astype(BF16)
        flat = jnp.concatenate([main, widen(pts[:, LANES:])], axis=1)
        norm = jnp.sum(flat * flat, axis=0, keepdims=True) * (-0.5 * log_scale)
        row = row_of((8, flat.shape[1]))
        extra = jnp.where((row >= ONES - NORM) & (row < END - NORM), 1.0, 0.0)
        for k, piece in enumerate(split(norm)):
            extra = jnp.where(row == k, piece, extra)
        blank = jnp.zeros((LANES - NORM - 8, flat.shape[1]), F32)
        flat = jnp.concatenate([flat, extra, blank], axis=0).T[0:group]
        loads[1].wait()
        main, rest = main_and_rest(vectors_ref[...].astype(F32))
        block_ref[...] = jnp.concatenate([flat, main, rest], axis=0).astype(BF16)
        count = cols_hbm.shape[0]
        sends = [
            pltpu.make_async_copy(block_ref, cols_hbm.at[i], sems.at[2 + i]) for i in range(count)
        ]
        for send in sends:
            send.start()
        for send in sends:
            send.wait()

    return body


def blocks_of(count):
    lanes = count * LANES
    main = [(at, WIDTH) for at in range(0, lanes, WIDTH)]
    return main, (lanes, lanes // 4)


def put_columns(cols_ref, left_ref, vec_ref):
    count = cols_ref.shape[0]
    total = left_ref.shape[0]
    for i in range(count):
        left_ref[i * LANES : (i + 1) * LANES, :] = cols_ref[i, 0:128]
        at = count * LANES + i * REST
        left_ref[at : at + REST, :] = cols_ref[i, 128:160]
    vec_ref[32:48, :] = jnp.where(row_of((16, total)) == 0, 1.0, 0.0).astype(BF16)
    for i in range(count):
        vec_ref[0:32, i * LANES : (i + 1) * LANES] = cols_ref[i, 160:192]
    for m in range(count // 4):
        rests = [cols_ref[4 * m + q, 192:200].astype(F32) for q in range(4)]
        at = (count + m) * LANES
        vec_ref[0:32, at : at + LANES] = unfold(rests).astype(BF16)


def put_rows(log_scale, rows_ref, core, right_ref):
    count = rows_ref.shape[0] // 2

    def put(tile, raw):
        at = tile * LANES
        scaled = raw * log_scale
        first = scaled.astype(BF16)
        norm = jnp.sum(raw * raw, axis=0, keepdims=True) * (-0.5 * log_scale)
        row = row_of((16, LANES))
        extra = jnp.where(row < ONES - NORM, 1.0, 0.0)
        for i, piece in enumerate(split(norm)):
            extra = jnp.where(row == ONES - NORM + i, piece, extra)
        right_ref[0:64, at : at + LANES] = first
        right_ref[64:80, at : at + LANES] = extra.astype(BF16)
        right_ref[80:128, at : at + LANES] = jnp.zeros((48, LANES), BF16)
        right_ref[128:192, at : at + LANES] = (scaled - first.astype(F32)).astype(BF16)
        right_ref[192:256, at : at + LANES] = jnp.zeros((64, LANES), BF16)

    for i in range(count):
        put(i, rows_ref[2 * i + core, 0:64].astype(F32))
    for m in range(count // 4):
        rests = [rows_ref[2 * (4 * m + q) + core, 64:80].astype(F32) for q in range(4)]
        put(count + m, unfold(rests))


def affinity_product(left_ref, right_ref, vec_ref, aff_ref, send_ref):
    total = left_ref.shape[0]
    main, rest = blocks_of(send_ref.shape[0])
    chunk = 512

    def weights(at, width):
        right = right_ref[:, at : at + width]
        for start in range(0, total, chunk):
            left = left_ref[start : start + chunk, :]
            power = jnp.dot(
                jnp.concatenate([left, left], axis=1), right, preferred_element_type=F32
            )
            aff_ref[start : start + chunk, at : at + width] = jnp.exp2(power).astype(BF16)

    def product(at, width):
        return jnp.dot(
            vec_ref[...], aff_ref[:, at : at + width], preferred_element_type=F32
        )

    def send_main(at, width):
        out = product(at, width)
        for k in range(width // LANES):
            tile = out[:, k * LANES : (k + 1) * LANES]
            send_ref[at // LANES + k, 0:32, :] = tile[0:32]
            send_ref[at // LANES + k, 40:41, :] = tile[32:33]

    def send_rest(at, width):
        out = product(at, width)
        row = row_of((8, LANES))
        for m in range(width // LANES):
            tile = out[:, m * LANES : (m + 1) * LANES]
            for q in range(4):
                send_ref[4 * m + q, 32:40, :] = fold(tile[0:32], q)
                degree = jnp.broadcast_to(roll(tile[32:40], -REST * q)[0:1], (8, LANES))
                send_ref[4 * m + q, 40:48, :] = jnp.where(row == 1, degree, 0.0)

    weights(*main[0])
    weights(*rest)
    send_rest(*rest)
    send_main(*main[0])
    for block in main[1:]:
        weights(*block)
        send_main(*block)


def away_body(right_ref, cols_ref, aff_ref, send_ref, left_ref, vec_ref):
    put_columns(cols_ref, left_ref, vec_ref)
    affinity_product(left_ref, right_ref, vec_ref, aff_ref, send_ref)


def rows_body(log_scale):
    def body(rows_ref, away_right_ref, home_right_ref):
        core = lax.axis_index("core")
        put_rows(log_scale, rows_ref, 1 - core, away_right_ref)
        put_rows(log_scale, rows_ref, core, home_right_ref)

    return body


def join_body(mine_ref, other_ref, out_ref):
    out_ref[...] = mine_ref[...] + other_ref[...]


def gram_of(x):
    return lax.dot_general(
        x,
        x,
        (((1,), (1,)), ((), ())),
        precision=lax.Precision.HIGHEST,
        preferred_element_type=F32,
    )


def whole(main, rest):
    return jnp.concatenate([main, unfold([rest])], axis=1)


def scale_body(recv_ref, spread_ref, degree_ref):
    total = jnp.sum(recv_ref[...], axis=0)
    rest = jnp.where(lane_of((1, LANES)) < REST, total[41:42], 0.0)
    rest = jnp.broadcast_to(rest, (8, LANES))
    rest = (rest + roll(rest, REST)) + (roll(rest, 2 * REST) + roll(rest, 3 * REST))
    degree_ref[0:8, :] = jnp.broadcast_to(total[40:41], (8, LANES))
    degree_ref[8:16, :] = rest
    main, rest = total[0:32] / total[40:41], total[32:40] / rest
    copies(spread_ref, jnp.concatenate([main, rest], axis=0))


def put_vectors(spread_ref, vec_ref):
    count = spread_ref.shape[0]

    def put(tile, value):
        first = value.astype(BF16)
        at = tile * LANES
        vec_ref[0:32, at : at + LANES] = first
        vec_ref[32:64, at : at + LANES] = (value - first.astype(F32)).astype(BF16)

    for i in range(count):
        put(i, spread_ref[i, 0:32, :])
    for m in range(count // 4):
        put(count + m, unfold([spread_ref[4 * m + q, 32:40, :] for q in range(4)]))


def second_product(aff_ref, vec_ref, send_ref):
    main, rest = blocks_of(send_ref.shape[0])

    def product(at, width):
        out = jnp.dot(vec_ref[...], aff_ref[:, at : at + width], preferred_element_type=F32)
        return out[0:32] + out[32:64]

    out = product(*rest)
    for m in range(rest[1] // LANES):
        for q in range(4):
            send_ref[4 * m + q, 32:40, :] = fold(out[:, m * LANES : (m + 1) * LANES], q)
    for at, width in main:
        out = product(at, width)
        for k in range(width // LANES):
            send_ref[at // LANES + k, 0:32, :] = out[:, k * LANES : (k + 1) * LANES]


def put_gram(gram, send_ref):
    for i in range(send_ref.shape[0]):
        send_ref[i, 40:48, :] = gram


def away_again_body(aff_ref, spread_ref, send_ref, vec_ref, gram_ref):
    put_vectors(spread_ref, vec_ref)
    vec = vec_ref[...]
    gram = lax.dot_general(vec, vec, (((1,), (1,)), ((), ())), preferred_element_type=F32)
    gram = gram[0:32] + gram[32:64]
    gram = fold(widen(gram[:, 0:32] + gram[:, 32:64]))
    gram_ref[...] = gram
    second_product(aff_ref, vec_ref, send_ref)
    put_gram(gram, send_ref)


def home_again_body(aff_ref, vec_ref, gram_ref, send_ref):
    second_product(aff_ref, vec_ref, send_ref)
    put_gram(gram_ref[...], send_ref)


def solved(gram, right):
    size = 4 * gram.shape[0]
    wide = right.shape[1] // LANES
    columns = [
        jnp.concatenate(
            [
                jnp.broadcast_to(gram[:, REST * g + k : REST * g + k + 1], (8, LANES))
                for g in range(k // 8, 4)
            ],
            axis=0,
        )
        for k in range(size)
    ]
    rows = [right[8 * g : 8 * g + 8] for g in range(size // 8)]
    for j in range(size):
        base, at = j // 8, j % 8
        pivot = columns[j][at : at + 1]
        scale = lax.rsqrt(pivot)
        scale = scale * (1.5 - 0.5 * pivot * scale * scale)
        factor = columns[j] * scale
        for k in range(j + 1, size):
            skip = 8 * (k // 8 - base)
            mine = factor[k - 8 * base : k - 8 * base + 1]
            columns[k] = columns[k] - factor[skip:] * mine
        top = rows[base][at : at + 1] * jnp.concatenate([scale] * wide, axis=1)
        for g in range(base, size // 8):
            part = factor[8 * (g - base) : 8 * (g - base) + 8]
            if g == base:
                row = row_of((8, LANES))
                part = jnp.where(row > at, part, 0.0)
            new = rows[g] - jnp.concatenate([part] * wide, axis=1) * top
            if g == base:
                new = jnp.where(row_of(new.shape) == at, top, new)
            rows[g] = new
    return jnp.concatenate(rows, axis=0)


def middle_body(points):
    def body(recv_ref, degree_ref, scaled_ref, gram_ref):
        total = jnp.sum(recv_ref[...], axis=0)
        main = total[0:32] / degree_ref[0:1, :]
        rest = total[32:40] / degree_ref[8:16, :]
        scaled = solved(total[40:48] / points, whole(main, rest))
        scaled_ref[...] = scaled
        copies(gram_ref, fold(widen(gram_of(scaled))))

    return body


def again_body(recv_ref, gram_ref):
    copies(gram_ref, jnp.sum(recv_ref[...], axis=0))


def last_body(points):
    def body(recv_ref, scaled_ref, out_ref):
        gram = jnp.sum(recv_ref[...], axis=0) / points
        out_ref[...] = solved(gram, scaled_ref[...])[:, 0 : out_ref.shape[1]]

    return body


def shards(points, start_vectors):
    group, features = points.shape
    row, half, cores = lax.axis_size("row"), lax.axis_size("z"), lax.axis_size("core")
    col = half * cores
    total = group * row * col
    log_scale = 2.0 * KERNEL_SCALE / features * math.log2(math.e)
    lanes = half * group
    right_shape = pltpu.VMEM((256, lanes), BF16)
    shape = jax.ShapeDtypeStruct

    def exchange(x, axis):
        return lax.all_to_all(x, axis, 0, 0, tiled=True)

    def swap(x):
        return lax.ppermute(x, "core", [(0, 1), (1, 0)])

    def call(body, out_shape, *args, scratch=(), **kwargs):
        return pl.pallas_call(
            body, out_shape=out_shape, scratch_shapes=scratch, compiler_params=PARAMS, **kwargs
        )(*args)

    hbm_space = pl.BlockSpec(memory_space=pltpu.HBM)
    cols, rows = call(
        pack_body(log_scale),
        (shape((row, group + 40, LANES), BF16), pltpu.VMEM((80, LANES), BF16)),
        pltpu.with_memory_space_constraint(points.T, pltpu.HBM),
        pltpu.with_memory_space_constraint(start_vectors.T, pltpu.HBM),
        scratch=(
            pltpu.VMEM((features, group), BF16),
            pltpu.VMEM((start_vectors.shape[1], group), BF16),
            pltpu.VMEM((group + 40, LANES), BF16),
            pltpu.SemaphoreType.DMA((2 + row,)),
        ),
        in_specs=[hbm_space, hbm_space],
        out_specs=(hbm_space, pl.BlockSpec(memory_space=pltpu.VMEM)),
    )
    cols = exchange(cols, "row")
    rows = lax.all_gather(rows, ("z", "core"))
    away_right, home_right = call(rows_body(log_scale), (right_shape, right_shape), rows)
    aff_shape = pltpu.VMEM((row * group, lanes), BF16)
    send_shape = shape((half, 48, LANES), F32)
    away_aff, away_send, left, vec = call(
        away_body,
        (
            aff_shape,
            send_shape,
            pltpu.VMEM((row * group, LANES), BF16),
            pltpu.VMEM((48, row * group), BF16),
        ),
        away_right,
        cols,
    )
    other = swap(away_send)
    home_aff, home_send = call(affinity_product, (aff_shape, send_shape), left, home_right, vec)
    send = call(join_body, send_shape, home_send, other)
    spread, degree = call(
        scale_body, (shape((row, 40, LANES), F32), shape((16, LANES), F32)), exchange(send, "z")
    )
    away_send, vec, gram = call(
        away_again_body,
        (send_shape, pltpu.VMEM((64, row * group), BF16), pltpu.VMEM((8, LANES), F32)),
        away_aff,
        exchange(spread, "row"),
    )
    other = swap(away_send)
    home_send = call(home_again_body, send_shape, home_aff, vec, gram)
    send = call(join_body, send_shape, home_send, other)
    scaled, gram = call(
        middle_body(total),
        (shape((32, 2 * LANES), F32), shape((col, 8, LANES), F32)),
        exchange(send, "z"),
        degree,
    )
    gram = exchange(gram, ("z", "core"))
    gram = call(again_body, shape((row, 8, LANES), F32), gram)
    out = call(last_body(total), shape((32, group), F32), exchange(gram, "row"), scaled)
    return out.T


def solution(mesh):
    rows, cols = mesh.devices.shape
    finer = Mesh(mesh.devices.reshape(rows, cols // 2, 2), ("row", "z", "core"))
    spec = P(("row", "z", "core"), None)
    return jax.shard_map(
        shards, mesh=finer, in_specs=(spec, spec), out_specs=spec, check_vma=False
    )
```

```python
import math

import jax
import jax.numpy as jnp
from jax import lax
from jax.experimental import pallas as pl
from jax.experimental.pallas import tpu as pltpu
from jax.sharding import Mesh
from jax.sharding import PartitionSpec as P

KERNEL_SCALE = 5.12
F32 = jnp.float32
BF16 = jnp.bfloat16
LANES = 128
PARAMS = pltpu.CompilerParams(vmem_limit_bytes=32 * 1024 * 1024)
REST = 32
WIDTH = 512
NORM, ONES, END = 64, 67, 70


def lane_of(shape):
    return lax.broadcasted_iota(jnp.int32, shape, len(shape) - 1)


def row_of(shape):
    return lax.broadcasted_iota(jnp.int32, shape, len(shape) - 2)


def roll(x, shift):
    shift %= LANES
    return pltpu.roll(x, shift, 1) if shift else x


def fold(x, place=0):
    h = x.shape[0] // 4
    group = lane_of((h, LANES)) // REST
    out = jnp.zeros((h, LANES), F32)
    for g in range(4):
        out = jnp.where(group == g, roll(x[g * h : (g + 1) * h], REST * (g - place)), out)
    return out


def unfold(pieces):
    h = pieces[0].shape[0]
    group = lane_of((h, LANES)) // REST
    rows = []
    for g in range(4):
        out = jnp.zeros((h, LANES), F32)
        for q, piece in enumerate(pieces):
            out = jnp.where(group == q, roll(piece, REST * (q - g)), out)
        rows.append(out)
    return jnp.concatenate(rows, axis=0)


def split(x):
    first = x.astype(BF16).astype(F32)
    second = (x - first).astype(BF16).astype(F32)
    return first, second, x - first - second


def widen(x):
    return jnp.concatenate([x, jnp.zeros((x.shape[0], LANES - x.shape[1]), x.dtype)], axis=1)


def main_and_rest(x):
    return x[:, 0:LANES], fold(widen(x[:, LANES : LANES + REST]))


def copies(ref, value):
    for i in range(ref.shape[0]):
        ref[i] = value


def pack_body(log_scale):
    def body(points_hbm, vectors_hbm, cols_hbm, rows_ref, points_ref, vectors_ref, block_ref, sems):
        loads = (
            pltpu.make_async_copy(points_hbm, points_ref, sems.at[0]),
            pltpu.make_async_copy(vectors_hbm, vectors_ref, sems.at[1]),
        )
        for load in loads:
            load.start()
        loads[0].wait()
        pts = points_ref[...].astype(F32)
        group = pts.shape[1]
        main, rest = main_and_rest(pts)
        rows_ref[...] = jnp.concatenate([main, rest], axis=0).astype(BF16)
        flat = jnp.concatenate([main, widen(pts[:, LANES:])], axis=1)
        norm = jnp.sum(flat * flat, axis=0, keepdims=True) * (-0.5 * log_scale)
        row = row_of((8, flat.shape[1]))
        extra = jnp.where((row >= ONES - NORM) & (row < END - NORM), 1.0, 0.0)
        for k, piece in enumerate(split(norm)):
            extra = jnp.where(row == k, piece, extra)
        blank = jnp.zeros((LANES - NORM - 8, flat.shape[1]), F32)
        flat = jnp.concatenate([flat, extra, blank], axis=0).T[0:group]
        loads[1].wait()
        main, rest = main_and_rest(vectors_ref[...].astype(F32))
        block_ref[...] = jnp.concatenate([flat, main, rest], axis=0).astype(BF16)
        count = cols_hbm.shape[0]
        sends = [
            pltpu.make_async_copy(block_ref, cols_hbm.at[i], sems.at[2 + i]) for i in range(count)
        ]
        for send in sends:
            send.start()
        for send in sends:
            send.wait()

    return body


def blocks_of(count):
    lanes = count * LANES
    main = [(at, WIDTH) for at in range(0, lanes, WIDTH)]
    return main, (lanes, lanes // 4)


def put_columns(cols_ref, left_ref, vec_ref):
    count = cols_ref.shape[0]
    total = left_ref.shape[0]
    for i in range(count):
        left_ref[i * LANES : (i + 1) * LANES, :] = cols_ref[i, 0:128]
        at = count * LANES + i * REST
        left_ref[at : at + REST, :] = cols_ref[i, 128:160]
    vec_ref[32:48, :] = jnp.where(row_of((16, total)) == 0, 1.0, 0.0).astype(BF16)
    for i in range(count):
        vec_ref[0:32, i * LANES : (i + 1) * LANES] = cols_ref[i, 160:192]
    for m in range(count // 4):
        rests = [cols_ref[4 * m + q, 192:200].astype(F32) for q in range(4)]
        at = (count + m) * LANES
        vec_ref[0:32, at : at + LANES] = unfold(rests).astype(BF16)


def put_rows(log_scale, rows_ref, core, right_ref):
    count = rows_ref.shape[0] // 2

    def put(tile, raw):
        at = tile * LANES
        scaled = raw * log_scale
        first = scaled.astype(BF16)
        norm = jnp.sum(raw * raw, axis=0, keepdims=True) * (-0.5 * log_scale)
        row = row_of((16, LANES))
        extra = jnp.where(row < ONES - NORM, 1.0, 0.0)
        for i, piece in enumerate(split(norm)):
            extra = jnp.where(row == ONES - NORM + i, piece, extra)
        right_ref[0:64, at : at + LANES] = first
        right_ref[64:80, at : at + LANES] = extra.astype(BF16)
        right_ref[80:128, at : at + LANES] = jnp.zeros((48, LANES), BF16)
        right_ref[128:192, at : at + LANES] = (scaled - first.astype(F32)).astype(BF16)
        right_ref[192:256, at : at + LANES] = jnp.zeros((64, LANES), BF16)

    for i in range(count):
        put(i, rows_ref[2 * i + core, 0:64].astype(F32))
    for m in range(count // 4):
        rests = [rows_ref[2 * (4 * m + q) + core, 64:80].astype(F32) for q in range(4)]
        put(count + m, unfold(rests))


def affinity_product(left_ref, right_ref, vec_ref, aff_ref, send_ref):
    total = left_ref.shape[0]
    main, rest = blocks_of(send_ref.shape[0])
    chunk = 512

    def weights(at, width):
        right = right_ref[:, at : at + width]
        for start in range(0, total, chunk):
            left = left_ref[start : start + chunk, :]
            power = jnp.dot(
                jnp.concatenate([left, left], axis=1), right, preferred_element_type=F32
            )
            aff_ref[start : start + chunk, at : at + width] = jnp.exp2(power).astype(BF16)

    def product(at, width):
        return jnp.dot(
            vec_ref[...], aff_ref[:, at : at + width], preferred_element_type=F32
        )

    def send_main(at, width):
        out = product(at, width)
        for k in range(width // LANES):
            tile = out[:, k * LANES : (k + 1) * LANES]
            send_ref[at // LANES + k, 0:32, :] = tile[0:32]
            send_ref[at // LANES + k, 40:41, :] = tile[32:33]

    def send_rest(at, width):
        out = product(at, width)
        row = row_of((8, LANES))
        for m in range(width // LANES):
            tile = out[:, m * LANES : (m + 1) * LANES]
            for q in range(4):
                send_ref[4 * m + q, 32:40, :] = fold(tile[0:32], q)
                degree = jnp.broadcast_to(roll(tile[32:40], -REST * q)[0:1], (8, LANES))
                send_ref[4 * m + q, 40:48, :] = jnp.where(row == 1, degree, 0.0)

    weights(*main[0])
    weights(*rest)
    send_rest(*rest)
    send_main(*main[0])
    for block in main[1:]:
        weights(*block)
        send_main(*block)


def away_body(log_scale):
    def body(rows_ref, cols_ref, aff_ref, send_ref, left_ref, vec_ref, right_ref):
        put_rows(log_scale, rows_ref, 1 - lax.axis_index("core"), right_ref)
        put_columns(cols_ref, left_ref, vec_ref)
        affinity_product(left_ref, right_ref, vec_ref, aff_ref, send_ref)

    return body


def home_body(log_scale):
    def body(rows_ref, left_ref, vec_ref, aff_ref, send_ref, right_ref):
        put_rows(log_scale, rows_ref, lax.axis_index("core"), right_ref)
        affinity_product(left_ref, right_ref, vec_ref, aff_ref, send_ref)

    return body


def join_body(mine_ref, other_ref, out_ref):
    out_ref[...] = mine_ref[...] + other_ref[...]


def gram_of(x):
    return lax.dot_general(
        x,
        x,
        (((1,), (1,)), ((), ())),
        precision=lax.Precision.HIGHEST,
        preferred_element_type=F32,
    )


def whole(main, rest):
    return jnp.concatenate([main, unfold([rest])], axis=1)


def scale_body(recv_ref, spread_ref, degree_ref):
    total = jnp.sum(recv_ref[...], axis=0)
    rest = jnp.where(lane_of((1, LANES)) < REST, total[41:42], 0.0)
    rest = jnp.broadcast_to(rest, (8, LANES))
    rest = (rest + roll(rest, REST)) + (roll(rest, 2 * REST) + roll(rest, 3 * REST))
    degree_ref[0:8, :] = jnp.broadcast_to(total[40:41], (8, LANES))
    degree_ref[8:16, :] = rest
    main, rest = total[0:32] / total[40:41], total[32:40] / rest
    copies(spread_ref, jnp.concatenate([main, rest], axis=0))


def put_vectors(spread_ref, vec_ref):
    count = spread_ref.shape[0]

    def put(tile, value):
        first = value.astype(BF16)
        at = tile * LANES
        vec_ref[0:32, at : at + LANES] = first
        vec_ref[32:64, at : at + LANES] = (value - first.astype(F32)).astype(BF16)

    for i in range(count):
        put(i, spread_ref[i, 0:32, :])
    for m in range(count // 4):
        put(count + m, unfold([spread_ref[4 * m + q, 32:40, :] for q in range(4)]))


def second_product(aff_ref, vec_ref, send_ref):
    main, rest = blocks_of(send_ref.shape[0])

    def product(at, width):
        out = jnp.dot(vec_ref[...], aff_ref[:, at : at + width], preferred_element_type=F32)
        return out[0:32] + out[32:64]

    out = product(*rest)
    for m in range(rest[1] // LANES):
        for q in range(4):
            send_ref[4 * m + q, 32:40, :] = fold(out[:, m * LANES : (m + 1) * LANES], q)
    for at, width in main:
        out = product(at, width)
        for k in range(width // LANES):
            send_ref[at // LANES + k, 0:32, :] = out[:, k * LANES : (k + 1) * LANES]


def put_gram(gram, send_ref):
    for i in range(send_ref.shape[0]):
        send_ref[i, 40:48, :] = gram


def away_again_body(aff_ref, spread_ref, send_ref, vec_ref, gram_ref):
    put_vectors(spread_ref, vec_ref)
    vec = vec_ref[...]
    gram = lax.dot_general(vec, vec, (((1,), (1,)), ((), ())), preferred_element_type=F32)
    gram = gram[0:32] + gram[32:64]
    gram = fold(widen(gram[:, 0:32] + gram[:, 32:64]))
    gram_ref[...] = gram
    second_product(aff_ref, vec_ref, send_ref)
    put_gram(gram, send_ref)


def home_again_body(aff_ref, vec_ref, gram_ref, send_ref):
    second_product(aff_ref, vec_ref, send_ref)
    put_gram(gram_ref[...], send_ref)


def solved(gram, right):
    size = 4 * gram.shape[0]
    wide = right.shape[1] // LANES
    columns = [
        jnp.concatenate(
            [
                jnp.broadcast_to(gram[:, REST * g + k : REST * g + k + 1], (8, LANES))
                for g in range(k // 8, 4)
            ],
            axis=0,
        )
        for k in range(size)
    ]
    rows = [right[8 * g : 8 * g + 8] for g in range(size // 8)]
    for j in range(size):
        base, at = j // 8, j % 8
        pivot = columns[j][at : at + 1]
        scale = lax.rsqrt(pivot)
        scale = scale * (1.5 - 0.5 * pivot * scale * scale)
        factor = columns[j] * scale
        for k in range(j + 1, size):
            skip = 8 * (k // 8 - base)
            mine = factor[k - 8 * base : k - 8 * base + 1]
            columns[k] = columns[k] - factor[skip:] * mine
        top = rows[base][at : at + 1] * jnp.concatenate([scale] * wide, axis=1)
        for g in range(base, size // 8):
            part = factor[8 * (g - base) : 8 * (g - base) + 8]
            if g == base:
                row = row_of((8, LANES))
                part = jnp.where(row > at, part, 0.0)
            new = rows[g] - jnp.concatenate([part] * wide, axis=1) * top
            if g == base:
                new = jnp.where(row_of(new.shape) == at, top, new)
            rows[g] = new
    return jnp.concatenate(rows, axis=0)


def middle_body(points):
    def body(recv_ref, degree_ref, scaled_ref, gram_ref):
        total = jnp.sum(recv_ref[...], axis=0)
        main = total[0:32] / degree_ref[0:1, :]
        rest = total[32:40] / degree_ref[8:16, :]
        scaled = solved(total[40:48] / points, whole(main, rest))
        scaled_ref[...] = scaled
        copies(gram_ref, fold(widen(gram_of(scaled))))

    return body


def again_body(recv_ref, gram_ref):
    copies(gram_ref, jnp.sum(recv_ref[...], axis=0))


def last_body(points):
    def body(recv_ref, scaled_ref, out_ref):
        gram = jnp.sum(recv_ref[...], axis=0) / points
        out_ref[...] = solved(gram, scaled_ref[...])[:, 0 : out_ref.shape[1]]

    return body


def shards(points, start_vectors):
    group, features = points.shape
    row, half, cores = lax.axis_size("row"), lax.axis_size("z"), lax.axis_size("core")
    col = half * cores
    total = group * row * col
    log_scale = 2.0 * KERNEL_SCALE / features * math.log2(math.e)
    lanes = half * group
    right_shape = pltpu.VMEM((256, lanes), BF16)
    shape = jax.ShapeDtypeStruct

    def exchange(x, axis):
        return lax.all_to_all(x, axis, 0, 0, tiled=True)

    def swap(x):
        return lax.ppermute(x, "core", [(0, 1), (1, 0)])

    def call(body, out_shape, *args, scratch=(), **kwargs):
        return pl.pallas_call(
            body, out_shape=out_shape, scratch_shapes=scratch, compiler_params=PARAMS, **kwargs
        )(*args)

    hbm_space = pl.BlockSpec(memory_space=pltpu.HBM)
    cols, rows = call(
        pack_body(log_scale),
        (shape((row, group + 40, LANES), BF16), pltpu.VMEM((80, LANES), BF16)),
        pltpu.with_memory_space_constraint(points.T, pltpu.HBM),
        pltpu.with_memory_space_constraint(start_vectors.T, pltpu.HBM),
        scratch=(
            pltpu.VMEM((features, group), BF16),
            pltpu.VMEM((start_vectors.shape[1], group), BF16),
            pltpu.VMEM((group + 40, LANES), BF16),
            pltpu.SemaphoreType.DMA((2 + row,)),
        ),
        in_specs=[hbm_space, hbm_space],
        out_specs=(hbm_space, pl.BlockSpec(memory_space=pltpu.VMEM)),
    )
    cols = exchange(cols, "row")
    rows = lax.all_gather(rows, ("z", "core"))
    aff_shape = pltpu.VMEM((row * group, lanes), BF16)
    send_shape = shape((half, 48, LANES), F32)
    away_aff, away_send, left, vec = call(
        away_body(log_scale),
        (
            aff_shape,
            send_shape,
            pltpu.VMEM((row * group, LANES), BF16),
            pltpu.VMEM((48, row * group), BF16),
        ),
        rows,
        cols,
        scratch=(right_shape,),
    )
    other = swap(away_send)
    home_aff, home_send = call(
        home_body(log_scale), (aff_shape, send_shape), rows, left, vec, scratch=(right_shape,)
    )
    send = call(join_body, send_shape, home_send, other)
    spread, degree = call(
        scale_body, (shape((row, 40, LANES), F32), shape((16, LANES), F32)), exchange(send, "z")
    )
    away_send, vec, gram = call(
        away_again_body,
        (send_shape, pltpu.VMEM((64, row * group), BF16), pltpu.VMEM((8, LANES), F32)),
        away_aff,
        exchange(spread, "row"),
    )
    other = swap(away_send)
    home_send = call(home_again_body, send_shape, home_aff, vec, gram)
    send = call(join_body, send_shape, home_send, other)
    scaled, gram = call(
        middle_body(total),
        (shape((32, 2 * LANES), F32), shape((col, 8, LANES), F32)),
        exchange(send, "z"),
        degree,
    )
    gram = exchange(gram, ("z", "core"))
    gram = call(again_body, shape((row, 8, LANES), F32), gram)
    out = call(last_body(total), shape((32, group), F32), exchange(gram, "row"), scaled)
    return out.T


def solution(mesh):
    rows, cols = mesh.devices.shape
    finer = Mesh(mesh.devices.reshape(rows, cols // 2, 2), ("row", "z", "core"))
    spec = P(("row", "z", "core"), None)
    return jax.shard_map(
        shards, mesh=finer, in_specs=(spec, spec), out_specs=spec, check_vma=False
    )
```

```python
import math

import jax
import jax.numpy as jnp
from jax import lax
from jax.experimental import pallas as pl
from jax.experimental.pallas import tpu as pltpu
from jax.sharding import Mesh
from jax.sharding import PartitionSpec as P

KERNEL_SCALE = 5.12
F32 = jnp.float32
BF16 = jnp.bfloat16
LANES = 128
PARAMS = pltpu.CompilerParams(vmem_limit_bytes=32 * 1024 * 1024)
REST = 32
WIDTH = 512
NORM, ONES, END = 64, 67, 70


def lane_of(shape):
    return lax.broadcasted_iota(jnp.int32, shape, len(shape) - 1)


def row_of(shape):
    return lax.broadcasted_iota(jnp.int32, shape, len(shape) - 2)


def roll(x, shift):
    shift %= LANES
    return pltpu.roll(x, shift, 1) if shift else x


def fold(x, place=0):
    h = x.shape[0] // 4
    group = lane_of((h, LANES)) // REST
    out = jnp.zeros((h, LANES), F32)
    for g in range(4):
        out = jnp.where(group == g, roll(x[g * h : (g + 1) * h], REST * (g - place)), out)
    return out


def unfold(pieces):
    h = pieces[0].shape[0]
    group = lane_of((h, LANES)) // REST
    rows = []
    for g in range(4):
        out = jnp.zeros((h, LANES), F32)
        for q, piece in enumerate(pieces):
            out = jnp.where(group == q, roll(piece, REST * (q - g)), out)
        rows.append(out)
    return jnp.concatenate(rows, axis=0)


def split(x):
    first = x.astype(BF16).astype(F32)
    second = (x - first).astype(BF16).astype(F32)
    return first, second, x - first - second


def widen(x):
    return jnp.concatenate([x, jnp.zeros((x.shape[0], LANES - x.shape[1]), x.dtype)], axis=1)


def main_and_rest(x):
    return x[:, 0:LANES], fold(widen(x[:, LANES : LANES + REST]))


def copies(ref, value):
    for i in range(ref.shape[0]):
        ref[i] = value


def pack_body(log_scale):
    def body(points_hbm, vectors_hbm, cols_hbm, rows_ref, points_ref, vectors_ref, block_ref, sems):
        loads = (
            pltpu.make_async_copy(points_hbm, points_ref, sems.at[0]),
            pltpu.make_async_copy(vectors_hbm, vectors_ref, sems.at[1]),
        )
        for load in loads:
            load.start()
        loads[0].wait()
        pts = points_ref[...].astype(F32)
        group = pts.shape[1]
        main, rest = main_and_rest(pts)
        rows_ref[...] = jnp.concatenate([main, rest], axis=0).astype(BF16)
        flat = jnp.concatenate([main, widen(pts[:, LANES:])], axis=1)
        norm = jnp.sum(flat * flat, axis=0, keepdims=True) * (-0.5 * log_scale)
        row = row_of((8, flat.shape[1]))
        extra = jnp.where((row >= ONES - NORM) & (row < END - NORM), 1.0, 0.0)
        for k, piece in enumerate(split(norm)):
            extra = jnp.where(row == k, piece, extra)
        blank = jnp.zeros((LANES - NORM - 8, flat.shape[1]), F32)
        flat = jnp.concatenate([flat, extra, blank], axis=0).T[0:group]
        loads[1].wait()
        main, rest = main_and_rest(vectors_ref[...].astype(F32))
        block_ref[...] = jnp.concatenate([flat, main, rest], axis=0).astype(BF16)
        count = cols_hbm.shape[0]
        sends = [
            pltpu.make_async_copy(block_ref, cols_hbm.at[i], sems.at[2 + i]) for i in range(count)
        ]
        for send in sends:
            send.start()
        for send in sends:
            send.wait()

    return body


def blocks_of(count):
    lanes = count * LANES
    main = [(at, WIDTH) for at in range(0, lanes, WIDTH)]
    return main, (lanes, lanes // 4)


def put_columns(cols_ref, left_ref, vec_ref):
    count = cols_ref.shape[0]
    total = left_ref.shape[0]
    for i in range(count):
        left_ref[i * LANES : (i + 1) * LANES, :] = cols_ref[i, 0:128]
        at = count * LANES + i * REST
        left_ref[at : at + REST, :] = cols_ref[i, 128:160]
    vec_ref[32:48, :] = jnp.where(row_of((16, total)) == 0, 1.0, 0.0).astype(BF16)
    for i in range(count):
        vec_ref[0:32, i * LANES : (i + 1) * LANES] = cols_ref[i, 160:192]
    for m in range(count // 4):
        rests = [cols_ref[4 * m + q, 192:200].astype(F32) for q in range(4)]
        at = (count + m) * LANES
        vec_ref[0:32, at : at + LANES] = unfold(rests).astype(BF16)


def put_rows(log_scale, rows_ref, core, right_ref):
    count = rows_ref.shape[0] // 2

    def put(tile, raw):
        at = tile * LANES
        scaled = raw * log_scale
        first = scaled.astype(BF16)
        norm = jnp.sum(raw * raw, axis=0, keepdims=True) * (-0.5 * log_scale)
        row = row_of((16, LANES))
        extra = jnp.where(row < ONES - NORM, 1.0, 0.0)
        for i, piece in enumerate(split(norm)):
            extra = jnp.where(row == ONES - NORM + i, piece, extra)
        right_ref[0:64, at : at + LANES] = first
        right_ref[64:80, at : at + LANES] = extra.astype(BF16)
        right_ref[80:128, at : at + LANES] = jnp.zeros((48, LANES), BF16)
        right_ref[128:192, at : at + LANES] = (scaled - first.astype(F32)).astype(BF16)
        right_ref[192:256, at : at + LANES] = jnp.zeros((64, LANES), BF16)

    for i in range(count):
        put(i, rows_ref[2 * i + core, 0:64].astype(F32))
    for m in range(count // 4):
        rests = [rows_ref[2 * (4 * m + q) + core, 64:80].astype(F32) for q in range(4)]
        put(count + m, unfold(rests))


def affinity_product(left_ref, right_ref, vec_ref, aff_ref, send_ref):
    total = left_ref.shape[0]
    main, rest = blocks_of(send_ref.shape[0])
    chunk = 512

    def weights(at, width):
        right = right_ref[:, at : at + width]
        for start in range(0, total, chunk):
            left = left_ref[start : start + chunk, :]
            power = jnp.dot(
                jnp.concatenate([left, left], axis=1), right, preferred_element_type=F32
            )
            aff_ref[start : start + chunk, at : at + width] = jnp.exp2(power).astype(BF16)

    def product(at, width):
        return jnp.dot(
            vec_ref[...], aff_ref[:, at : at + width], preferred_element_type=F32
        )

    def send_main(at, width):
        out = product(at, width)
        for k in range(width // LANES):
            tile = out[:, k * LANES : (k + 1) * LANES]
            send_ref[at // LANES + k, 0:32, :] = tile[0:32]
            send_ref[at // LANES + k, 40:41, :] = tile[32:33]

    def send_rest(at, width):
        out = product(at, width)
        row = row_of((8, LANES))
        for m in range(width // LANES):
            tile = out[:, m * LANES : (m + 1) * LANES]
            for q in range(4):
                send_ref[4 * m + q, 32:40, :] = fold(tile[0:32], q)
                degree = jnp.broadcast_to(roll(tile[32:40], -REST * q)[0:1], (8, LANES))
                send_ref[4 * m + q, 40:48, :] = jnp.where(row == 1, degree, 0.0)

    weights(*main[0])
    weights(*rest)
    send_rest(*rest)
    send_main(*main[0])
    for block in main[1:]:
        weights(*block)
        send_main(*block)


def away_body(right_ref, cols_ref, aff_ref, send_ref, left_ref, vec_ref):
    put_columns(cols_ref, left_ref, vec_ref)
    affinity_product(left_ref, right_ref, vec_ref, aff_ref, send_ref)


def rows_body(log_scale):
    def body(rows_ref, away_right_ref, home_right_ref):
        core = lax.axis_index("core")
        put_rows(log_scale, rows_ref, 1 - core, away_right_ref)
        put_rows(log_scale, rows_ref, core, home_right_ref)

    return body


def join_body(mine_ref, other_ref, out_ref):
    out_ref[...] = mine_ref[...] + other_ref[...]


def gram_of(x):
    return lax.dot_general(
        x,
        x,
        (((1,), (1,)), ((), ())),
        precision=lax.Precision.HIGHEST,
        preferred_element_type=F32,
    )


def whole(main, rest):
    return jnp.concatenate([main, unfold([rest])], axis=1)


def scale_body(recv_ref, spread_ref, degree_ref):
    total = jnp.sum(recv_ref[...], axis=0)
    rest = jnp.where(lane_of((1, LANES)) < REST, total[41:42], 0.0)
    rest = jnp.broadcast_to(rest, (8, LANES))
    rest = (rest + roll(rest, REST)) + (roll(rest, 2 * REST) + roll(rest, 3 * REST))
    degree_ref[0:8, :] = jnp.broadcast_to(total[40:41], (8, LANES))
    degree_ref[8:16, :] = rest
    main, rest = total[0:32] / total[40:41], total[32:40] / rest
    copies(spread_ref, jnp.concatenate([main, rest], axis=0))


def put_vectors(spread_ref, vec_ref):
    count = spread_ref.shape[0]

    def put(tile, value):
        first = value.astype(BF16)
        at = tile * LANES
        vec_ref[0:32, at : at + LANES] = first
        vec_ref[32:64, at : at + LANES] = (value - first.astype(F32)).astype(BF16)

    for i in range(count):
        put(i, spread_ref[i, 0:32, :])
    for m in range(count // 4):
        put(count + m, unfold([spread_ref[4 * m + q, 32:40, :] for q in range(4)]))


def second_product(vec_ref, aff_ref, at, width):
    out = lax.dot_general(
        vec_ref[...],
        aff_ref[at : at + width, :],
        (((1,), (1,)), ((), ())),
        preferred_element_type=F32,
    )
    return out[0:32] + out[32:64]


def gram_folded(vec_ref):
    vec = vec_ref[...]
    gram = lax.dot_general(vec, vec, (((1,), (1,)), ((), ())), preferred_element_type=F32)
    gram = gram[0:32] + gram[32:64]
    return fold(widen(gram[:, 0:32] + gram[:, 32:64]))


def home_again_body(aff_ref, spread_ref, part_ref, gram_ref, vec_ref):
    put_vectors(spread_ref, vec_ref)
    gram_ref[...] = gram_folded(vec_ref)
    for at in range(0, part_ref.shape[1], WIDTH):
        part_ref[:, at : at + WIDTH] = second_product(vec_ref, aff_ref, at, WIDTH)


def away_again_body(aff_ref, spread_ref, part_ref, gram_ref, send_ref, vec_ref):
    put_vectors(spread_ref, vec_ref)
    gram = gram_folded(vec_ref) + gram_ref[...]
    main, rest = blocks_of(send_ref.shape[0])
    for at, width in [rest] + main:
        out = part_ref[:, at : at + width] + second_product(vec_ref, aff_ref, at, width)
        for k in range(width // LANES):
            tile = out[:, k * LANES : (k + 1) * LANES]
            if at == rest[0]:
                for q in range(4):
                    send_ref[4 * k + q, 32:40, :] = fold(tile, q)
            else:
                send_ref[at // LANES + k, 0:32, :] = tile
    for i in range(send_ref.shape[0]):
        send_ref[i, 40:48, :] = gram


def solved(gram, right):
    size = 4 * gram.shape[0]
    wide = right.shape[1] // LANES
    columns = [
        jnp.concatenate(
            [
                jnp.broadcast_to(gram[:, REST * g + k : REST * g + k + 1], (8, LANES))
                for g in range(k // 8, 4)
            ],
            axis=0,
        )
        for k in range(size)
    ]
    rows = [right[8 * g : 8 * g + 8] for g in range(size // 8)]
    for j in range(size):
        base, at = j // 8, j % 8
        pivot = columns[j][at : at + 1]
        scale = lax.rsqrt(pivot)
        scale = scale * (1.5 - 0.5 * pivot * scale * scale)
        factor = columns[j] * scale
        for k in range(j + 1, size):
            skip = 8 * (k // 8 - base)
            mine = factor[k - 8 * base : k - 8 * base + 1]
            columns[k] = columns[k] - factor[skip:] * mine
        top = rows[base][at : at + 1] * jnp.concatenate([scale] * wide, axis=1)
        for g in range(base, size // 8):
            part = factor[8 * (g - base) : 8 * (g - base) + 8]
            if g == base:
                row = row_of((8, LANES))
                part = jnp.where(row > at, part, 0.0)
            new = rows[g] - jnp.concatenate([part] * wide, axis=1) * top
            if g == base:
                new = jnp.where(row_of(new.shape) == at, top, new)
            rows[g] = new
    return jnp.concatenate(rows, axis=0)


def middle_body(points):
    def body(recv_ref, degree_ref, scaled_ref, gram_ref):
        total = jnp.sum(recv_ref[...], axis=0)
        main = total[0:32] / degree_ref[0:1, :]
        rest = total[32:40] / degree_ref[8:16, :]
        scaled = solved(total[40:48] / points, whole(main, rest))
        scaled_ref[...] = scaled
        copies(gram_ref, fold(widen(gram_of(scaled))))

    return body


def again_body(recv_ref, gram_ref):
    copies(gram_ref, jnp.sum(recv_ref[...], axis=0))


def last_body(points):
    def body(recv_ref, scaled_ref, out_ref):
        gram = jnp.sum(recv_ref[...], axis=0) / points
        out_ref[...] = solved(gram, scaled_ref[...])[:, 0 : out_ref.shape[1]]

    return body


def shards(points, start_vectors):
    group, features = points.shape
    row, half, cores = lax.axis_size("row"), lax.axis_size("z"), lax.axis_size("core")
    col = half * cores
    total = group * row * col
    log_scale = 2.0 * KERNEL_SCALE / features * math.log2(math.e)
    lanes = half * group
    right_shape = pltpu.VMEM((256, lanes), BF16)
    shape = jax.ShapeDtypeStruct

    def exchange(x, axis):
        return lax.all_to_all(x, axis, 0, 0, tiled=True)

    def swap(x):
        return lax.ppermute(x, "core", [(0, 1), (1, 0)])

    def call(body, out_shape, *args, scratch=(), **kwargs):
        return pl.pallas_call(
            body,
            out_shape=out_shape,
            scratch_shapes=scratch,
            compiler_params=PARAMS,
            **kwargs,
        )(*args)

    hbm_space = pl.BlockSpec(memory_space=pltpu.HBM)
    cols, rows = call(
        pack_body(log_scale),
        (shape((row, group + 40, LANES), BF16), pltpu.VMEM((80, LANES), BF16)),
        pltpu.with_memory_space_constraint(points.T, pltpu.HBM),
        pltpu.with_memory_space_constraint(start_vectors.T, pltpu.HBM),
        scratch=(
            pltpu.VMEM((features, group), BF16),
            pltpu.VMEM((start_vectors.shape[1], group), BF16),
            pltpu.VMEM((group + 40, LANES), BF16),
            pltpu.SemaphoreType.DMA((2 + row,)),
        ),
        in_specs=[hbm_space, hbm_space],
        out_specs=(hbm_space, pl.BlockSpec(memory_space=pltpu.VMEM)),
    )
    cols = exchange(cols, "row")
    rows = lax.all_gather(rows, ("z", "core"))
    away_right, home_right = call(
        rows_body(log_scale), (right_shape, right_shape), rows
    )
    aff_shape = pltpu.VMEM((row * group, lanes), BF16)
    send_shape = shape((half, 48, LANES), F32)
    away_aff, away_send, left, vec = call(
        away_body,
        (
            aff_shape,
            send_shape,
            pltpu.VMEM((row * group, LANES), BF16),
            pltpu.VMEM((48, row * group), BF16),
        ),
        away_right,
        cols,
    )
    other = swap(away_send)
    home_aff, home_send = call(
        affinity_product, (aff_shape, send_shape), left, home_right, vec
    )
    send = call(join_body, send_shape, home_send, other)
    spread, degree = call(
        scale_body,
        (shape((half, 40, LANES), F32), shape((16, LANES), F32)),
        exchange(send, "z"),
    )
    home_spread = exchange(spread, "z")
    away_spread = swap(home_spread)
    vec_shape = pltpu.VMEM((64, lanes), BF16)
    part, gram = call(
        home_again_body,
        (pltpu.VMEM((32, row * group), F32), pltpu.VMEM((8, LANES), F32)),
        home_aff,
        home_spread,
        scratch=(vec_shape,),
    )
    send = call(
        away_again_body,
        shape((row, 48, LANES), F32),
        away_aff,
        away_spread,
        part,
        gram,
        scratch=(vec_shape,),
    )
    scaled, gram = call(
        middle_body(total),
        (shape((32, 2 * LANES), F32), shape((row, 8, LANES), F32)),
        exchange(send, "row"),
        degree,
    )
    gram = exchange(gram, "row")
    gram = call(again_body, shape((col, 8, LANES), F32), gram)
    out = call(
        last_body(total), shape((32, group), F32), exchange(gram, ("z", "core")), scaled
    )
    return out.T


def solution(mesh):
    rows, cols = mesh.devices.shape
    finer = Mesh(mesh.devices.reshape(rows, cols // 2, 2), ("row", "z", "core"))
    spec = P(("row", "z", "core"), None)
    return jax.shard_map(
        shards, mesh=finer, in_specs=(spec, spec), out_specs=spec, check_vma=False
    )
```

```python
import math

import jax
import jax.numpy as jnp
from jax import lax
from jax.experimental import pallas as pl
from jax.experimental.pallas import tpu as pltpu
from jax.sharding import Mesh
from jax.sharding import PartitionSpec as P

KERNEL_SCALE = 5.12
F32 = jnp.float32
BF16 = jnp.bfloat16
LANES = 128
PARAMS = pltpu.CompilerParams(vmem_limit_bytes=32 * 1024 * 1024)
REST = 32
WIDTH = 512
NORM, ONES, END = 64, 67, 70


def lane_of(shape):
    return lax.broadcasted_iota(jnp.int32, shape, len(shape) - 1)


def row_of(shape):
    return lax.broadcasted_iota(jnp.int32, shape, len(shape) - 2)


def roll(x, shift):
    shift %= LANES
    return pltpu.roll(x, shift, 1) if shift else x


def fold(x, place=0):
    h = x.shape[0] // 4
    group = lane_of((h, LANES)) // REST
    out = jnp.zeros((h, LANES), F32)
    for g in range(4):
        out = jnp.where(group == g, roll(x[g * h : (g + 1) * h], REST * (g - place)), out)
    return out


def unfold(pieces):
    h = pieces[0].shape[0]
    group = lane_of((h, LANES)) // REST
    rows = []
    for g in range(4):
        out = jnp.zeros((h, LANES), F32)
        for q, piece in enumerate(pieces):
            out = jnp.where(group == q, roll(piece, REST * (q - g)), out)
        rows.append(out)
    return jnp.concatenate(rows, axis=0)


def split(x):
    first = x.astype(BF16).astype(F32)
    second = (x - first).astype(BF16).astype(F32)
    return first, second, x - first - second


def widen(x):
    return jnp.concatenate([x, jnp.zeros((x.shape[0], LANES - x.shape[1]), x.dtype)], axis=1)


def main_and_rest(x):
    return x[:, 0:LANES], fold(widen(x[:, LANES : LANES + REST]))


def copies(ref, value):
    for i in range(ref.shape[0]):
        ref[i] = value


def pack_body(points_hbm, vectors_hbm, cols_hbm, rows_ref, points_ref, vectors_ref, block_ref, sems):
    loads = (
        pltpu.make_async_copy(points_hbm, points_ref, sems.at[0]),
        pltpu.make_async_copy(vectors_hbm, vectors_ref, sems.at[1]),
    )
    for load in loads:
        load.start()
    loads[0].wait()
    pts = points_ref[...].astype(F32)
    group = pts.shape[1]
    main, rest = main_and_rest(pts)
    rows_ref[...] = jnp.concatenate([main, rest], axis=0).astype(BF16)
    flat = jnp.concatenate([main, widen(pts[:, LANES:])], axis=1)
    norm = jnp.sum(flat * flat, axis=0, keepdims=True) * -0.5
    row = row_of((8, flat.shape[1]))
    extra = jnp.where((row >= ONES - NORM) & (row < END - NORM), 1.0, 0.0)
    for k, piece in enumerate(split(norm)):
        extra = jnp.where(row == k, piece, extra)
    blank = jnp.zeros((LANES - NORM - 8, flat.shape[1]), F32)
    flat = jnp.concatenate([flat, extra, blank], axis=0).T[0:group]
    loads[1].wait()
    main, rest = main_and_rest(vectors_ref[...].astype(F32))
    block_ref[...] = jnp.concatenate([flat, main, rest], axis=0).astype(BF16)
    count = cols_hbm.shape[0]
    sends = [
        pltpu.make_async_copy(block_ref, cols_hbm.at[i], sems.at[2 + i]) for i in range(count)
    ]
    for send in sends:
        send.start()
    for send in sends:
        send.wait()


def blocks_of(count):
    lanes = count * LANES
    main = [(at, WIDTH) for at in range(0, lanes, WIDTH)]
    return main, (lanes, lanes // 4)


def put_columns(cols_ref, left_ref, vec_ref):
    count = cols_ref.shape[0]
    total = left_ref.shape[0]
    for i in range(count):
        left_ref[i * LANES : (i + 1) * LANES, :] = cols_ref[i, 0:128]
        at = count * LANES + i * REST
        left_ref[at : at + REST, :] = cols_ref[i, 128:160]
    vec_ref[32:48, :] = jnp.where(row_of((16, total)) == 0, 1.0, 0.0).astype(BF16)
    for i in range(count):
        vec_ref[0:32, i * LANES : (i + 1) * LANES] = cols_ref[i, 160:192]
    for m in range(count // 4):
        rests = [cols_ref[4 * m + q, 192:200].astype(F32) for q in range(4)]
        at = (count + m) * LANES
        vec_ref[0:32, at : at + LANES] = unfold(rests).astype(BF16)


def put_rows(rows_ref, core, right_ref):
    count = rows_ref.shape[0] // 2

    def put(tile, raw):
        at = tile * LANES
        norm = jnp.sum(raw * raw, axis=0, keepdims=True) * -0.5
        row = row_of((16, LANES))
        extra = jnp.where(row < ONES - NORM, 1.0, 0.0)
        for i, piece in enumerate(split(norm)):
            extra = jnp.where(row == ONES - NORM + i, piece, extra)
        right_ref[0:64, at : at + LANES] = raw.astype(BF16)
        right_ref[64:80, at : at + LANES] = extra.astype(BF16)
        right_ref[80:128, at : at + LANES] = jnp.zeros((48, LANES), BF16)

    for i in range(count):
        put(i, rows_ref[2 * i + core, 0:64].astype(F32))
    for m in range(count // 4):
        rests = [rows_ref[2 * (4 * m + q) + core, 64:80].astype(F32) for q in range(4)]
        put(count + m, unfold(rests))


def affinity_product(log_scale, left_ref, right_ref, vec_ref, aff_ref, send_ref):
    total = left_ref.shape[0]
    main, rest = blocks_of(send_ref.shape[0])
    chunk = 640

    def weights(at, width):
        right = right_ref[:, at : at + width]
        for start in range(0, total, chunk):
            left = left_ref[start : start + chunk, :]
            power = jnp.dot(left, right, preferred_element_type=F32) * log_scale
            aff_ref[start : start + chunk, at : at + width] = jnp.exp2(power).astype(BF16)

    def product(at, width):
        return jnp.dot(
            vec_ref[...], aff_ref[:, at : at + width], preferred_element_type=F32
        )

    def send_main(at, width):
        out = product(at, width)
        for k in range(width // LANES):
            tile = out[:, k * LANES : (k + 1) * LANES]
            send_ref[at // LANES + k, 0:32, :] = tile[0:32]
            send_ref[at // LANES + k, 40:41, :] = tile[32:33]

    def send_rest(at, width):
        out = product(at, width)
        row = row_of((8, LANES))
        for m in range(width // LANES):
            tile = out[:, m * LANES : (m + 1) * LANES]
            for q in range(4):
                send_ref[4 * m + q, 32:40, :] = fold(tile[0:32], q)
                degree = jnp.broadcast_to(roll(tile[32:40], -REST * q)[0:1], (8, LANES))
                send_ref[4 * m + q, 40:48, :] = jnp.where(row == 1, degree, 0.0)

    weights(*main[0])
    weights(*rest)
    send_rest(*rest)
    send_main(*main[0])
    for block in main[1:]:
        weights(*block)
        send_main(*block)


def away_body(log_scale):
    def body(right_ref, cols_ref, aff_ref, send_ref, left_ref, vec_ref):
        put_columns(cols_ref, left_ref, vec_ref)
        affinity_product(log_scale, left_ref, right_ref, vec_ref, aff_ref, send_ref)

    return body


def home_body(log_scale):
    def body(left_ref, right_ref, vec_ref, aff_ref, send_ref):
        affinity_product(log_scale, left_ref, right_ref, vec_ref, aff_ref, send_ref)

    return body


def rows_body(rows_ref, away_right_ref, home_right_ref):
    core = lax.axis_index("core")
    put_rows(rows_ref, 1 - core, away_right_ref)
    put_rows(rows_ref, core, home_right_ref)


def join_body(mine_ref, other_ref, out_ref):
    out_ref[...] = mine_ref[...] + other_ref[...]


def gram_of(x):
    return lax.dot_general(
        x,
        x,
        (((1,), (1,)), ((), ())),
        precision=lax.Precision.HIGHEST,
        preferred_element_type=F32,
    )


def whole(main, rest):
    return jnp.concatenate([main, unfold([rest])], axis=1)


def scale_body(recv_ref, spread_ref, degree_ref):
    total = jnp.sum(recv_ref[...], axis=0)
    rest = jnp.where(lane_of((1, LANES)) < REST, total[41:42], 0.0)
    rest = jnp.broadcast_to(rest, (8, LANES))
    rest = (rest + roll(rest, REST)) + (roll(rest, 2 * REST) + roll(rest, 3 * REST))
    degree_ref[0:8, :] = jnp.broadcast_to(total[40:41], (8, LANES))
    degree_ref[8:16, :] = rest
    main, rest = total[0:32] / total[40:41], total[32:40] / rest
    copies(spread_ref, jnp.concatenate([main, rest], axis=0))


def put_vectors(spread_ref, vec_ref):
    count = spread_ref.shape[0]

    def put(tile, value):
        first = value.astype(BF16)
        at = tile * LANES
        vec_ref[0:32, at : at + LANES] = first
        vec_ref[32:64, at : at + LANES] = (value - first.astype(F32)).astype(BF16)

    for i in range(count):
        put(i, spread_ref[i, 0:32, :])
    for m in range(count // 4):
        put(count + m, unfold([spread_ref[4 * m + q, 32:40, :] for q in range(4)]))


def second_product(aff_ref, vec_ref, send_ref):
    main, rest = blocks_of(send_ref.shape[0])

    def product(at, width):
        out = jnp.dot(vec_ref[...], aff_ref[:, at : at + width], preferred_element_type=F32)
        return out[0:32] + out[32:64]

    out = product(*rest)
    for m in range(rest[1] // LANES):
        for q in range(4):
            send_ref[4 * m + q, 32:40, :] = fold(out[:, m * LANES : (m + 1) * LANES], q)
    for at, width in main:
        out = product(at, width)
        for k in range(width // LANES):
            send_ref[at // LANES + k, 0:32, :] = out[:, k * LANES : (k + 1) * LANES]


def put_gram(gram, send_ref):
    for i in range(send_ref.shape[0]):
        send_ref[i, 40:48, :] = gram


def away_again_body(aff_ref, spread_ref, send_ref, vec_ref, gram_ref):
    put_vectors(spread_ref, vec_ref)
    vec = vec_ref[...]
    gram = lax.dot_general(vec, vec, (((1,), (1,)), ((), ())), preferred_element_type=F32)
    gram = gram[0:32] + gram[32:64]
    gram = fold(widen(gram[:, 0:32] + gram[:, 32:64]))
    gram_ref[...] = gram
    second_product(aff_ref, vec_ref, send_ref)
    put_gram(gram, send_ref)


def home_again_body(aff_ref, vec_ref, gram_ref, send_ref):
    second_product(aff_ref, vec_ref, send_ref)
    put_gram(gram_ref[...], send_ref)


def solved(gram, right):
    size = 4 * gram.shape[0]
    wide = right.shape[1] // LANES
    columns = [
        jnp.concatenate(
            [
                jnp.broadcast_to(gram[:, REST * g + k : REST * g + k + 1], (8, LANES))
                for g in range(k // 8, 4)
            ],
            axis=0,
        )
        for k in range(size)
    ]
    rows = [right[8 * g : 8 * g + 8] for g in range(size // 8)]
    for j in range(size):
        base, at = j // 8, j % 8
        pivot = columns[j][at : at + 1]
        scale = lax.rsqrt(pivot)
        scale = scale * (1.5 - 0.5 * pivot * scale * scale)
        factor = columns[j] * scale
        for k in range(j + 1, size):
            skip = 8 * (k // 8 - base)
            mine = factor[k - 8 * base : k - 8 * base + 1]
            columns[k] = columns[k] - factor[skip:] * mine
        top = rows[base][at : at + 1] * jnp.concatenate([scale] * wide, axis=1)
        for g in range(base, size // 8):
            part = factor[8 * (g - base) : 8 * (g - base) + 8]
            if g == base:
                row = row_of((8, LANES))
                part = jnp.where(row > at, part, 0.0)
            new = rows[g] - jnp.concatenate([part] * wide, axis=1) * top
            if g == base:
                new = jnp.where(row_of(new.shape) == at, top, new)
            rows[g] = new
    return jnp.concatenate(rows, axis=0)


def middle_body(points):
    def body(recv_ref, degree_ref, scaled_ref, gram_ref):
        total = jnp.sum(recv_ref[...], axis=0)
        main = total[0:32] / degree_ref[0:1, :]
        rest = total[32:40] / degree_ref[8:16, :]
        scaled = solved(total[40:48] / points, whole(main, rest))
        scaled_ref[...] = scaled
        copies(gram_ref, fold(widen(gram_of(scaled))))

    return body


def again_body(recv_ref, gram_ref):
    copies(gram_ref, jnp.sum(recv_ref[...], axis=0))


def last_body(points):
    def body(recv_ref, scaled_ref, out_ref):
        gram = jnp.sum(recv_ref[...], axis=0) / points
        out_ref[...] = solved(gram, scaled_ref[...])[:, 0 : out_ref.shape[1]]

    return body


def shards(points, start_vectors):
    group, features = points.shape
    row, half, cores = lax.axis_size("row"), lax.axis_size("z"), lax.axis_size("core")
    col = half * cores
    total = group * row * col
    log_scale = 2.0 * KERNEL_SCALE / features * math.log2(math.e)
    lanes = half * group
    right_shape = pltpu.VMEM((LANES, lanes), BF16)
    shape = jax.ShapeDtypeStruct

    def exchange(x, axis):
        return lax.all_to_all(x, axis, 0, 0, tiled=True)

    def swap(x):
        return lax.ppermute(x, "core", [(0, 1), (1, 0)])

    def call(body, out_shape, *args, scratch=(), **kwargs):
        return pl.pallas_call(
            body, out_shape=out_shape, scratch_shapes=scratch, compiler_params=PARAMS, **kwargs
        )(*args)

    hbm_space = pl.BlockSpec(memory_space=pltpu.HBM)
    cols, rows = call(
        pack_body,
        (shape((row, group + 40, LANES), BF16), pltpu.VMEM((80, LANES), BF16)),
        pltpu.with_memory_space_constraint(points.T, pltpu.HBM),
        pltpu.with_memory_space_constraint(start_vectors.T, pltpu.HBM),
        scratch=(
            pltpu.VMEM((features, group), BF16),
            pltpu.VMEM((start_vectors.shape[1], group), BF16),
            pltpu.VMEM((group + 40, LANES), BF16),
            pltpu.SemaphoreType.DMA((2 + row,)),
        ),
        in_specs=[hbm_space, hbm_space],
        out_specs=(hbm_space, pl.BlockSpec(memory_space=pltpu.VMEM)),
    )
    cols = exchange(cols, "row")
    rows = lax.all_gather(rows, ("z", "core"))
    away_right, home_right = call(rows_body, (right_shape, right_shape), rows)
    aff_shape = pltpu.VMEM((row * group, lanes), BF16)
    send_shape = shape((half, 48, LANES), F32)
    away_aff, away_send, left, vec = call(
        away_body(log_scale),
        (
            aff_shape,
            send_shape,
            pltpu.VMEM((row * group, LANES), BF16),
            pltpu.VMEM((48, row * group), BF16),
        ),
        away_right,
        cols,
    )
    other = swap(away_send)
    home_aff, home_send = call(home_body(log_scale), (aff_shape, send_shape), left, home_right, vec)
    send = call(join_body, send_shape, home_send, other)
    spread, degree = call(
        scale_body, (shape((row, 40, LANES), F32), shape((16, LANES), F32)), exchange(send, "z")
    )
    away_send, vec, gram = call(
        away_again_body,
        (send_shape, pltpu.VMEM((64, row * group), BF16), pltpu.VMEM((8, LANES), F32)),
        away_aff,
        exchange(spread, "row"),
    )
    other = swap(away_send)
    home_send = call(home_again_body, send_shape, home_aff, vec, gram)
    send = call(join_body, send_shape, home_send, other)
    scaled, gram = call(
        middle_body(total),
        (shape((32, 2 * LANES), F32), shape((col, 8, LANES), F32)),
        exchange(send, "z"),
        degree,
    )
    gram = exchange(gram, ("z", "core"))
    gram = call(again_body, shape((row, 8, LANES), F32), gram)
    out = call(last_body(total), shape((32, group), F32), exchange(gram, "row"), scaled)
    return out.T


def solution(mesh):
    rows, cols = mesh.devices.shape
    finer = Mesh(mesh.devices.reshape(rows, cols // 2, 2), ("row", "z", "core"))
    spec = P(("row", "z", "core"), None)
    return jax.shard_map(
        shards, mesh=finer, in_specs=(spec, spec), out_specs=spec, check_vma=False
    )
```

```python
import math

import jax
import jax.numpy as jnp
from jax import lax
from jax.experimental import pallas as pl
from jax.experimental.pallas import tpu as pltpu
from jax.sharding import Mesh
from jax.sharding import PartitionSpec as P

KERNEL_SCALE = 5.12
F32 = jnp.float32
BF16 = jnp.bfloat16
LANES = 128
PARAMS = pltpu.CompilerParams(vmem_limit_bytes=32 * 1024 * 1024)
REST = 32
WIDTH = 512
NORM, ONES, END = 64, 67, 70


def lane_of(shape):
    return lax.broadcasted_iota(jnp.int32, shape, len(shape) - 1)


def row_of(shape):
    return lax.broadcasted_iota(jnp.int32, shape, len(shape) - 2)


def roll(x, shift):
    shift %= LANES
    return pltpu.roll(x, shift, 1) if shift else x


def fold(x, place=0):
    h = x.shape[0] // 4
    group = lane_of((h, LANES)) // REST
    out = jnp.zeros((h, LANES), F32)
    for g in range(4):
        out = jnp.where(group == g, roll(x[g * h : (g + 1) * h], REST * (g - place)), out)
    return out


def unfold(pieces):
    h = pieces[0].shape[0]
    group = lane_of((h, LANES)) // REST
    rows = []
    for g in range(4):
        out = jnp.zeros((h, LANES), F32)
        for q, piece in enumerate(pieces):
            out = jnp.where(group == q, roll(piece, REST * (q - g)), out)
        rows.append(out)
    return jnp.concatenate(rows, axis=0)


def split(x):
    first = x.astype(BF16).astype(F32)
    second = (x - first).astype(BF16).astype(F32)
    return first, second, x - first - second


def widen(x):
    return jnp.concatenate([x, jnp.zeros((x.shape[0], LANES - x.shape[1]), x.dtype)], axis=1)


def main_and_rest(x):
    return x[:, 0:LANES], fold(widen(x[:, LANES : LANES + REST]))


def copies(ref, value):
    for i in range(ref.shape[0]):
        ref[i] = value


def pack_body(points_hbm, vectors_hbm, cols_hbm, rows_ref, points_ref, vectors_ref, block_ref, sems):
    loads = (
        pltpu.make_async_copy(points_hbm, points_ref, sems.at[0]),
        pltpu.make_async_copy(vectors_hbm, vectors_ref, sems.at[1]),
    )
    for load in loads:
        load.start()
    for load in loads:
        load.wait()
    pts = points_ref[...].astype(F32)
    group = pts.shape[1]
    main, rest = main_and_rest(pts)
    rows_ref[...] = jnp.concatenate([main, rest], axis=0).astype(BF16)
    flat = jnp.concatenate([main, widen(pts[:, LANES:])], axis=1)
    norm = jnp.sum(flat * flat, axis=0, keepdims=True) * -0.5
    row = row_of((8, flat.shape[1]))
    extra = jnp.where((row >= ONES - NORM) & (row < END - NORM), 1.0, 0.0)
    for k, piece in enumerate(split(norm)):
        extra = jnp.where(row == k, piece, extra)
    blank = jnp.zeros((LANES - NORM - 8, flat.shape[1]), F32)
    flat = jnp.concatenate([flat, extra, blank], axis=0).T[0:group]
    main, rest = main_and_rest(vectors_ref[...].astype(F32))
    block_ref[group:, :] = jnp.concatenate([main, rest], axis=0).astype(BF16)
    block_ref[0:group, :] = flat.astype(BF16)
    count = cols_hbm.shape[0]
    sends = [
        pltpu.make_async_copy(block_ref, cols_hbm.at[i], sems.at[2 + i]) for i in range(count)
    ]
    for send in sends:
        send.start()
    for send in sends:
        send.wait()


def blocks_of(count):
    lanes = count * LANES
    main = [(at, WIDTH) for at in range(0, lanes, WIDTH)]
    return main, (lanes, lanes // 4)


def put_columns(cols_ref, left_ref, vec_ref):
    count = cols_ref.shape[0]
    total = left_ref.shape[0]
    for i in range(count):
        left_ref[i * LANES : (i + 1) * LANES, :] = cols_ref[i, 0:128]
        at = count * LANES + i * REST
        left_ref[at : at + REST, :] = cols_ref[i, 128:160]
    vec_ref[32:48, :] = jnp.where(row_of((16, total)) == 0, 1.0, 0.0).astype(BF16)
    for i in range(count):
        vec_ref[0:32, i * LANES : (i + 1) * LANES] = cols_ref[i, 160:192]
    for m in range(count // 4):
        rests = [cols_ref[4 * m + q, 192:200].astype(F32) for q in range(4)]
        at = (count + m) * LANES
        vec_ref[0:32, at : at + LANES] = unfold(rests).astype(BF16)


def put_rows(rows_ref, core, right_ref):
    count = rows_ref.shape[0] // 2

    def put(tile, raw):
        at = tile * LANES
        norm = jnp.sum(raw * raw, axis=0, keepdims=True) * -0.5
        row = row_of((16, LANES))
        extra = jnp.where(row < ONES - NORM, 1.0, 0.0)
        for i, piece in enumerate(split(norm)):
            extra = jnp.where(row == ONES - NORM + i, piece, extra)
        right_ref[0:64, at : at + LANES] = raw.astype(BF16)
        right_ref[64:80, at : at + LANES] = extra.astype(BF16)
        right_ref[80:128, at : at + LANES] = jnp.zeros((48, LANES), BF16)

    for i in range(count):
        put(i, rows_ref[2 * i + core, 0:64].astype(F32))
    for m in range(count // 4):
        rests = [rows_ref[2 * (4 * m + q) + core, 64:80].astype(F32) for q in range(4)]
        put(count + m, unfold(rests))


def affinity_product(log_scale, left_ref, right_ref, vec_ref, aff_ref, send_ref):
    total = left_ref.shape[0]
    main, rest = blocks_of(send_ref.shape[0])
    chunk = 640

    def weights(at, width):
        right = right_ref[:, at : at + width]
        for start in range(0, total, chunk):
            left = left_ref[start : start + chunk, :]
            power = jnp.dot(left, right, preferred_element_type=F32) * log_scale
            aff_ref[start : start + chunk, at : at + width] = jnp.exp2(power).astype(BF16)

    def product(at, width):
        return jnp.dot(
            vec_ref[...], aff_ref[:, at : at + width], preferred_element_type=F32
        )

    def send_main(at, width):
        out = product(at, width)
        for k in range(width // LANES):
            tile = out[:, k * LANES : (k + 1) * LANES]
            send_ref[at // LANES + k, 0:32, :] = tile[0:32]
            send_ref[at // LANES + k, 40:41, :] = tile[32:33]

    def send_rest(at, width):
        out = product(at, width)
        row = row_of((8, LANES))
        for m in range(width // LANES):
            tile = out[:, m * LANES : (m + 1) * LANES]
            for q in range(4):
                send_ref[4 * m + q, 32:40, :] = fold(tile[0:32], q)
                degree = jnp.broadcast_to(roll(tile[32:40], -REST * q)[0:1], (8, LANES))
                send_ref[4 * m + q, 40:48, :] = jnp.where(row == 1, degree, 0.0)

    weights(*main[0])
    weights(*rest)
    send_rest(*rest)
    send_main(*main[0])
    for block in main[1:]:
        weights(*block)
        send_main(*block)


def away_body(log_scale):
    def body(rows_ref, cols_ref, aff_ref, send_ref, left_ref, vec_ref, right_ref):
        put_rows(rows_ref, 1 - lax.axis_index("core"), right_ref)
        put_columns(cols_ref, left_ref, vec_ref)
        affinity_product(log_scale, left_ref, right_ref, vec_ref, aff_ref, send_ref)

    return body


def home_body(log_scale):
    def body(rows_ref, left_ref, vec_ref, aff_ref, send_ref, right_ref):
        put_rows(rows_ref, lax.axis_index("core"), right_ref)
        affinity_product(log_scale, left_ref, right_ref, vec_ref, aff_ref, send_ref)

    return body


def join_body(mine_ref, other_ref, out_ref):
    out_ref[...] = mine_ref[...] + other_ref[...]


def gram_of(x):
    return lax.dot_general(
        x,
        x,
        (((1,), (1,)), ((), ())),
        precision=lax.Precision.HIGHEST,
        preferred_element_type=F32,
    )


def whole(main, rest):
    return jnp.concatenate([main, unfold([rest])], axis=1)


def scale_body(recv_ref, spread_ref, degree_ref):
    total = jnp.sum(recv_ref[...], axis=0)
    rest = jnp.where(lane_of((1, LANES)) < REST, total[41:42], 0.0)
    rest = jnp.broadcast_to(rest, (8, LANES))
    rest = (rest + roll(rest, REST)) + (roll(rest, 2 * REST) + roll(rest, 3 * REST))
    degree_ref[0:8, :] = jnp.broadcast_to(total[40:41], (8, LANES))
    degree_ref[8:16, :] = rest
    main, rest = total[0:32] / total[40:41], total[32:40] / rest
    copies(spread_ref, jnp.concatenate([main, rest], axis=0))


def put_vectors(spread_ref, vec_ref):
    count = spread_ref.shape[0]

    def put(tile, value):
        first = value.astype(BF16)
        at = tile * LANES
        vec_ref[0:32, at : at + LANES] = first
        vec_ref[32:64, at : at + LANES] = (value - first.astype(F32)).astype(BF16)

    for i in range(count):
        put(i, spread_ref[i, 0:32, :])
    for m in range(count // 4):
        put(count + m, unfold([spread_ref[4 * m + q, 32:40, :] for q in range(4)]))


def second_product(aff_ref, vec_ref, send_ref):
    main, rest = blocks_of(send_ref.shape[0])

    def product(at, width):
        out = jnp.dot(vec_ref[...], aff_ref[:, at : at + width], preferred_element_type=F32)
        return out[0:32] + out[32:64]

    out = product(*rest)
    for m in range(rest[1] // LANES):
        for q in range(4):
            send_ref[4 * m + q, 32:40, :] = fold(out[:, m * LANES : (m + 1) * LANES], q)
    for at, width in main:
        out = product(at, width)
        for k in range(width // LANES):
            send_ref[at // LANES + k, 0:32, :] = out[:, k * LANES : (k + 1) * LANES]


def put_gram(gram, send_ref):
    for i in range(send_ref.shape[0]):
        send_ref[i, 40:48, :] = gram


def away_again_body(aff_ref, spread_ref, send_ref, vec_ref, gram_ref):
    put_vectors(spread_ref, vec_ref)
    vec = vec_ref[...]
    gram = lax.dot_general(vec, vec, (((1,), (1,)), ((), ())), preferred_element_type=F32)
    gram = gram[0:32] + gram[32:64]
    gram = fold(widen(gram[:, 0:32] + gram[:, 32:64]))
    gram_ref[...] = gram
    second_product(aff_ref, vec_ref, send_ref)
    put_gram(gram, send_ref)


def home_again_body(aff_ref, vec_ref, gram_ref, send_ref):
    second_product(aff_ref, vec_ref, send_ref)
    put_gram(gram_ref[...], send_ref)


def solved(gram, right):
    size = 4 * gram.shape[0]
    wide = right.shape[1] // LANES
    columns = [
        jnp.concatenate(
            [
                jnp.broadcast_to(gram[:, REST * g + k : REST * g + k + 1], (8, LANES))
                for g in range(k // 8, 4)
            ],
            axis=0,
        )
        for k in range(size)
    ]
    rows = [right[8 * g : 8 * g + 8] for g in range(size // 8)]
    for j in range(size):
        base, at = j // 8, j % 8
        pivot = columns[j][at : at + 1]
        scale = lax.rsqrt(pivot)
        scale = scale * (1.5 - 0.5 * pivot * scale * scale)
        factor = columns[j] * scale
        for k in range(j + 1, size):
            skip = 8 * (k // 8 - base)
            mine = factor[k - 8 * base : k - 8 * base + 1]
            columns[k] = columns[k] - factor[skip:] * mine
        top = rows[base][at : at + 1] * jnp.concatenate([scale] * wide, axis=1)
        for g in range(base, size // 8):
            part = factor[8 * (g - base) : 8 * (g - base) + 8]
            if g == base:
                row = row_of((8, LANES))
                part = jnp.where(row > at, part, 0.0)
            new = rows[g] - jnp.concatenate([part] * wide, axis=1) * top
            if g == base:
                new = jnp.where(row_of(new.shape) == at, top, new)
            rows[g] = new
    return jnp.concatenate(rows, axis=0)


def middle_body(points):
    def body(recv_ref, degree_ref, scaled_ref, gram_ref):
        total = jnp.sum(recv_ref[...], axis=0)
        main = total[0:32] / degree_ref[0:1, :]
        rest = total[32:40] / degree_ref[8:16, :]
        scaled = solved(total[40:48] / points, whole(main, rest))
        scaled_ref[...] = scaled
        copies(gram_ref, fold(widen(gram_of(scaled))))

    return body


def again_body(recv_ref, gram_ref):
    copies(gram_ref, jnp.sum(recv_ref[...], axis=0))


def last_body(points):
    def body(recv_ref, scaled_ref, out_ref):
        gram = jnp.sum(recv_ref[...], axis=0) / points
        out_ref[...] = solved(gram, scaled_ref[...])[:, 0 : out_ref.shape[1]]

    return body


def shards(points, start_vectors):
    group, features = points.shape
    row, half, cores = lax.axis_size("row"), lax.axis_size("z"), lax.axis_size("core")
    col = half * cores
    total = group * row * col
    log_scale = 2.0 * KERNEL_SCALE / features * math.log2(math.e)
    lanes = half * group
    right_shape = pltpu.VMEM((LANES, lanes), BF16)
    shape = jax.ShapeDtypeStruct

    def exchange(x, axis):
        return lax.all_to_all(x, axis, 0, 0, tiled=True)

    def swap(x):
        return lax.ppermute(x, "core", [(0, 1), (1, 0)])

    def call(body, out_shape, *args, scratch=(), **kwargs):
        return pl.pallas_call(
            body, out_shape=out_shape, scratch_shapes=scratch, compiler_params=PARAMS, **kwargs
        )(*args)

    hbm_space = pl.BlockSpec(memory_space=pltpu.HBM)
    cols, rows = call(
        pack_body,
        (shape((row, group + 40, LANES), BF16), pltpu.VMEM((80, LANES), BF16)),
        pltpu.with_memory_space_constraint(points.T, pltpu.HBM),
        pltpu.with_memory_space_constraint(start_vectors.T, pltpu.HBM),
        scratch=(
            pltpu.VMEM((features, group), BF16),
            pltpu.VMEM((start_vectors.shape[1], group), BF16),
            pltpu.VMEM((group + 40, LANES), BF16),
            pltpu.SemaphoreType.DMA((2 + row,)),
        ),
        in_specs=[hbm_space, hbm_space],
        out_specs=(hbm_space, pl.BlockSpec(memory_space=pltpu.VMEM)),
    )
    cols = exchange(cols, "row")
    rows = lax.all_gather(rows, ("z", "core"))
    aff_shape = pltpu.VMEM((row * group, lanes), BF16)
    send_shape = shape((half, 48, LANES), F32)
    away_aff, away_send, left, vec = call(
        away_body(log_scale),
        (
            aff_shape,
            send_shape,
            pltpu.VMEM((row * group, LANES), BF16),
            pltpu.VMEM((48, row * group), BF16),
        ),
        rows,
        cols,
        scratch=(right_shape,),
    )
    other = swap(away_send)
    home_aff, home_send = call(
        home_body(log_scale), (aff_shape, send_shape), rows, left, vec, scratch=(right_shape,)
    )
    send = call(join_body, send_shape, home_send, other)
    spread, degree = call(
        scale_body, (shape((row, 40, LANES), F32), shape((16, LANES), F32)), exchange(send, "z")
    )
    away_send, vec, gram = call(
        away_again_body,
        (send_shape, pltpu.VMEM((64, row * group), BF16), pltpu.VMEM((8, LANES), F32)),
        away_aff,
        exchange(spread, "row"),
    )
    other = swap(away_send)
    home_send = call(home_again_body, send_shape, home_aff, vec, gram)
    send = call(join_body, send_shape, home_send, other)
    scaled, gram = call(
        middle_body(total),
        (shape((32, 2 * LANES), F32), shape((col, 8, LANES), F32)),
        exchange(send, "z"),
        degree,
    )
    gram = exchange(gram, ("z", "core"))
    gram = call(again_body, shape((row, 8, LANES), F32), gram)
    out = call(last_body(total), shape((32, group), F32), exchange(gram, "row"), scaled)
    return out.T


def solution(mesh):
    rows, cols = mesh.devices.shape
    finer = Mesh(mesh.devices.reshape(rows, cols // 2, 2), ("row", "z", "core"))
    spec = P(("row", "z", "core"), None)
    return jax.shard_map(
        shards, mesh=finer, in_specs=(spec, spec), out_specs=spec, check_vma=False
    )
```
